32 devices in a mesh: dp: 8 (over z, y), mp: 4 (over x, core).
Axes of the slice: x: 2, y: 2, z: 4, core: 2. Of those that a mesh axis runs over, the one named last changes fastest.
Arguments:
- gradient: bfloat16 [1, 4096, 4096], P(None, 'mp', 'dp'), may hold values from -6 to 6
- first_moment: float32 [1, 4096, 4096], P(None, 'mp', 'dp'), may hold values from -3 to 3
- second_moment: float32 [1, 4096, 4096], P(None, 'mp', 'dp'), may hold values from 0.0625 to 1
- left_factor: float32 [1, 4096, 4096], P(None, 'mp', 'dp'), may hold values from -18 to 18
- right_factor: float32 [1, 4096, 4096], P(None, 'mp', 'dp'), may hold values from -18 to 18
- left_basis: bfloat16 [1, 4096, 4096], P(None, 'dp', 'mp'), may hold values from -0.09375 to 0.09375
- right_basis: bfloat16 [1, 4096, 4096], P(None, 'mp', 'dp'), may hold values from -0.09375 to 0.09375
Outputs:
- new_first_moment: float32 [1, 4096, 4096], P(None, 'mp', 'dp')
- new_second_moment: float32 [1, 4096, 4096], P(None, 'mp', 'dp')
- new_left_factor: float32 [1, 4096, 4096], P(None, 'mp', 'dp')
- new_right_factor: float32 [1, 4096, 4096], P(None, 'mp', 'dp')
- update: bfloat16 [1, 4096, 4096], P(None, 'mp', 'dp')
The draws below stay inside these ranges and needn't reach their ends.
All inputs are finite; a program needn't handle non-finite values.
Results may differ from the reference program's by a relative error of at most 0.014.
Values may be sent and summed in bfloat16 or wider, within the bound.
A program may use at most 128 MiB of HBM per device.

```python
import math
import jax
import jax.numpy as jnp
from jax import lax

B = 4096
BLOCKS = 1


def shard_levels(rng, dims, split, low, high):
    def one(position, shards_of):
        steps = jax.random.uniform(jax.random.fold_in(jax.random.fold_in(rng, 6), position), (shards_of,), jnp.float32, low / len(split), high / len(split))
        return jnp.repeat(jnp.exp(steps), dims[position] // shards_of).reshape((-1,) + (1,) * (len(dims) - position - 1))

    level = one(*split[0])
    for cut in split[1:]:
        level = level * one(*cut)
    return level


def scatter_about(stream_key, shape, spread, reach, split=(), dtype=jnp.bfloat16):
    drawn = spread * jax.random.normal(stream_key, shape, jnp.float32)
    if split:
        drawn = drawn * shard_levels(stream_key, shape, split, -0.22, 0.18)
    return jnp.clip(drawn, -reach, reach).astype(dtype)


def setup_inputs(seed: int = 0) -> dict:
    splits = jax.random.split(jax.random.key(seed), 8)
    gradient = scatter_about(splits[0], (BLOCKS, B, B), 1.0, 6.0, ((1, 4), (2, 8)))
    first_moment = scatter_about(splits[1], (BLOCKS, B, B), 0.5, 3.0, ((1, 4), (2, 8)), jnp.float32)
    second_moment = jnp.clip(jnp.exp(math.log(1.0) - 2.7725887 * jax.random.uniform(splits[2], (BLOCKS, B, B), jnp.float32) ** shard_levels(splits[2], (BLOCKS, B, B), ((1, 4), (2, 8)), -0.2, 0.2)), 0.0625, 1.0)
    left_factor = scatter_about(splits[3], (BLOCKS, B, B), 3.0, 18.0, ((1, 4), (2, 8)), jnp.float32)
    right_factor = scatter_about(splits[4], (BLOCKS, B, B), 3.0, 18.0, ((1, 4), (2, 8)), jnp.float32)
    left_basis = scatter_about(splits[5], (BLOCKS, B, B), B ** -0.5, 0.09375, ((1, 8), (2, 4)))
    right_basis = scatter_about(splits[6], (BLOCKS, B, B), B ** -0.5, 0.09375, ((1, 4), (2, 8)))
    return {"gradient": gradient, "first_moment": first_moment, "second_moment": second_moment, "left_factor": left_factor, "right_factor": right_factor, "left_basis": left_basis, "right_basis": right_basis}


decay_moment = 0.95
decay_factor = 0.95
epsilon = 1e-08

def product(left, right):
    return jnp.dot(left.astype(jnp.float32), right.astype(jnp.float32), precision=lax.Precision.HIGHEST)

def single_block(operands):
    gradient, first_moment, second_moment, left_factor, right_factor, left_basis, right_basis = operands
    scale = 1.0 - decay_factor
    new_left = decay_factor * left_factor + scale * product(gradient, gradient.T)
    new_right = decay_factor * right_factor + scale * product(gradient.T, gradient)
    rotated_left = product(left_basis.T, gradient).astype(jnp.bfloat16)
    rotated = product(rotated_left, right_basis)
    new_first = decay_moment * first_moment + (1.0 - decay_moment) * rotated
    new_second = decay_moment * second_moment + (1.0 - decay_moment) * rotated * rotated
    direction = (new_first / (jnp.sqrt(new_second) + epsilon)).astype(jnp.bfloat16)
    back_left = product(left_basis, direction).astype(jnp.bfloat16)
    update = product(back_left, right_basis.T).astype(jnp.bfloat16)
    return (new_first, new_second, new_left, new_right, update)

def reference(gradient, first_moment, second_moment, left_factor, right_factor, left_basis, right_basis):
    first_out, second_out, left_out, right_out, update_out = lax.map(single_block, (gradient, first_moment, second_moment, left_factor, right_factor, left_basis, right_basis))
    return (first_out, second_out, left_out, right_out, update_out)
```

```python
import functools

import jax
import jax.numpy as jnp
from jax import lax
from jax.experimental import pallas as pl
from jax.experimental.pallas import tpu as pltpu
from jax.sharding import PartitionSpec as P

decay_moment = 0.95
decay_factor = 0.95
epsilon = 1e-08
bf16, f32 = jnp.bfloat16, jnp.float32
MESH = pl.DeviceIdType.MESH


def kernel(dp, mp, rows, cols, chunks, *refs):
    (grad, first, second, left_f, right_f, left_b, right_b,
     out_first, out_second, out_left, out_right, out_update,
     gbuf, lbuf, rbuf, rrbuf, pbuf, ssend, rrecv, urecv, yrecv, zrecv,
     fac_l, fac_r, mom1, mom2, acc, dbuf, bbuf,
     load_sem, store_sem, zs_up, zs_dn, zr, ys, yr, es, er, as_, ar,
     rs, rr, us, ur, ps, pr, bys, byr, bzs, bzr) = refs
    Z, q = dp // 2, rows // cols
    cw = cols // chunks
    d, m = lax.axis_index("dp"), lax.axis_index("mp")
    z, y = lax.div(d, 2), lax.rem(d, 2)
    last = Z - 1
    ynbr = z * 2 + (1 - y)
    tile = min(256, rows)

    def send(src, dst, s, r, dev):
        return pltpu.make_async_remote_copy(
            src_ref=src, dst_ref=dst, send_sem=s, recv_sem=r, device_id=dev, device_id_type=MESH
        )

    def when(cond, fn):
        pl.when(cond)(fn)

    def loop(n, fn):
        def body(i, c):
            fn(i)
            return c
        lax.fori_loop(0, n, body, 0)

    def tiles(n, size, fn):
        loop(n // size, lambda i: fn(pl.ds(pl.multiple_of(i * size, size), size)))

    loads = [
        (grad, gbuf.at[d]), (left_b, lbuf.at[d]), (right_b, rbuf.at[m]),
        (first, mom1), (second, mom2), (left_f, fac_l), (right_f, fac_r),
    ]
    load = [pltpu.make_async_copy(a, b, load_sem.at[i]) for i, (a, b) in enumerate(loads)]
    for c in load:
        c.start()

    barrier = pltpu.get_barrier_semaphore()
    pl.semaphore_signal(barrier, inc=1, device_id=(ynbr, m), device_id_type=MESH)
    when(z > 0, lambda: pl.semaphore_signal(barrier, inc=1, device_id=(d - 2, m), device_id_type=MESH))
    when(z < last, lambda: pl.semaphore_signal(barrier, inc=1, device_id=(d + 2, m), device_id_type=MESH))
    for k in range(1, mp):
        pl.semaphore_signal(barrier, inc=1, device_id=(d, lax.rem(m + k, mp)), device_id_type=MESH)
    along = (z > 0).astype(jnp.int32) + (z < last).astype(jnp.int32)
    pl.semaphore_wait(barrier, mp + along)

    bufs = [gbuf, lbuf]

    def half(a, b, hb):
        n = bufs[a].shape[1] // 2
        return bufs[a].at[b, pl.ds(hb * n, n), :]

    def up(a, zb):
        blk = bufs[a].at[zb * 2 + y]
        return send(blk, blk, zs_up.at[a, zb], zr.at[a, zb], (d + 2, m))

    def dn(a, zb):
        blk = bufs[a].at[zb * 2 + y]
        return send(blk, blk, zs_dn.at[a, zb], zr.at[a, zb], (d - 2, m))

    def ysend(a, zb, hb):
        blk = half(a, zb * 2 + y, hb)
        return send(blk, blk, ys.at[a, zb, hb], yr.at[a, zb, hb], (ynbr, m))

    def yrecv_desc(a, zb, hb):
        blk = half(a, zb * 2 + (1 - y), hb)
        return send(blk, blk, ys.at[a, zb, hb], yr.at[a, zb, hb], (ynbr, m))

    def extra(a, k):
        zb = 0 if k == 0 else last
        blk = half(a, zb * 2 + (1 - y), 1)
        return send(blk, blk, es.at[a, k], er.at[a, k], (d + 2, m) if k == 0 else (d - 2, m))

    def in_line(zb):
        return jnp.logical_and(zb >= 0, zb <= last)

    def y_second(zb):
        inner = jnp.logical_and(zb > 0, zb < last)
        return jnp.logical_or(zb == z, inner)

    def y_sends(a, zb, op):
        op(ysend(a, zb, 0))
        when(y_second(zb), lambda: op(ysend(a, zb, 1)))

    def start(c):
        c.start()

    def ag_up_own(a):
        when(z < last, lambda: up(a, z).start())

    def ag_dn_own(a):
        when(z > 0, lambda: dn(a, z).start())

    def ag_step(a, s, then, on_block):
        below, above = z - s, z + s

        def from_below():
            up(a, below).wait_recv()
            when(z < last, lambda: up(a, below).start())

        def from_above():
            dn(a, above).wait_recv()
            when(z > 0, lambda: dn(a, above).start())

        when(below >= 0, from_below)
        if then:
            when(z == s, lambda: ag_up_own(1))
        when(above <= last, from_above)
        if then:
            when(last - z == s, lambda: ag_dn_own(1))
        when(below >= 0, lambda: y_sends(a, below, start))
        when(above <= last, lambda: y_sends(a, above, start))

        def extra_dn():
            when(z == last, lambda: yrecv_desc(a, z, 1).wait_recv())
            when(z < last, lambda: extra(a, 1).wait_recv())
            extra(a, 1).start()

        def extra_up():
            when(z == 0, lambda: yrecv_desc(a, z, 1).wait_recv())
            when(z > 0, lambda: extra(a, 0).wait_recv())
            extra(a, 0).start()

        when(jnp.logical_and(z == Z - s, z > 0), extra_dn)
        when(jnp.logical_and(z == s - 1, z < last), extra_up)
        if on_block is not None:
            when(below >= 0, lambda: on_block(below * 2 + y))
            when(above <= last, lambda: on_block(above * 2 + y))

    def wait_y(a, zb):
        yrecv_desc(a, zb, 0).wait_recv()
        inner = jnp.logical_and(zb > 0, zb < last)
        when(inner, lambda: yrecv_desc(a, zb, 1).wait_recv())
        when(jnp.logical_and(zb == last, z == 0), lambda: extra(a, 1).wait_recv())
        when(jnp.logical_and(zb == 0, z == last), lambda: extra(a, 0).wait_recv())

    def by_distance(fn, far_first=False):
        def step(i):
            s = last - i if far_first else i
            when(z - s >= 0, lambda: fn(z - s))
            when(jnp.logical_and(s > 0, z + s <= last), lambda: fn(z + s))
        loop(Z, step)

    def sub_rows(ref, db):
        off = pl.multiple_of(lax.rem(db, q) * cols, cols)
        return ref.at[lax.div(db, q), pl.ds(off, cols), :]

    def mp_send(a, buf, k):
        to = lax.rem(m + k, mp)
        return send(buf.at[m], buf.at[m], as_.at[a, k], ar.at[a, m], (d, to))

    def mp_wait(a, buf):
        for k in range(1, mp):
            src = lax.rem(m + k, mp)
            send(buf.at[src], buf.at[src], as_.at[a, k], ar.at[a, src], (d, src)).wait_recv()

    load[0].wait()
    when(z < last, lambda: up(0, z).start())
    when(z > 0, lambda: dn(0, z).start())
    y_sends(0, z, start)
    load[2].wait()
    for k in range(1, mp):
        mp_send(0, rbuf, k).start()
    load[1].wait()
    when(z == 0, lambda: ag_up_own(1))
    when(z == last, lambda: ag_dn_own(1))

    def r_send(db):
        to, sub = lax.div(db, q), lax.rem(db, q)
        return send(ssend.at[db], rrecv.at[m, sub], rs.at[db], rr.at[m, sub], (d, to))

    def r_term(db):
        def one(t):
            term = lax.dot_general(
                gbuf[db, :, t], gbuf[d], (((0,), (0,)), ((), ())), preferred_element_type=f32
            )
            ssend[db, t, :] = term.astype(bf16)
        tiles(cols, min(256, cols), one)
        when(lax.div(db, q) != m, lambda: r_send(db).start())

    def rr_term(db):
        rhs = sub_rows(rbuf, db)
        def one(t):
            acc[t, :] += jnp.dot(gbuf[db, t, :], rhs[...], preferred_element_type=f32)
        tiles(rows, tile, one)

    def zero_acc():
        def one(t):
            acc[t, :] = jnp.zeros((tile, cols), f32)
        tiles(rows, tile, one)

    r_term(d)
    loop(Z - 1, lambda i: ag_step(0, i + 1, True, r_term))
    y_sends(1, z, start)
    zero_acc()
    mp_wait(0, rbuf)
    by_distance(lambda zb: rr_term(zb * 2 + y))

    def y_block(zb):
        wait_y(0, zb)
        rr_term(zb * 2 + 1 - y)
        r_term(zb * 2 + 1 - y)
    by_distance(y_block)

    def rr_out(t):
        rrbuf[m, t, :] = acc[t, :].astype(bf16)
    tiles(rows, tile, rr_out)
    for k in range(1, mp):
        mp_send(1, rrbuf, k).start()

    owner = lax.div(d, q)
    core, chip = lax.rem(m, 2), lax.div(m, 2)
    own_chip, own_core = lax.div(owner, 2), lax.rem(owner, 2)
    partner = chip * 2 + (1 - core)
    hd = dp // 2
    pair_off = pl.multiple_of(lax.rem(d, q) * cols, cols)

    def p_send(hb, i, to):
        part = pbuf.at[pl.ds(hb * hd, hd)]
        return send(part, part, ps.at[i], pr.at[hb], (d, to))

    def to_chips(op):
        for k in range(1, mp // 2):
            other = lax.rem(chip + k, mp // 2)
            op(p_send(core, 2 + k, other * 2 + core))

    def own_pair():
        def copy(i):
            pbuf[i] = gbuf[i, pl.ds(pair_off, cols), :]
        loop(dp, copy)
        for hb in range(2):
            p_send(hb, hb, partner).start()
        to_chips(start)
    when(m == owner, own_pair)

    loop(Z - 1, lambda i: ag_step(1, i + 1, False, None))

    def near_pair():
        for hb in range(2):
            p_send(hb, hb, partner).wait_recv()
        to_chips(start)
    when(jnp.logical_and(chip == own_chip, m != owner), near_pair)

    mp_wait(1, rrbuf)
    zero_acc()

    def m_term(db):
        rhs = sub_rows(rrbuf, db)
        def one(t):
            acc[t, :] += lax.dot_general(
                lbuf[db, :, t], rhs[...], (((0,), (0,)), ((), ())), preferred_element_type=f32
            )
        tiles(rows, tile, one)
    by_distance(lambda zb: m_term(zb * 2 + y))

    def y_block2(zb):
        wait_y(1, zb)
        m_term(zb * 2 + 1 - y)
    by_distance(y_block2)
    load[3].wait()
    load[4].wait()

    def moments(t):
        rot = acc[t, :]
        new1 = decay_moment * mom1[t, :] + (1.0 - decay_moment) * rot
        new2 = decay_moment * mom2[t, :] + (1.0 - decay_moment) * rot * rot
        mom1[t, :] = new1
        mom2[t, :] = new2
        dbuf[t, :] = (new1 / (jnp.sqrt(new2) + epsilon)).astype(bf16)
    tiles(rows, min(128, rows), moments)

    def lanes(h):
        return pl.ds(h * cw, cw)

    def back_term(db, h, t):
        off = pl.multiple_of(lax.rem(db, q) * cols + h * cw, cw)
        rhs = rbuf[lax.div(db, q), pl.ds(off, cw), :]
        return lax.dot_general(
            dbuf[t, :], rhs, (((1,), (1,)), ((), ())), preferred_element_type=f32
        )

    def by_send(h, zb):
        return send(rrbuf.at[zb, :, lanes(h)], yrecv.at[h, zb], bys.at[h, zb], byr.at[h, zb], (ynbr, m))

    for k in range(1, mp):
        mp_send(1, rrbuf, k).wait_send()
    for h in range(chunks):
        def first_half(zb, h=h):
            def one(t):
                rrbuf[zb, t, lanes(h)] = back_term(zb * 2 + 1 - y, h, t).astype(bf16)
            tiles(rows, tile, one)
            by_send(h, zb).start()
        by_distance(first_half, far_first=True)

    stores = [
        pltpu.make_async_copy(a, b, store_sem.at[i])
        for i, (a, b) in enumerate([
            (mom1, out_first), (mom2, out_second), (fac_l, out_left), (fac_r, out_right), (dbuf, out_update)
        ])
    ]
    stores[0].start()
    stores[1].start()

    def far_pair():
        p_send(core, 0, partner).wait_recv()
        p_send(core, 0, partner).start()
        p_send(1 - core, 0, partner).wait_recv()
    when(chip != own_chip, far_pair)
    load[5].wait()
    load[6].wait()

    def r_final():
        for k in range(1, mp):
            src = lax.rem(m + k, mp)
            for sub in range(q):
                send(ssend.at[sub], rrecv.at[src, sub], rs.at[sub], rr.at[src, sub], (d, src)).wait_recv()
        for sub in range(q):
            def one(t, sub=sub):
                total = ssend[m * q + sub, t, :].astype(f32)
                for k in range(1, mp):
                    total += rrecv[lax.rem(m + k, mp), sub, t, :].astype(f32)
                where = pl.ds(pl.multiple_of(sub * cols + t.start, 128), 128)
                fac_r[where, :] = decay_factor * fac_r[where, :] + (1.0 - decay_factor) * total
            tiles(cols, 128, one)
    r_final()
    stores[3].start()

    def l_scale(t):
        fac_l[t, :] = decay_factor * fac_l[t, :]
    tiles(rows, tile, l_scale)

    def l_term(db):
        def one(t):
            fac_l[t, :] += (1.0 - decay_factor) * lax.dot_general(
                gbuf[db, t, :], pbuf[db], (((1,), (1,)), ((), ())), preferred_element_type=f32
            )
        tiles(rows, tile, one)
    loop(dp, l_term)
    stores[2].start()
    loop(dp, lambda db: when(lax.div(db, q) != m, lambda: r_send(db).wait_send()))

    def bz_up(h, zb):
        return send(yrecv.at[h, zb], zrecv.at[h, zb], bzs.at[h, zb], bzr.at[h, zb], (d + 2, m))

    def bz_dn(h, zb):
        slot = jnp.where(zb == z - 1, Z, zb)
        return send(yrecv.at[h, zb], zrecv.at[h, slot], bzs.at[h, zb], bzr.at[h, slot], (d - 2, m))

    def bz_wait(h, slot):
        send(zrecv.at[h, slot], zrecv.at[h, slot], bzs.at[h, 0], bzr.at[h, slot], (ynbr, m)).wait_recv()

    def u_send(h, db):
        to, sub = lax.div(db, q), lax.rem(db, q)
        return send(
            ssend.at[db, :, lanes(h)],
            urecv.at[m, sub, :, lanes(h)], us.at[h, db], ur.at[h, m, sub], (d, to),
        )

    for h in range(chunks):
        def line(zb, h=h):
            by_send(h, zb).wait_recv()

            def one(t):
                acc[t, lanes(0)] = back_term(zb * 2 + y, h, t) + yrecv[h, zb, t, :].astype(f32)
            tiles(rows, tile, one)

            def add(slot):
                bz_wait(h, slot)
                def more(t):
                    acc[t, lanes(0)] += zrecv[h, slot, t, :].astype(f32)
                tiles(rows, tile, more)
            when(jnp.logical_and(zb >= z, z > 0), lambda: add(zb))
            when(jnp.logical_and(zb < z, z < last), lambda: add(zb))
            when(jnp.logical_and(zb == z, z < last), lambda: add(Z))

            def pack(t):
                yrecv[h, zb, t, :] = acc[t, lanes(0)].astype(bf16)

            def keep(t):
                bbuf[t, lanes(h)] = acc[t, lanes(0)].astype(bf16)
            when(zb != z, lambda: tiles(rows, tile, pack))
            when(zb > z, lambda: bz_up(h, zb).start())
            when(zb < z, lambda: bz_dn(h, zb).start())
            when(zb == z, lambda: tiles(rows, tile, keep))
        by_distance(line, far_first=True)

        def u_term(i, h=h):
            db = lax.rem(m * q + dp // 2 + i, dp)
            ssend[db, :, lanes(h)] = jnp.dot(
                lbuf[db], bbuf[:, lanes(h)], preferred_element_type=f32
            ).astype(bf16)
            when(lax.div(db, q) != m, lambda: u_send(h, db).start())
        loop(dp, u_term)

    for h in range(chunks):
        for k in range(1, mp):
            src = lax.rem(m + k, mp)
            for sub in range(q):
                dst = urecv.at[src, sub, :, lanes(h)]
                send(dst, dst, us.at[h, 0], ur.at[h, src, sub], (d, src)).wait_recv()
        for sub in range(q):
            def one(t, sub=sub, h=h):
                total = ssend[m * q + sub, t, lanes(h)].astype(f32)
                for k in range(1, mp):
                    total += urecv[lax.rem(m + k, mp), sub, t, lanes(h)].astype(f32)
                where = pl.ds(pl.multiple_of(sub * cols + t.start, 128), 128)
                dbuf[where, lanes(h)] = total.astype(bf16)
            tiles(cols, 128, one)
    stores[4].start()

    for a in range(2):
        def sent(i, a=a):
            when(jnp.logical_and(z < last, i <= z), lambda: up(a, i).wait_send())
            when(jnp.logical_and(z > 0, i >= z), lambda: dn(a, i).wait_send())
            y_sends(a, i, lambda c: c.wait_send())
        loop(Z, sent)
        when(z > 0, lambda a=a: extra(a, 1).wait_send())
        when(z < last, lambda a=a: extra(a, 0).wait_send())
    for k in range(1, mp):
        mp_send(0, rbuf, k).wait_send()

    def near_sent():
        to_chips(lambda c: c.wait_send())
    when(chip == own_chip, near_sent)

    def own_sent():
        for hb in range(2):
            p_send(hb, hb, partner).wait_send()
    when(m == owner, own_sent)
    when(chip != own_chip, lambda: p_send(core, 0, partner).wait_send())
    for h in range(chunks):
        def b_sent(i, h=h):
            by_send(h, i).wait_send()
            when(i != z, lambda: bz_up(h, i).wait_send())
        loop(Z, b_sent)
        loop(dp, lambda db, h=h: when(lax.div(db, q) != m, lambda: u_send(h, db).wait_send()))
    for c in stores:
        c.wait()


def solution(mesh):
    dp, mp = mesh.shape["dp"], mesh.shape["mp"]
    Z = dp // 2

    def per_device(*args):
        _, rows, cols = args[0].shape
        q = rows // cols
        chunks = 2
        cw = cols // chunks
        flat = [a.reshape(a.shape[1:]) for a in args]
        dma = pltpu.SemaphoreType.DMA
        outs = pl.pallas_call(
            functools.partial(kernel, dp, mp, rows, cols, chunks),
            out_shape=[jax.ShapeDtypeStruct((rows, cols), t) for t in (f32, f32, f32, f32, bf16)],
            in_specs=[pl.BlockSpec(memory_space=pl.ANY)] * 7,
            out_specs=[pl.BlockSpec(memory_space=pl.ANY)] * 5,
            scratch_shapes=[
                pltpu.VMEM((dp, rows, cols), bf16),
                pltpu.VMEM((dp, cols, rows), bf16),
                pltpu.VMEM((mp, rows, cols), bf16),
                pltpu.VMEM((mp, rows, cols), bf16),
                pltpu.VMEM((dp, cols, cols), bf16),
                pltpu.VMEM((dp, cols, cols), bf16),
                pltpu.VMEM((mp, q, cols, cols), bf16),
                pltpu.VMEM((mp, q, cols, cols), bf16),
                pltpu.VMEM((chunks, Z, rows, cw), bf16),
                pltpu.VMEM((chunks, Z + 1, rows, cw), bf16),
                pltpu.VMEM((rows, cols), f32),
                pltpu.VMEM((rows, cols), f32),
                pltpu.VMEM((rows, cols), f32),
                pltpu.VMEM((rows, cols), f32),
                pltpu.VMEM((rows, cols), f32),
                pltpu.VMEM((rows, cols), bf16),
                pltpu.VMEM((rows, cols), bf16),
                dma((7,)),
                dma((5,)),
                dma((2, Z)),
                dma((2, Z)),
                dma((2, Z)),
                dma((2, Z, 2)),
                dma((2, Z, 2)),
                dma((2, 2)),
                dma((2, 2)),
                dma((2, mp)),
                dma((2, mp)),
                dma((dp,)),
                dma((mp, q)),
                dma((chunks, dp)),
                dma((chunks, mp, q)),
                dma((2 + mp // 2,)),
                dma((2,)),
                dma((chunks, Z)),
                dma((chunks, Z)),
                dma((chunks, Z)),
                dma((chunks, Z + 1)),
            ],
            compiler_params=pltpu.CompilerParams(
                collective_id=0, has_side_effects=True, vmem_limit_bytes=67043328
            ),
        )(*flat)
        return tuple(o.reshape((1,) + o.shape) for o in outs)

    return jax.shard_map(
        per_device,
        mesh=mesh,
        in_specs=(P(None, "mp", "dp"),) * 5 + (P(None, "dp", "mp"), P(None, "mp", "dp")),
        out_specs=(P(None, "mp", "dp"),) * 5,
        check_vma=False,
    )
```

```python
import functools

import jax
import jax.numpy as jnp
from jax import lax
from jax.experimental import pallas as pl
from jax.experimental.pallas import tpu as pltpu
from jax.sharding import PartitionSpec as P

decay_moment = 0.95
decay_factor = 0.95
epsilon = 1e-08
bf16, f32 = jnp.bfloat16, jnp.float32
MESH = pl.DeviceIdType.MESH
PARTS, LAST = 2, 4


def kernel(dp, mp, rows, cols, parts, last_chunks, *refs):
    (grad, first, second, left_f, right_f, left_b, right_b,
     out_first, out_second, out_left, out_right, out_update,
     gbuf, lbuf, rbuf, rrbuf, pbuf, ssend, rrecv, urecv, ysrc, yrecv, zrecv,
     fac_l, fac_r, mom1, mom2, acc, dbuf, bbuf,
     load_sem, store_sem, zs_up, zs_dn, zr, ys, yr, es, er, as_, ar,
     rs, rr, us1, ur1, us2, ur2, ps, pr, bys, byr, bzs, bzr) = refs
    Z, q, X = dp // 2, rows // cols, mp // 2
    part = rows // parts
    d, m = lax.axis_index("dp"), lax.axis_index("mp")
    z, y = lax.div(d, 2), lax.rem(d, 2)
    core, chip = lax.rem(m, 2), lax.div(m, 2)
    partner = chip * 2 + (1 - core)
    last = Z - 1
    ynbr = z * 2 + (1 - y)
    tile = min(256, part)
    pieces = []
    for p in range(parts):
        n = last_chunks if p == parts - 1 else 1
        pieces.append([(p, i * (cols // n), cols // n) for i in range(n)])
    first_piece = [sum(len(x) for x in pieces[:p]) for p in range(parts)]

    def send(src, dst, s, r, dev):
        return pltpu.make_async_remote_copy(
            src_ref=src, dst_ref=dst, send_sem=s, recv_sem=r, device_id=dev, device_id_type=MESH
        )

    def when(cond, fn):
        pl.when(cond)(fn)

    def loop(n, fn):
        def body(i, c):
            fn(i)
            return c
        lax.fori_loop(0, n, body, 0)

    def tiles(n, size, fn, base=0):
        loop(n // size, lambda i: fn(pl.ds(pl.multiple_of(base + i * size, size), size)))

    loads = [
        (grad, gbuf.at[d]), (right_b, rbuf.at[m]),
        (first, mom1), (second, mom2), (left_f, fac_l), (right_f, fac_r),
    ]
    loads += [(left_b.at[:, pl.ds(p * part, part)], lbuf.at[p, d]) for p in range(parts)]
    load = [pltpu.make_async_copy(a, b, load_sem.at[i]) for i, (a, b) in enumerate(loads)]
    for c in load:
        c.start()

    barrier = pltpu.get_barrier_semaphore()
    pl.semaphore_signal(barrier, inc=1, device_id=(ynbr, m), device_id_type=MESH)
    when(z > 0, lambda: pl.semaphore_signal(barrier, inc=1, device_id=(d - 2, m), device_id_type=MESH))
    when(z < last, lambda: pl.semaphore_signal(barrier, inc=1, device_id=(d + 2, m), device_id_type=MESH))
    for k in range(1, mp):
        pl.semaphore_signal(barrier, inc=1, device_id=(d, lax.rem(m + k, mp)), device_id_type=MESH)
    along = (z > 0).astype(jnp.int32) + (z < last).astype(jnp.int32)
    pl.semaphore_wait(barrier, mp + along)

    def view(a, b):
        if a < 2:
            return gbuf.at[b, pl.ds(a * (rows // 2), rows // 2), :]
        return lbuf.at[a - 2, b]

    def half(a, b, hb):
        if a < 2:
            return gbuf.at[b, pl.ds(a * (rows // 2) + hb * (rows // 4), rows // 4), :]
        return lbuf.at[a - 2, b, pl.ds(hb * (cols // 2), cols // 2), :]

    def up(a, zb):
        blk = view(a, zb * 2 + y)
        return send(blk, blk, zs_up.at[a, zb], zr.at[a, zb], (d + 2, m))

    def dn(a, zb):
        blk = view(a, zb * 2 + y)
        return send(blk, blk, zs_dn.at[a, zb], zr.at[a, zb], (d - 2, m))

    def ysend(a, zb, hb):
        blk = half(a, zb * 2 + y, hb)
        return send(blk, blk, ys.at[a, zb, hb], yr.at[a, zb, hb], (ynbr, m))

    def yrecv_desc(a, zb, hb):
        blk = half(a, zb * 2 + (1 - y), hb)
        return send(blk, blk, ys.at[a, zb, hb], yr.at[a, zb, hb], (ynbr, m))

    def extra(a, k):
        zb = 0 if k == 0 else last
        blk = half(a, zb * 2 + (1 - y), 1)
        return send(blk, blk, es.at[a, k], er.at[a, k], (d + 2, m) if k == 0 else (d - 2, m))

    def y_second(zb):
        inner = jnp.logical_and(zb > 0, zb < last)
        return jnp.logical_or(zb == z, inner)

    def y_sends(a, zb, op):
        when(y_second(zb), lambda: op(ysend(a, zb, 1)))
        op(ysend(a, zb, 0))

    def start(c):
        c.start()

    def ag_own(a):
        when(z < last, lambda: up(a, z).start())
        when(z > 0, lambda: dn(a, z).start())

    def ag_step(a, s, then=None):
        below, above = z - s, z + s

        def from_below():
            up(a, below).wait_recv()
            when(z < last, lambda: up(a, below).start())

        def from_above():
            dn(a, above).wait_recv()
            when(z > 0, lambda: dn(a, above).start())

        when(below >= 0, from_below)
        when(above <= last, from_above)
        when(below >= 0, lambda: y_sends(a, below, start))
        when(above <= last, lambda: y_sends(a, above, start))

        def extra_dn():
            when(z == last, lambda: yrecv_desc(a, z, 1).wait_recv())
            when(z < last, lambda: extra(a, 1).wait_recv())
            extra(a, 1).start()
            if then is not None:
                dn(then, z).start()

        def extra_up():
            when(z == 0, lambda: yrecv_desc(a, z, 1).wait_recv())
            when(z > 0, lambda: extra(a, 0).wait_recv())
            extra(a, 0).start()
            if then is not None:
                up(then, z).start()

        when(jnp.logical_and(z == Z - s, z > 0), extra_dn)
        when(jnp.logical_and(z == s - 1, z < last), extra_up)

    def wait_y(a, zb):
        yrecv_desc(a, zb, 0).wait_recv()
        inner = jnp.logical_and(zb > 0, zb < last)
        when(inner, lambda: yrecv_desc(a, zb, 1).wait_recv())
        when(jnp.logical_and(zb == last, z == 0), lambda: extra(a, 1).wait_recv())
        when(jnp.logical_and(zb == 0, z == last), lambda: extra(a, 0).wait_recv())

    def at_distance(s, fn):
        when(z - s >= 0, lambda: fn(z - s))
        when(jnp.logical_and(s > 0, z + s <= last), lambda: fn(z + s))

    def by_distance(fn, far_first=False):
        loop(Z, lambda i: at_distance(last - i if far_first else i, fn))

    def sub_rows(ref, db):
        off = pl.multiple_of(lax.rem(db, q) * cols, cols)
        return ref.at[lax.div(db, q), pl.ds(off, cols), :]

    def mp_copy(a, buf, src, k, to):
        return send(buf.at[src], buf.at[src], as_.at[a, k], ar.at[a, src], (d, to))

    def mp_first(a, buf, op):
        for k in range(1, X):
            op(mp_copy(a, buf, m, X + k, lax.rem(chip + k, X) * 2 + core))
        op(mp_copy(a, buf, m, 0, partner))

    def mp_relay(a, buf):
        for k in range(1, X):
            src = lax.rem(chip + k, X) * 2 + core
            mp_copy(a, buf, src, k, partner).wait_recv()
            mp_copy(a, buf, src, k, partner).start()

    def mp_wait(a, buf):
        for k in range(X):
            src = lax.rem(chip + k, X) * 2 + 1 - core
            mp_copy(a, buf, src, k, partner).wait_recv()

    def mp_sent(a, buf):
        mp_first(a, buf, lambda c: c.wait_send())
        for k in range(1, X):
            mp_copy(a, buf, lax.rem(chip + k, X) * 2 + core, k, partner).wait_send()

    load[0].wait()
    for a in range(2):
        ag_own(a)
        y_sends(a, z, start)
    load[1].wait()
    mp_first(0, rbuf, start)
    for p in range(parts):
        load[6 + p].wait()

    def r_send(db):
        to, sub = lax.div(db, q), lax.rem(db, q)
        return send(ssend.at[db], rrecv.at[m, sub], rs.at[db], rr.at[m, sub], (d, to))

    def r_term(db):
        def one(t):
            term = lax.dot_general(
                gbuf[db, :, t], gbuf[d], (((0,), (0,)), ((), ())), preferred_element_type=f32
            )
            ssend[db, t, :] = term.astype(bf16)
        tiles(cols, min(256, cols), one)
        when(lax.div(db, q) != m, lambda: r_send(db).start())

    def rr_term(db):
        rhs = sub_rows(rbuf, db)
        def one(t):
            acc[t, :] += jnp.dot(gbuf[db, t, :], rhs[...], preferred_element_type=f32)
        tiles(rows, tile, one)

    def zero_acc():
        def one(t):
            acc[t, :] = jnp.zeros((tile, cols), f32)
        tiles(rows, tile, one)

    r_term(d)

    def g_step(i):
        s = i + 1
        ag_step(0, s)
        ag_step(1, s, then=2)
        when(s == min(2, last), lambda: mp_relay(0, rbuf))
        at_distance(s, lambda zb: r_term(zb * 2 + y))
    loop(Z - 1, g_step)
    y_sends(2, z, start)
    zero_acc()
    mp_wait(0, rbuf)
    by_distance(lambda zb: rr_term(zb * 2 + y))

    def y_block(zb):
        wait_y(0, zb)
        wait_y(1, zb)
        rr_term(zb * 2 + 1 - y)
    by_distance(y_block)

    def rr_out(t):
        rrbuf[m, t, :] = acc[t, :].astype(bf16)
    tiles(rows, tile, rr_out)
    mp_first(1, rrbuf, start)
    zero_acc()

    owner = lax.div(d, q)
    own_chip = lax.div(owner, 2)
    hd = dp // 2
    pair_off = pl.multiple_of(lax.rem(d, q) * cols, cols)

    def p_send(hb, i, to):
        view_p = pbuf.at[pl.ds(hb * hd, hd)]
        return send(view_p, view_p, ps.at[i], pr.at[hb], (d, to))

    def to_chips(op):
        for k in range(1, X):
            op(p_send(core, 2 + k, lax.rem(chip + k, X) * 2 + core))

    def own_pair():
        def copy(i):
            pbuf[i] = gbuf[i, pl.ds(pair_off, cols), :]
        loop(dp, copy)
        for hb in range(2):
            p_send(hb, hb, partner).start()
        to_chips(start)

    def near_pair():
        for hb in range(2):
            p_send(hb, hb, partner).wait_recv()
        to_chips(start)

    def far_pair():
        p_send(core, 0, partner).wait_recv()
        p_send(core, 0, partner).start()
        p_send(1 - core, 0, partner).wait_recv()

    when(m == owner, own_pair)

    def back_term(db, piece, t):
        _, c0, cw = piece
        off = pl.multiple_of(lax.rem(db, q) * cols + c0, cw)
        rhs = rbuf[lax.div(db, q), pl.ds(off, cw), :]
        return lax.dot_general(
            dbuf[t, :], rhs, (((1,), (1,)), ((), ())), preferred_element_type=f32
        )

    def by_send(i, piece, zb):
        p, c0, cw = piece
        c = pl.ds(c0, cw)
        return send(ysrc.at[zb, :, c], yrecv.at[p, zb, :, c], bys.at[i, zb], byr.at[i, zb], (ynbr, m))

    def rows_of(t, p):
        return pl.ds(pl.multiple_of(t.start + p * part, tile), tile)

    def scatter_first(p):
        for i, piece in enumerate(pieces[p], first_piece[p]):
            c = pl.ds(piece[1], piece[2])

            def one_block(zb, i=i, piece=piece, c=c):
                def one(t):
                    ysrc[zb, t, c] = back_term(zb * 2 + 1 - y, piece, rows_of(t, p)).astype(bf16)
                tiles(part, tile, one)
                by_send(i, piece, zb).start()
            by_distance(one_block, far_first=True)

    def bz_up(i, piece, zb):
        p, c0, cw = piece
        c = pl.ds(c0, cw)
        return send(yrecv.at[p, zb, :, c], zrecv.at[p, zb, :, c], bzs.at[i, zb], bzr.at[i, zb], (d + 2, m))

    def bz_dn(i, piece, zb):
        p, c0, cw = piece
        c = pl.ds(c0, cw)
        slot = jnp.where(zb == z - 1, Z, zb)
        return send(yrecv.at[p, zb, :, c], zrecv.at[p, slot, :, c], bzs.at[i, zb], bzr.at[i, slot], (d - 2, m))

    def line(i, piece, zb):
        p, c0, cw = piece
        c = pl.ds(c0, cw)
        by_send(i, piece, zb).wait_recv()

        def one(t):
            acc[t, pl.ds(0, cw)] = back_term(zb * 2 + y, piece, rows_of(t, p)) + yrecv[p, zb, t, c].astype(f32)
        tiles(part, tile, one)

        def add(slot):
            dst = zrecv.at[p, slot, :, c]
            send(dst, dst, bzs.at[i, 0], bzr.at[i, slot], (ynbr, m)).wait_recv()

            def more(t):
                acc[t, pl.ds(0, cw)] += zrecv[p, slot, t, c].astype(f32)
            tiles(part, tile, more)
        when(jnp.logical_and(zb >= z, z > 0), lambda: add(zb))
        when(jnp.logical_and(zb < z, z < last), lambda: add(zb))
        when(jnp.logical_and(zb == z, z < last), lambda: add(Z))

        def pack(t):
            yrecv[p, zb, t, c] = acc[t, pl.ds(0, cw)].astype(bf16)

        def keep(t):
            bbuf[rows_of(t, p), c] = acc[t, pl.ds(0, cw)].astype(bf16)
        when(zb != z, lambda: tiles(part, tile, pack))
        when(zb > z, lambda: bz_up(i, piece, zb).start())
        when(zb < z, lambda: bz_dn(i, piece, zb).start())
        when(zb == z, lambda: tiles(part, tile, keep))

    def scatter_step(p, s):
        for i, piece in enumerate(pieces[p], first_piece[p]):
            at_distance(s, lambda zb, i=i, piece=piece: line(i, piece, zb))

    def y_scattered(p):
        for i, piece in enumerate(pieces[p], first_piece[p]):
            loop(Z, lambda zb, i=i, piece=piece: by_send(i, piece, zb).wait_send())

    mom_tile = min(128, part)

    def m_term(p, db):
        rhs = sub_rows(rrbuf, db)
        def one(t):
            acc[t, :] += lax.dot_general(
                lbuf[p, db, :, t], rhs[...], (((0,), (0,)), ((), ())), preferred_element_type=f32
            )
        tiles(part, tile, one)

    def zero_part():
        def one(t):
            acc[t, :] = jnp.zeros((tile, cols), f32)
        tiles(part, tile, one)

    def moments(p):
        def one(t):
            w = pl.ds(pl.multiple_of(t.start + p * part, mom_tile), mom_tile)
            rot = acc[t, :]
            new1 = decay_moment * mom1[w, :] + (1.0 - decay_moment) * rot
            new2 = decay_moment * mom2[w, :] + (1.0 - decay_moment) * rot * rot
            mom1[w, :] = new1
            mom2[w, :] = new2
            dbuf[w, :] = (new1 / (jnp.sqrt(new2) + epsilon)).astype(bf16)
        tiles(part, mom_tile, one)

    def direction(p):
        def y_part(zb):
            wait_y(2 + p, zb)
            m_term(p, zb * 2 + 1 - y)
        by_distance(y_part)
        moments(p)

    by_distance(lambda zb: r_term(zb * 2 + 1 - y))

    def l_step(i):
        s = i + 1
        when(s == last, lambda: mp_relay(1, rrbuf))
        ag_step(2, s, then=3 if parts > 1 else None)
        when(jnp.logical_and(s == min(2, last), jnp.logical_and(chip == own_chip, m != owner)), near_pair)
    loop(Z - 1, l_step)
    if parts > 1:
        y_sends(3, z, start)
    mp_wait(1, rrbuf)
    load[2].wait()
    load[3].wait()
    by_distance(lambda zb: m_term(0, zb * 2 + y))
    direction(0)
    scatter_first(0)
    for p in range(1, parts):
        def both(i, p=p):
            s = i + 1
            ag_step(2 + p, s, then=3 + p if p + 1 < parts else None)
            scatter_step(p - 1, Z - s)
        loop(Z - 1, both)
        if p + 1 < parts:
            y_sends(3 + p, z, start)
        scatter_step(p - 1, 0)
        zero_part()
        by_distance(lambda zb, p=p: m_term(p, zb * 2 + y))
        direction(p)
        y_scattered(p - 1)
        scatter_first(p)

    stores = [
        pltpu.make_async_copy(a, b, store_sem.at[i])
        for i, (a, b) in enumerate([
            (mom1, out_first), (mom2, out_second), (fac_l, out_left), (fac_r, out_right), (dbuf, out_update)
        ])
    ]
    stores[0].start()
    stores[1].start()

    when(chip != own_chip, far_pair)
    load[4].wait()
    load[5].wait()

    for k in range(1, mp):
        src = lax.rem(m + k, mp)
        for sub in range(q):
            send(ssend.at[sub], rrecv.at[src, sub], rs.at[sub], rr.at[src, sub], (d, src)).wait_recv()
    for sub in range(q):
        def r_one(t, sub=sub):
            total = ssend[m * q + sub, t, :].astype(f32)
            for k in range(1, mp):
                total += rrecv[lax.rem(m + k, mp), sub, t, :].astype(f32)
            where = pl.ds(pl.multiple_of(sub * cols + t.start, 128), 128)
            fac_r[where, :] = decay_factor * fac_r[where, :] + (1.0 - decay_factor) * total
        tiles(cols, 128, r_one)
    stores[3].start()

    def l_scale(t):
        fac_l[t, :] = decay_factor * fac_l[t, :]
    tiles(rows, tile, l_scale)

    def l_term(db):
        def one(t):
            fac_l[t, :] += (1.0 - decay_factor) * lax.dot_general(
                gbuf[db, t, :], pbuf[db], (((1,), (1,)), ((), ())), preferred_element_type=f32
            )
        tiles(rows, tile, one)
    loop(dp, l_term)
    stores[2].start()
    loop(dp, lambda db: when(lax.div(db, q) != m, lambda: r_send(db).wait_send()))

    def u_near(h, c, xb, sub):
        db = (xb * 2 + 1 - core) * q + sub
        return send(
            ssend.at[db, :, c], urecv.at[0, xb, sub, :, c], us1.at[h, xb, sub], ur1.at[h, xb, sub], (d, partner)
        )

    def u_far(h, c, xb, sub):
        db = (xb * 2 + core) * q + sub
        return send(
            ssend.at[db, :, c], urecv.at[1, chip, sub, :, c], us2.at[h, xb, sub], ur2.at[h, chip, sub],
            (d, xb * 2 + core),
        )

    def u_got(h, c, which, xb, sub):
        dst = urecv.at[which, xb, sub, :, c]
        sem = ur1 if which == 0 else ur2
        send(dst, dst, us1.at[h, 0, 0], sem.at[h, xb, sub], (d, partner)).wait_recv()

    def u_dot(db, c):
        total = None
        for p in range(parts):
            term = jnp.dot(lbuf[p, db], bbuf[pl.ds(p * part, part), c], preferred_element_type=f32)
            total = term if total is None else total + term
        return total

    def u_terms(h, c):
        def near(i):
            xb, sub = lax.rem(chip + 1 + lax.div(i, q), X), lax.rem(i, q)
            db = (xb * 2 + 1 - core) * q + sub
            ssend[db, :, c] = u_dot(db, c).astype(bf16)
            u_near(h, c, xb, sub).start()
        loop(X * q, near)

        def far(i):
            xb, sub = lax.rem(chip + 1 + lax.div(i, q), X), lax.rem(i, q)
            db = (xb * 2 + core) * q + sub
            mine = u_dot(db, c)
            u_got(h, c, 0, xb, sub)
            ssend[db, :, c] = (mine + urecv[0, xb, sub, :, c].astype(f32)).astype(bf16)
            when(xb != chip, lambda: u_far(h, c, xb, sub).start())
        loop(X * q, far)

    def u_final(h, c):
        for sub in range(q):
            for k in range(1, X):
                u_got(h, c, 1, lax.rem(chip + k, X), sub)

            def one(t, sub=sub):
                total = ssend[m * q + sub, t, c].astype(f32)
                for k in range(1, X):
                    total += urecv[1, lax.rem(chip + k, X), sub, t, c].astype(f32)
                where = pl.ds(pl.multiple_of(sub * cols + t.start, 128), 128)
                bout[where, c] = total.astype(bf16)
            tiles(cols, 128, one)

    bout = dbuf
    p = parts - 1
    for h, piece in enumerate(pieces[p]):
        c = pl.ds(piece[1], piece[2])
        i = first_piece[p] + h
        by_distance(lambda zb, i=i, piece=piece: line(i, piece, zb), far_first=True)
        u_terms(h, c)
    for h, piece in enumerate(pieces[p]):
        u_final(h, pl.ds(piece[1], piece[2]))
    stores[4].start()

    for a in range(2 + parts):
        def sent(i, a=a):
            when(jnp.logical_and(z < last, i <= z), lambda: up(a, i).wait_send())
            when(jnp.logical_and(z > 0, i >= z), lambda: dn(a, i).wait_send())
            y_sends(a, i, lambda c: c.wait_send())
        loop(Z, sent)
        when(z > 0, lambda a=a: extra(a, 1).wait_send())
        when(z < last, lambda a=a: extra(a, 0).wait_send())
    mp_sent(0, rbuf)
    mp_sent(1, rrbuf)

    def near_sent():
        to_chips(lambda c: c.wait_send())
    when(chip == own_chip, near_sent)

    def own_sent():
        for hb in range(2):
            p_send(hb, hb, partner).wait_send()
    when(m == owner, own_sent)
    when(chip != own_chip, lambda: p_send(core, 0, partner).wait_send())
    y_scattered(parts - 1)
    for p in range(parts):
        for i, piece in enumerate(pieces[p], first_piece[p]):
            loop(Z, lambda zb, i=i, piece=piece: when(zb != z, lambda: bz_up(i, piece, zb).wait_send()))
    for h, piece in enumerate(pieces[parts - 1]):
        c = pl.ds(piece[1], piece[2])
        for sub in range(q):
            for xb in range(X):
                u_near(h, c, xb, sub).wait_send()
                when(xb != chip, lambda h=h, c=c, xb=xb, sub=sub: u_far(h, c, xb, sub).wait_send())
    for c in stores:
        c.wait()


def solution(mesh):
    dp, mp = mesh.shape["dp"], mesh.shape["mp"]
    Z, X = dp // 2, mp // 2

    def per_device(*args):
        _, rows, cols = args[0].shape
        q = rows // cols
        parts = min(PARTS, rows // 128)
        last_chunks = min(LAST, cols // 128)
        part, pieces = rows // parts, parts - 1 + last_chunks
        flat = [a.reshape(a.shape[1:]) for a in args]
        dma = pltpu.SemaphoreType.DMA
        outs = pl.pallas_call(
            functools.partial(kernel, dp, mp, rows, cols, parts, last_chunks),
            out_shape=[jax.ShapeDtypeStruct((rows, cols), t) for t in (f32, f32, f32, f32, bf16)],
            in_specs=[pl.BlockSpec(memory_space=pl.ANY)] * 7,
            out_specs=[pl.BlockSpec(memory_space=pl.ANY)] * 5,
            scratch_shapes=[
                pltpu.VMEM((dp, rows, cols), bf16),
                pltpu.VMEM((parts, dp, cols, part), bf16),
                pltpu.VMEM((mp, rows, cols), bf16),
                pltpu.VMEM((mp, rows, cols), bf16),
                pltpu.VMEM((dp, cols, cols), bf16),
                pltpu.VMEM((dp, cols, cols), bf16),
                pltpu.VMEM((mp, q, cols, cols), bf16),
                pltpu.VMEM((2, X, q, cols, cols), bf16),
                pltpu.VMEM((Z, part, cols), bf16),
                pltpu.VMEM((parts, Z, part, cols), bf16),
                pltpu.VMEM((parts, Z + 1, part, cols), bf16),
                pltpu.VMEM((rows, cols), f32),
                pltpu.VMEM((rows, cols), f32),
                pltpu.VMEM((rows, cols), f32),
                pltpu.VMEM((rows, cols), f32),
                pltpu.VMEM((rows, cols), f32),
                pltpu.VMEM((rows, cols), bf16),
                pltpu.VMEM((rows, cols), bf16),
                dma((6 + parts,)),
                dma((5,)),
                dma((2 + parts, Z)),
                dma((2 + parts, Z)),
                dma((2 + parts, Z)),
                dma((2 + parts, Z, 2)),
                dma((2 + parts, Z, 2)),
                dma((2 + parts, 2)),
                dma((2 + parts, 2)),
                dma((2, 2 * X)),
                dma((2, mp)),
                dma((dp,)),
                dma((mp, q)),
                dma((last_chunks, X, q)),
                dma((last_chunks, X, q)),
                dma((last_chunks, X, q)),
                dma((last_chunks, X, q)),
                dma((2 + X,)),
                dma((2,)),
                dma((pieces, Z)),
                dma((pieces, Z)),
                dma((pieces, Z)),
                dma((pieces, Z + 1)),
            ],
            compiler_params=pltpu.CompilerParams(
                collective_id=0, has_side_effects=True, vmem_limit_bytes=67043328
            ),
        )(*flat)
        return tuple(o.reshape((1,) + o.shape) for o in outs)

    return jax.shard_map(
        per_device,
        mesh=mesh,
        in_specs=(P(None, "mp", "dp"),) * 5 + (P(None, "dp", "mp"), P(None, "mp", "dp")),
        out_specs=(P(None, "mp", "dp"),) * 5,
        check_vma=False,
    )
```

```python
import functools

import jax
import jax.numpy as jnp
from jax import lax
from jax.experimental import pallas as pl
from jax.experimental.pallas import tpu as pltpu
from jax.sharding import PartitionSpec as P

decay_moment = 0.95
decay_factor = 0.95
epsilon = 1e-08
bf16, f32 = jnp.bfloat16, jnp.float32
MESH = pl.DeviceIdType.MESH
PARTS, LAST = 2, 4
Y_FIRST, Z_FIRST = 0, 1


def scatter_pieces(rows, cols, parts, last_chunks):
    part = rows // parts
    out = [[] for _ in range(parts)]
    for p in range(parts - 1):
        out[p].append((p, 0, part // 2, 0, cols, Z_FIRST))
        out[p].append((p, part // 2, part // 2, 0, cols, Y_FIRST))
    for h in range(last_chunks):
        cw = cols // last_chunks
        out[parts - 1].append((parts - 1, 0, part, h * cw, cw, Y_FIRST))
    return out


def kernel(dp, mp, rows, cols, parts, last_chunks, *refs):
    pieces = scatter_pieces(rows, cols, parts, last_chunks)
    first_piece = [sum(len(x) for x in pieces[:p]) for p in range(parts)]
    n_pieces = sum(len(x) for x in pieces)
    (grad, first, second, left_f, right_f, left_b, right_b,
     out_first, out_second, out_left, out_right, out_update,
     gbuf, lbuf, rbuf, rrbuf, pbuf, ssend, r1buf, r2buf, u1buf, u2buf,
     fac, mom1, mom2, acc, dbuf, bbuf,
     load_sem, store_sem, zs_up, zs_dn, zr, ys, yr, es, er, as_, ar,
     rs1, rr1, rs2, rr2, us1, ur1, us2, ur2, ps, pr, bys, byr, bzs, bzr) = refs[:53]
    out_bufs = refs[53:53 + n_pieces]
    y_bufs = refs[53 + n_pieces:53 + 2 * n_pieces]
    z_bufs = refs[53 + 2 * n_pieces:]
    Z, q, X = dp // 2, rows // cols, mp // 2
    part, cw = rows // parts, cols // last_chunks
    d, m = lax.axis_index("dp"), lax.axis_index("mp")
    z, y = lax.div(d, 2), lax.rem(d, 2)
    core, chip = lax.rem(m, 2), lax.div(m, 2)
    partner = chip * 2 + (1 - core)
    last = Z - 1
    ynbr = z * 2 + (1 - y)
    tile = min(256, part)

    def send(src, dst, s, r, dev):
        return pltpu.make_async_remote_copy(
            src_ref=src, dst_ref=dst, send_sem=s, recv_sem=r, device_id=dev, device_id_type=MESH
        )

    def when(cond, fn):
        pl.when(cond)(fn)

    def loop(n, fn):
        def body(i, c):
            fn(i)
            return c
        lax.fori_loop(0, n, body, 0)

    def tiles(n, size, fn, base=0):
        loop(n // size, lambda i: fn(pl.ds(pl.multiple_of(base + i * size, size), size)))

    loads = [
        (grad, gbuf.at[d]), (right_b, rbuf.at[m]), (right_f, fac),
    ]
    loads += [(left_b.at[:, pl.ds(p * part, part)], lbuf.at[p, d]) for p in range(parts)]
    load = [pltpu.make_async_copy(a, b, load_sem.at[i]) for i, (a, b) in enumerate(loads)]
    for c in load:
        c.start()

    def part_rows(ref, p):
        return ref.at[pl.ds(p * part, part), :]

    def mom_loads(p):
        n = 4 + parts + 2 * p
        return [
            pltpu.make_async_copy(part_rows(a, p), b, load_sem.at[n + i])
            for i, (a, b) in enumerate([(first, mom1), (second, mom2)])
        ]

    def mom_stores(p):
        return [
            pltpu.make_async_copy(b, part_rows(a, p), store_sem.at[3 + 2 * p + i])
            for i, (a, b) in enumerate([(out_first, mom1), (out_second, mom2)])
        ]

    load_left = pltpu.make_async_copy(left_f, fac, load_sem.at[3 + parts])
    store_right = pltpu.make_async_copy(fac, out_right, store_sem.at[0])
    store_left = pltpu.make_async_copy(fac, out_left, store_sem.at[1])
    store_update = pltpu.make_async_copy(dbuf, out_update, store_sem.at[2])
    for c in mom_loads(0):
        c.start()

    barrier = pltpu.get_barrier_semaphore()
    pl.semaphore_signal(barrier, inc=1, device_id=(ynbr, m), device_id_type=MESH)
    when(z > 0, lambda: pl.semaphore_signal(barrier, inc=1, device_id=(d - 2, m), device_id_type=MESH))
    when(z < last, lambda: pl.semaphore_signal(barrier, inc=1, device_id=(d + 2, m), device_id_type=MESH))
    for k in range(1, mp):
        pl.semaphore_signal(barrier, inc=1, device_id=(d, lax.rem(m + k, mp)), device_id_type=MESH)
    along = (z > 0).astype(jnp.int32) + (z < last).astype(jnp.int32)
    pl.semaphore_wait(barrier, mp + along)

    def view(a, b):
        if a < 2:
            return gbuf.at[b, pl.ds(a * (rows // 2), rows // 2), :]
        return lbuf.at[a - 2, b]

    def half(a, b, hb):
        if a < 2:
            return gbuf.at[b, pl.ds(a * (rows // 2) + hb * (rows // 4), rows // 4), :]
        return lbuf.at[a - 2, b, pl.ds(hb * (cols // 2), cols // 2), :]

    def up(a, zb):
        blk = view(a, zb * 2 + y)
        return send(blk, blk, zs_up.at[a, zb], zr.at[a, zb], (d + 2, m))

    def dn(a, zb):
        blk = view(a, zb * 2 + y)
        return send(blk, blk, zs_dn.at[a, zb], zr.at[a, zb], (d - 2, m))

    def ysend(a, zb, hb):
        blk = half(a, zb * 2 + y, hb)
        return send(blk, blk, ys.at[a, zb, hb], yr.at[a, zb, hb], (ynbr, m))

    def yrecv_desc(a, zb, hb):
        blk = half(a, zb * 2 + (1 - y), hb)
        return send(blk, blk, ys.at[a, zb, hb], yr.at[a, zb, hb], (ynbr, m))

    def extra(a, k):
        zb = 0 if k == 0 else last
        blk = half(a, zb * 2 + (1 - y), 1)
        return send(blk, blk, es.at[a, k], er.at[a, k], (d + 2, m) if k == 0 else (d - 2, m))

    def y_second(zb):
        inner = jnp.logical_and(zb > 0, zb < last)
        return jnp.logical_or(zb == z, inner)

    def y_sends(a, zb, op):
        when(y_second(zb), lambda: op(ysend(a, zb, 1)))
        op(ysend(a, zb, 0))

    def start(c):
        c.start()

    def ag_own(a):
        when(z < last, lambda: up(a, z).start())
        when(z > 0, lambda: dn(a, z).start())

    def ag_step(a, s, then=None):
        below, above = z - s, z + s

        def from_below():
            up(a, below).wait_recv()
            when(z < last, lambda: up(a, below).start())

        def from_above():
            dn(a, above).wait_recv()
            when(z > 0, lambda: dn(a, above).start())

        when(below >= 0, from_below)
        when(above <= last, from_above)
        when(below >= 0, lambda: y_sends(a, below, start))
        when(above <= last, lambda: y_sends(a, above, start))

        def extra_dn():
            when(z == last, lambda: yrecv_desc(a, z, 1).wait_recv())
            when(z < last, lambda: extra(a, 1).wait_recv())
            extra(a, 1).start()
            if then is not None:
                dn(then, z).start()

        def extra_up():
            when(z == 0, lambda: yrecv_desc(a, z, 1).wait_recv())
            when(z > 0, lambda: extra(a, 0).wait_recv())
            extra(a, 0).start()
            if then is not None:
                up(then, z).start()

        when(jnp.logical_and(z == Z - s, z > 0), extra_dn)
        when(jnp.logical_and(z == s - 1, z < last), extra_up)

    def wait_y(a, zb):
        yrecv_desc(a, zb, 0).wait_recv()
        inner = jnp.logical_and(zb > 0, zb < last)
        when(inner, lambda: yrecv_desc(a, zb, 1).wait_recv())
        when(jnp.logical_and(zb == last, z == 0), lambda: extra(a, 1).wait_recv())
        when(jnp.logical_and(zb == 0, z == last), lambda: extra(a, 0).wait_recv())

    def at_distance(s, fn):
        when(z - s >= 0, lambda: fn(z - s))
        when(jnp.logical_and(s > 0, z + s <= last), lambda: fn(z + s))

    def by_distance(fn, far_first=False):
        loop(Z, lambda i: at_distance(last - i if far_first else i, fn))

    def sub_rows(ref, db):
        off = pl.multiple_of(lax.rem(db, q) * cols, cols)
        return ref.at[lax.div(db, q), pl.ds(off, cols), :]

    def mp_copy(a, buf, src, k, to):
        return send(buf.at[src], buf.at[src], as_.at[a, k], ar.at[a, src], (d, to))

    def mp_first(a, buf, op):
        for k in range(1, X):
            op(mp_copy(a, buf, m, X + k, lax.rem(chip + k, X) * 2 + core))
        op(mp_copy(a, buf, m, 0, partner))

    def mp_relay(a, buf):
        for k in range(1, X):
            src = lax.rem(chip + k, X) * 2 + core
            mp_copy(a, buf, src, k, partner).wait_recv()
            mp_copy(a, buf, src, k, partner).start()

    def mp_wait(a, buf):
        for k in range(X):
            src = lax.rem(chip + k, X) * 2 + 1 - core
            mp_copy(a, buf, src, k, partner).wait_recv()

    def mp_sent(a, buf):
        mp_first(a, buf, lambda c: c.wait_send())
        for k in range(1, X):
            mp_copy(a, buf, lax.rem(chip + k, X) * 2 + core, k, partner).wait_send()

    load[0].wait()
    for a in range(2):
        ag_own(a)
        y_sends(a, z, start)
    load[1].wait()
    mp_first(0, rbuf, start)
    for p in range(parts):
        load[3 + p].wait()

    def far_slot(k):
        return lax.rem(k + X, X) - 1

    def r_near(db):
        xb, sub = lax.div(db, 2 * q), lax.rem(db, q)
        return send(ssend.at[:, db], r1buf.at[:, xb, sub], rs1.at[xb, sub], rr1.at[xb, sub], (d, partner))

    def r_far(db):
        xb, sub = lax.div(db, 2 * q), lax.rem(db, q)
        slot = far_slot(chip - xb)
        return send(ssend.at[:, db], r2buf.at[:, slot, sub], rs2.at[xb, sub], rr2.at[slot, sub], (d, xb * 2 + core))

    def r_term(db):
        xb, sub = lax.div(db, 2 * q), lax.rem(db, q)
        mine = lax.rem(lax.div(db, q), 2) == core

        def one(t):
            term = lax.dot_general(
                gbuf[db, :, t], gbuf[d], (((0,), (0,)), ((), ())), preferred_element_type=f32
            )
            for h in range(last_chunks):
                ssend[h, db, t, :] = term[:, h * cw:(h + 1) * cw].astype(bf16)
        tiles(cols, min(256, cols), one)

        def add():
            got = r1buf.at[:, xb, sub]
            send(got, got, rs1.at[0, 0], rr1.at[xb, sub], (d, partner)).wait_recv()
            for h in range(last_chunks):
                ssend[h, db] = (ssend[h, db].astype(f32) + r1buf[h, xb, sub].astype(f32)).astype(bf16)
            when(xb != chip, lambda: r_far(db).start())
        when(jnp.logical_not(mine), lambda: r_near(db).start())
        when(mine, add)

    def rr_term(db):
        rhs = sub_rows(rbuf, db)
        def one(t):
            acc[t, :] += jnp.dot(gbuf[db, t, :], rhs[...], preferred_element_type=f32)
        tiles(rows, tile, one)

    def zero_acc():
        def one(t):
            acc[t, :] = jnp.zeros((tile, cols), f32)
        tiles(rows, tile, one)

    r_term(d)

    def g_step(i):
        s = i + 1
        ag_step(0, s)
        ag_step(1, s, then=2)
        when(s == min(2, last), lambda: mp_relay(0, rbuf))
        at_distance(s, lambda zb: r_term(zb * 2 + y))
    loop(Z - 1, g_step)
    y_sends(2, z, start)
    zero_acc()
    mp_wait(0, rbuf)
    by_distance(lambda zb: rr_term(zb * 2 + y))

    def y_block(zb):
        wait_y(0, zb)
        wait_y(1, zb)
        rr_term(zb * 2 + 1 - y)
    by_distance(y_block)

    def rr_out(t):
        rrbuf[m, t, :] = acc[t, :].astype(bf16)
    tiles(rows, tile, rr_out)
    mp_first(1, rrbuf, start)
    zero_acc()

    owner = lax.div(d, q)
    own_chip = lax.div(owner, 2)
    hd = dp // 2
    pair_off = pl.multiple_of(lax.rem(d, q) * cols, cols)

    def p_send(hb, i, to):
        view_p = pbuf.at[pl.ds(hb * hd, hd)]
        return send(view_p, view_p, ps.at[i], pr.at[hb], (d, to))

    def to_chips(op):
        for k in range(1, X):
            op(p_send(core, 2 + k, lax.rem(chip + k, X) * 2 + core))

    def own_pair():
        def copy(i):
            pbuf[i] = gbuf[i, pl.ds(pair_off, cols), :]
        loop(dp, copy)
        for hb in range(2):
            p_send(hb, hb, partner).start()
        to_chips(start)

    def near_pair():
        for hb in range(2):
            p_send(hb, hb, partner).wait_recv()
        to_chips(start)

    def far_pair():
        p_send(core, 0, partner).wait_recv()
        p_send(core, 0, partner).start()
        p_send(1 - core, 0, partner).wait_recv()

    when(m == owner, own_pair)

    def back_term(db, piece, t):
        p, r0, _, c0, w, _ = piece
        off = pl.multiple_of(lax.rem(db, q) * cols + c0, w)
        rhs = rbuf[lax.div(db, q), pl.ds(off, w), :]
        mine = pl.ds(pl.multiple_of(t.start + (p * part + r0), t.size), t.size)
        return lax.dot_general(
            dbuf[mine, :], rhs, (((1,), (1,)), ((), ())), preferred_element_type=f32
        )

    def piece_tiles(piece, fn):
        tiles(piece[2], min(256, piece[2]), fn)

    def by_send(i, zb):
        return send(out_bufs[i].at[zb], y_bufs[i].at[zb], bys.at[i, zb], byr.at[i, zb], (ynbr, m))

    def by_last(i):
        return send(out_bufs[i].at[z, 1 - y], y_bufs[i], bys.at[i, 0], byr.at[i, 0], (ynbr, m))

    def bz_up(i, zb, src):
        return send(src.at[zb], z_bufs[i].at[zb], bzs.at[i, zb], bzr.at[i, zb], (d + 2, m))

    def bz_dn(i, zb, src):
        slot = jnp.where(zb == z - 1, Z, zb)
        return send(src.at[zb], z_bufs[i].at[slot], bzs.at[i, zb], bzr.at[i, slot], (d - 2, m))

    def z_arrivals(i, zb, add):
        def one(slot):
            dst = z_bufs[i].at[slot]
            send(dst, dst, bzs.at[i, 0], bzr.at[i, slot], (ynbr, m)).wait_recv()
            add(slot)
        when(jnp.logical_and(zb >= z, z > 0), lambda: one(zb))
        when(jnp.logical_and(zb < z, z < last), lambda: one(zb))
        when(jnp.logical_and(zb == z, z < last), lambda: one(Z))

    def z_send(i, zb, src):
        when(zb > z, lambda: bz_up(i, zb, src).start())
        when(zb < z, lambda: bz_dn(i, zb, src).start())

    def to_back(piece, t, value):
        p, r0, _, c0, w, _ = piece
        mine = pl.ds(pl.multiple_of(t.start + (p * part + r0), t.size), t.size)
        bbuf[mine, pl.ds(c0, w)] = value.astype(bf16)

    def line_y_first(i, piece, zb):
        c = pl.ds(0, piece[4])
        by_send(i, zb).wait_recv()

        def one(t):
            acc[t, c] = back_term(zb * 2 + y, piece, t) + y_bufs[i][zb, t, :].astype(f32)
        piece_tiles(piece, one)

        def add(slot):
            def more(t):
                acc[t, c] += z_bufs[i][slot, t, :].astype(f32)
            piece_tiles(piece, more)
        z_arrivals(i, zb, add)

        def pack(t):
            y_bufs[i][zb, t, :] = acc[t, c].astype(bf16)
        when(zb != z, lambda: piece_tiles(piece, pack))
        z_send(i, zb, y_bufs[i])
        when(zb == z, lambda: piece_tiles(piece, lambda t: to_back(piece, t, acc[t, c])))

    def line_z_first(i, piece, zb):
        n = piece[2]

        def rows_of(t, yy):
            return pl.ds(pl.multiple_of(t.start + yy * n, t.size), t.size)
        for yy in range(2):
            def one(t, yy=yy):
                acc[rows_of(t, yy), :] = back_term(zb * 2 + yy, piece, t)
            piece_tiles(piece, one)

        def add(slot):
            for yy in range(2):
                def more(t, yy=yy):
                    acc[rows_of(t, yy), :] += z_bufs[i][slot, yy, t, :].astype(f32)
                piece_tiles(piece, more)
        z_arrivals(i, zb, add)
        for yy in range(2):
            def pack(t, yy=yy):
                out_bufs[i][zb, yy, t, :] = acc[rows_of(t, yy), :].astype(bf16)
            piece_tiles(piece, pack)
        z_send(i, zb, out_bufs[i])
        when(zb == z, lambda: by_last(i).start())

    def finish_z_first(i, piece):
        by_last(i).wait_recv()

        def one(t):
            mine = out_bufs[i][z, y, t, :].astype(f32) + y_bufs[i][t, :].astype(f32)
            to_back(piece, t, mine)
        piece_tiles(piece, one)

    def numbered(p):
        return list(enumerate(pieces[p], first_piece[p]))

    def scatter_first(p):
        for i, piece in numbered(p):
            if piece[5] == Z_FIRST:
                continue

            def one_block(zb, i=i, piece=piece):
                def one(t):
                    out_bufs[i][zb, t, :] = back_term(zb * 2 + 1 - y, piece, t).astype(bf16)
                piece_tiles(piece, one)
                by_send(i, zb).start()
            by_distance(one_block, far_first=True)

    def scatter_step(i, piece, s):
        fn = line_z_first if piece[5] == Z_FIRST else line_y_first
        at_distance(s, lambda zb: fn(i, piece, zb))

    mom_tile = min(128, part)

    def m_term(p, db):
        rhs = sub_rows(rrbuf, db)
        def one(t):
            acc[t, :] += lax.dot_general(
                lbuf[p, db, :, t], rhs[...], (((0,), (0,)), ((), ())), preferred_element_type=f32
            )
        tiles(part, tile, one)

    def zero_part():
        def one(t):
            acc[t, :] = jnp.zeros((tile, cols), f32)
        tiles(part, tile, one)

    def moments(p):
        def one(t):
            w = pl.ds(pl.multiple_of(t.start + p * part, mom_tile), mom_tile)
            rot = acc[t, :]
            new1 = decay_moment * mom1[t, :] + (1.0 - decay_moment) * rot
            new2 = decay_moment * mom2[t, :] + (1.0 - decay_moment) * rot * rot
            mom1[t, :] = new1
            mom2[t, :] = new2
            dbuf[w, :] = (new1 / (jnp.sqrt(new2) + epsilon)).astype(bf16)
        tiles(part, mom_tile, one)

    def direction(p):
        def y_part(zb):
            wait_y(2 + p, zb)
            m_term(p, zb * 2 + 1 - y)
        by_distance(y_part)
        for c in mom_loads(p):
            c.wait()
        moments(p)
        for c in mom_stores(p):
            c.start()

    by_distance(lambda zb: r_term(zb * 2 + 1 - y))

    def l_step(i):
        s = i + 1
        when(s == last, lambda: mp_relay(1, rrbuf))
        ag_step(2, s, then=3 if parts > 1 else None)
        when(jnp.logical_and(s == min(2, last), jnp.logical_and(chip == own_chip, m != owner)), near_pair)
    loop(Z - 1, l_step)
    if parts > 1:
        y_sends(3, z, start)
    mp_wait(1, rrbuf)
    by_distance(lambda zb: m_term(0, zb * 2 + y))
    direction(0)
    scatter_first(0)

    def r_final():
        for sub in range(q):
            for k in range(1, X):
                got = r2buf.at[:, k - 1, sub]
                send(got, got, rs1.at[0, 0], rr2.at[k - 1, sub], (d, partner)).wait_recv()
            for h in range(last_chunks):
                def one(t, sub=sub, h=h):
                    total = ssend[h, m * q + sub, t, :].astype(f32)
                    for k in range(1, X):
                        total += r2buf[h, k - 1, sub, t, :].astype(f32)
                    where = pl.ds(pl.multiple_of(sub * cols + t.start, 128), 128)
                    c = pl.ds(h * cw, cw)
                    fac[where, c] = decay_factor * fac[where, c] + (1.0 - decay_factor) * total
                tiles(cols, 128, one)
    load[2].wait()
    r_final()
    store_right.start()

    def l_term(db):
        def one(t):
            fac[t, :] += (1.0 - decay_factor) * lax.dot_general(
                gbuf[db, t, :], pbuf[db], (((1,), (1,)), ((), ())), preferred_element_type=f32
            )
        tiles(rows, tile, one)

    for p in range(1, parts):
        def both(i, p=p):
            s = i + 1
            ag_step(2 + p, s, then=3 + p if p + 1 < parts else None)
            for j, piece in numbered(p - 1):
                scatter_step(j, piece, Z - s)
        loop(Z - 1, both)
        if p + 1 < parts:
            y_sends(3 + p, z, start)
        for j, piece in numbered(p - 1):
            scatter_step(j, piece, 0)
        zero_part()
        for c in mom_stores(p - 1):
            c.wait()
        for c in mom_loads(p):
            c.start()
        if p == 1:
            store_right.wait()
            load_left.start()
        by_distance(lambda zb, p=p: m_term(p, zb * 2 + y))
        direction(p)
        scatter_first(p)
        for j, piece in numbered(p - 1):
            if piece[5] == Z_FIRST:
                finish_z_first(j, piece)

    when(chip != own_chip, far_pair)
    load_left.wait()

    def l_scale(t):
        fac[t, :] = decay_factor * fac[t, :]
    tiles(rows, tile, l_scale)

    def r_sent(db):
        mine = lax.rem(lax.div(db, q), 2) == core
        when(jnp.logical_not(mine), lambda: r_near(db).wait_send())
        when(jnp.logical_and(mine, lax.div(db, 2 * q) != chip), lambda: r_far(db).wait_send())
    loop(dp, r_sent)

    def u_near(h, xb, sub):
        db = (xb * 2 + 1 - core) * q + sub
        return send(
            ssend.at[h, db], u1buf.at[h, xb, sub], us1.at[h, xb, sub], ur1.at[h, xb, sub], (d, partner)
        )

    def u_far(h, xb, sub):
        db = (xb * 2 + core) * q + sub
        slot = far_slot(chip - xb)
        return send(
            ssend.at[h, db], u2buf.at[h, slot, sub], us2.at[h, xb, sub], ur2.at[h, slot, sub], (d, xb * 2 + core)
        )

    def u_got(dst, sem):
        send(dst, dst, us1.at[0, 0, 0], sem, (d, partner)).wait_recv()

    def u_dot(h, db):
        c = pl.ds(h * cw, cw)
        total = None
        for p in range(parts):
            term = jnp.dot(lbuf[p, db], bbuf[pl.ds(p * part, part), c], preferred_element_type=f32)
            total = term if total is None else total + term
        return total

    def u_terms(h):
        def near(i):
            xb, sub = lax.rem(chip + 1 + lax.div(i, q), X), lax.rem(i, q)
            db = (xb * 2 + 1 - core) * q + sub
            ssend[h, db] = u_dot(h, db).astype(bf16)
            u_near(h, xb, sub).start()
        loop(X * q, near)

        def far(i):
            xb, sub = lax.rem(chip + 1 + lax.div(i, q), X), lax.rem(i, q)
            db = (xb * 2 + core) * q + sub
            mine = u_dot(h, db)
            u_got(u1buf.at[h, xb, sub], ur1.at[h, xb, sub])
            ssend[h, db] = (mine + u1buf[h, xb, sub].astype(f32)).astype(bf16)
            when(xb != chip, lambda: u_far(h, xb, sub).start())
        loop(X * q, far)

    def u_final(h):
        c = pl.ds(h * cw, cw)
        for sub in range(q):
            for k in range(1, X):
                u_got(u2buf.at[h, k - 1, sub], ur2.at[h, k - 1, sub])

            def one(t, sub=sub):
                total = ssend[h, m * q + sub, t, :].astype(f32)
                for k in range(1, X):
                    total += u2buf[h, k - 1, sub, t, :].astype(f32)
                where = pl.ds(pl.multiple_of(sub * cols + t.start, 128), 128)
                dbuf[where, c] = total.astype(bf16)
            tiles(cols, 128, one)

    done = 0
    for tau in range(last_chunks + Z - 1):
        for h, (i, piece) in enumerate(numbered(parts - 1)):
            if 0 <= tau - h <= last:
                scatter_step(i, piece, last - (tau - h))
                if tau - h == last:
                    u_terms(h)
        per = -(-dp // (last_chunks + Z - 2))
        for db in range(done, min(done + per, dp)):
            l_term(db)
        done = min(done + per, dp)
        if tau * per < dp <= (tau + 1) * per:
            store_left.start()
    for h in range(last_chunks):
        u_final(h)
    store_update.start()

    for a in range(2 + parts):
        def sent(i, a=a):
            when(jnp.logical_and(z < last, i <= z), lambda: up(a, i).wait_send())
            when(jnp.logical_and(z > 0, i >= z), lambda: dn(a, i).wait_send())
            y_sends(a, i, lambda c: c.wait_send())
        loop(Z, sent)
        when(z > 0, lambda a=a: extra(a, 1).wait_send())
        when(z < last, lambda a=a: extra(a, 0).wait_send())
    mp_sent(0, rbuf)
    mp_sent(1, rrbuf)

    def near_sent():
        to_chips(lambda c: c.wait_send())
    when(chip == own_chip, near_sent)

    def own_sent():
        for hb in range(2):
            p_send(hb, hb, partner).wait_send()
    when(m == owner, own_sent)
    when(chip != own_chip, lambda: p_send(core, 0, partner).wait_send())
    def line_sent(i, piece):
        src = out_bufs[i] if piece[5] == Z_FIRST else y_bufs[i]

        def one(zb):
            if piece[5] == Y_FIRST:
                by_send(i, zb).wait_send()
            when(zb != z, lambda: bz_up(i, zb, src).wait_send())
        loop(Z, one)
        if piece[5] == Z_FIRST:
            by_last(i).wait_send()
    for p in range(parts):
        for i, piece in numbered(p):
            line_sent(i, piece)
    for h in range(last_chunks):
        for sub in range(q):
            for xb in range(X):
                u_near(h, xb, sub).wait_send()
                when(xb != chip, lambda h=h, xb=xb, sub=sub: u_far(h, xb, sub).wait_send())
    for c in mom_stores(parts - 1) + [store_left, store_update]:
        c.wait()


def solution(mesh):
    dp, mp = mesh.shape["dp"], mesh.shape["mp"]
    Z, X = dp // 2, mp // 2

    def per_device(*args):
        _, rows, cols = args[0].shape
        q = rows // cols
        parts = min(PARTS, rows // 128)
        last_chunks = min(LAST, cols // 128)
        part, cw = rows // parts, cols // last_chunks
        pieces = sum(scatter_pieces(rows, cols, parts, last_chunks), [])
        n = len(pieces)
        out_b, y_b, z_b = [], [], []
        for _, _, nr, _, w, kind in pieces:
            lead = (2,) if kind == Z_FIRST else ()
            out_b.append(pltpu.VMEM((Z,) + lead + (nr, w), bf16))
            y_b.append(pltpu.VMEM((nr, w) if lead else (Z, nr, w), bf16))
            z_b.append(pltpu.VMEM((Z + 1,) + lead + (nr, w), bf16))
        flat = [a.reshape(a.shape[1:]) for a in args]
        dma = pltpu.SemaphoreType.DMA
        outs = pl.pallas_call(
            functools.partial(kernel, dp, mp, rows, cols, parts, last_chunks),
            out_shape=[jax.ShapeDtypeStruct((rows, cols), t) for t in (f32, f32, f32, f32, bf16)],
            in_specs=[pl.BlockSpec(memory_space=pl.ANY)] * 7,
            out_specs=[pl.BlockSpec(memory_space=pl.ANY)] * 5,
            scratch_shapes=[
                pltpu.VMEM((dp, rows, cols), bf16),
                pltpu.VMEM((parts, dp, cols, part), bf16),
                pltpu.VMEM((mp, rows, cols), bf16),
                pltpu.VMEM((mp, rows, cols), bf16),
                pltpu.VMEM((dp, cols, cols), bf16),
                pltpu.VMEM((last_chunks, dp, cols, cw), bf16),
                pltpu.VMEM((last_chunks, X, q, cols, cw), bf16),
                pltpu.VMEM((last_chunks, X - 1, q, cols, cw), bf16),
                pltpu.VMEM((last_chunks, X, q, cols, cw), bf16),
                pltpu.VMEM((last_chunks, X - 1, q, cols, cw), bf16),
                pltpu.VMEM((rows, cols), f32),
                pltpu.VMEM((part, cols), f32),
                pltpu.VMEM((part, cols), f32),
                pltpu.VMEM((rows, cols), f32),
                pltpu.VMEM((rows, cols), bf16),
                pltpu.VMEM((rows, cols), bf16),
                dma((4 + 3 * parts,)),
                dma((3 + 2 * parts,)),
                dma((2 + parts, Z)),
                dma((2 + parts, Z)),
                dma((2 + parts, Z)),
                dma((2 + parts, Z, 2)),
                dma((2 + parts, Z, 2)),
                dma((2 + parts, 2)),
                dma((2 + parts, 2)),
                dma((2, 2 * X)),
                dma((2, mp)),
                dma((X, q)),
                dma((X, q)),
                dma((X, q)),
                dma((X - 1, q)),
                dma((last_chunks, X, q)),
                dma((last_chunks, X, q)),
                dma((last_chunks, X, q)),
                dma((last_chunks, X - 1, q)),
                dma((2 + X,)),
                dma((2,)),
                dma((n, Z)),
                dma((n, Z)),
                dma((n, Z)),
                dma((n, Z + 1)),
            ] + out_b + y_b + z_b,
            compiler_params=pltpu.CompilerParams(
                collective_id=0, has_side_effects=True, vmem_limit_bytes=67043328
            ),
        )(*flat)
        return tuple(o.reshape((1,) + o.shape) for o in outs)

    return jax.shard_map(
        per_device,
        mesh=mesh,
        in_specs=(P(None, "mp", "dp"),) * 5 + (P(None, "dp", "mp"), P(None, "mp", "dp")),
        out_specs=(P(None, "mp", "dp"),) * 5,
        check_vma=False,
    )
```

```python
import functools

import jax
import jax.numpy as jnp
from jax import lax
from jax.experimental import pallas as pl
from jax.experimental.pallas import tpu as pltpu
from jax.sharding import PartitionSpec as P

decay_moment = 0.95
decay_factor = 0.95
epsilon = 1e-08
bf16, f32 = jnp.bfloat16, jnp.float32
MESH = pl.DeviceIdType.MESH
PARTS, LAST, LAST_Z, EARLY = 2, 4, 1, 4
Y_FIRST, Z_FIRST = 0, 1


def scatter_pieces(rows, cols, parts, last_chunks):
    part = rows // parts
    out = [[] for _ in range(parts)]
    for p in range(parts - 1):
        out[p].append((p, 0, part // 2, 0, cols, Z_FIRST))
        out[p].append((p, part // 2, part // 2, 0, cols, Y_FIRST))
    for h in range(last_chunks):
        cw = cols // last_chunks
        out[parts - 1].append((parts - 1, 0, part, h * cw, cw, Z_FIRST if h < LAST_Z else Y_FIRST))
    return out


def kernel(dp, mp, rows, cols, parts, last_chunks, *refs):
    pieces = scatter_pieces(rows, cols, parts, last_chunks)
    first_piece = [sum(len(x) for x in pieces[:p]) for p in range(parts)]
    n_pieces = sum(len(x) for x in pieces)
    NAMED = len(refs) - 3 * n_pieces
    (grad, first, second, left_f, right_f, left_b, right_b,
     out_first, out_second, out_left, out_right, out_update,
     gbuf, lbuf, rbuf, rrbuf, pbuf, ssend, r1buf, r2buf, u2buf,
     fac_l, fac_r, mom1, mom2, acc, dbuf, bbuf,
     load_sem, store_sem, zs_up, zs_dn, zr, ys, yr, es, er, as_, ar,
     rs1, rr1, rs2, rr2, us1, ur1, us2, ur2, ps, pr, bys, byr, bzs, bzr) = refs[:NAMED]
    out_bufs = refs[NAMED:NAMED + n_pieces]
    y_bufs = refs[NAMED + n_pieces:NAMED + 2 * n_pieces]
    z_bufs = refs[NAMED + 2 * n_pieces:]
    u1buf = r1buf
    Z, q, X = dp // 2, rows // cols, mp // 2
    part, cw = rows // parts, cols // last_chunks
    d, m = lax.axis_index("dp"), lax.axis_index("mp")
    z, y = lax.div(d, 2), lax.rem(d, 2)
    core, chip = lax.rem(m, 2), lax.div(m, 2)
    partner = chip * 2 + (1 - core)
    last = Z - 1
    ynbr = z * 2 + (1 - y)
    tile = min(256, part)

    def send(src, dst, s, r, dev):
        return pltpu.make_async_remote_copy(
            src_ref=src, dst_ref=dst, send_sem=s, recv_sem=r, device_id=dev, device_id_type=MESH
        )

    def when(cond, fn):
        pl.when(cond)(fn)

    def loop(n, fn):
        def body(i, c):
            fn(i)
            return c
        lax.fori_loop(0, n, body, 0)

    def tiles(n, size, fn, base=0):
        loop(n // size, lambda i: fn(pl.ds(pl.multiple_of(base + i * size, size), size)))

    loads = [
        (grad, gbuf.at[d]), (right_b, rbuf.at[m]), (right_f, fac_r), (left_f, fac_l),
    ]
    loads += [(left_b.at[:, pl.ds(p * part, part)], lbuf.at[p, d]) for p in range(parts)]
    load = [pltpu.make_async_copy(a, b, load_sem.at[i]) for i, (a, b) in enumerate(loads)]
    for c in load:
        c.start()

    def part_rows(ref, p):
        return ref.at[pl.ds(p * part, part), :]

    def mom_loads(p):
        n = 4 + parts + 2 * p
        return [
            pltpu.make_async_copy(part_rows(a, p), b, load_sem.at[n + i])
            for i, (a, b) in enumerate([(first, mom1), (second, mom2)])
        ]

    def mom_stores(p):
        return [
            pltpu.make_async_copy(b, part_rows(a, p), store_sem.at[3 + 2 * p + i])
            for i, (a, b) in enumerate([(out_first, mom1), (out_second, mom2)])
        ]

    store_right = pltpu.make_async_copy(fac_r, out_right, store_sem.at[0])
    store_left = pltpu.make_async_copy(fac_l, out_left, store_sem.at[1])
    store_update = pltpu.make_async_copy(dbuf, out_update, store_sem.at[2])
    for c in mom_loads(0):
        c.start()

    barrier = pltpu.get_barrier_semaphore()
    pl.semaphore_signal(barrier, inc=1, device_id=(ynbr, m), device_id_type=MESH)
    when(z > 0, lambda: pl.semaphore_signal(barrier, inc=1, device_id=(d - 2, m), device_id_type=MESH))
    when(z < last, lambda: pl.semaphore_signal(barrier, inc=1, device_id=(d + 2, m), device_id_type=MESH))
    for k in range(1, mp):
        pl.semaphore_signal(barrier, inc=1, device_id=(d, lax.rem(m + k, mp)), device_id_type=MESH)
    along = (z > 0).astype(jnp.int32) + (z < last).astype(jnp.int32)
    pl.semaphore_wait(barrier, mp + along)

    def view(a, b):
        if a < 2:
            return gbuf.at[b, pl.ds(a * (rows // 2), rows // 2), :]
        return lbuf.at[a - 2, b]

    def half(a, b, hb):
        if a < 2:
            return gbuf.at[b, pl.ds(a * (rows // 2) + hb * (rows // 4), rows // 4), :]
        return lbuf.at[a - 2, b, pl.ds(hb * (cols // 2), cols // 2), :]

    def up(a, zb):
        blk = view(a, zb * 2 + y)
        return send(blk, blk, zs_up.at[a, zb], zr.at[a, zb], (d + 2, m))

    def dn(a, zb):
        blk = view(a, zb * 2 + y)
        return send(blk, blk, zs_dn.at[a, zb], zr.at[a, zb], (d - 2, m))

    def ysend(a, zb, hb):
        blk = half(a, zb * 2 + y, hb)
        return send(blk, blk, ys.at[a, zb, hb], yr.at[a, zb, hb], (ynbr, m))

    def yrecv_desc(a, zb, hb):
        blk = half(a, zb * 2 + (1 - y), hb)
        return send(blk, blk, ys.at[a, zb, hb], yr.at[a, zb, hb], (ynbr, m))

    def extra(a, k):
        zb = 0 if k == 0 else last
        blk = half(a, zb * 2 + (1 - y), 1)
        return send(blk, blk, es.at[a, k], er.at[a, k], (d + 2, m) if k == 0 else (d - 2, m))

    def y_second(zb):
        inner = jnp.logical_and(zb > 0, zb < last)
        return jnp.logical_or(zb == z, inner)

    def y_sends(a, zb, op):
        when(y_second(zb), lambda: op(ysend(a, zb, 1)))
        op(ysend(a, zb, 0))

    def start(c):
        c.start()

    def ag_own(a):
        when(z < last, lambda: up(a, z).start())
        when(z > 0, lambda: dn(a, z).start())

    def ag_step(a, s, then=None):
        below, above = z - s, z + s

        def from_below():
            up(a, below).wait_recv()
            when(z < last, lambda: up(a, below).start())

        def from_above():
            dn(a, above).wait_recv()
            when(z > 0, lambda: dn(a, above).start())

        when(below >= 0, from_below)
        when(above <= last, from_above)
        when(below >= 0, lambda: y_sends(a, below, start))
        when(above <= last, lambda: y_sends(a, above, start))

        def extra_dn():
            when(z == last, lambda: yrecv_desc(a, z, 1).wait_recv())
            when(z < last, lambda: extra(a, 1).wait_recv())
            extra(a, 1).start()
            if then is not None:
                dn(then, z).start()

        def extra_up():
            when(z == 0, lambda: yrecv_desc(a, z, 1).wait_recv())
            when(z > 0, lambda: extra(a, 0).wait_recv())
            extra(a, 0).start()
            if then is not None:
                up(then, z).start()

        when(jnp.logical_and(z == Z - s, z > 0), extra_dn)
        when(jnp.logical_and(z == s - 1, z < last), extra_up)

    def wait_y(a, zb):
        yrecv_desc(a, zb, 0).wait_recv()
        inner = jnp.logical_and(zb > 0, zb < last)
        when(inner, lambda: yrecv_desc(a, zb, 1).wait_recv())
        when(jnp.logical_and(zb == last, z == 0), lambda: extra(a, 1).wait_recv())
        when(jnp.logical_and(zb == 0, z == last), lambda: extra(a, 0).wait_recv())

    def at_distance(s, fn):
        def side(j):
            zb = z + (2 * j - 1) * s
            ok = jnp.logical_and(zb >= 0, zb <= last)
            when(jnp.logical_and(ok, jnp.logical_or(s > 0, j == 0)), lambda: fn(zb))
        loop(2, side)

    def by_distance(fn, far_first=False):
        loop(Z, lambda i: at_distance(last - i if far_first else i, fn))

    def sub_rows(ref, db):
        off = pl.multiple_of(lax.rem(db, q) * cols, cols)
        return ref.at[lax.div(db, q), pl.ds(off, cols), :]

    def mp_copy(a, buf, src, k, to):
        return send(buf.at[src], buf.at[src], as_.at[a, k], ar.at[a, src], (d, to))

    def mp_first(a, buf, op):
        for k in range(1, X):
            op(mp_copy(a, buf, m, X + k, lax.rem(chip + k, X) * 2 + core))
        op(mp_copy(a, buf, m, 0, partner))

    def mp_relay(a, buf):
        for k in range(1, X):
            src = lax.rem(chip + k, X) * 2 + core
            mp_copy(a, buf, src, k, partner).wait_recv()
            mp_copy(a, buf, src, k, partner).start()

    def mp_wait(a, buf):
        for k in range(X):
            src = lax.rem(chip + k, X) * 2 + 1 - core
            mp_copy(a, buf, src, k, partner).wait_recv()

    def mp_sent(a, buf):
        mp_first(a, buf, lambda c: c.wait_send())
        for k in range(1, X):
            mp_copy(a, buf, lax.rem(chip + k, X) * 2 + core, k, partner).wait_send()

    load[0].wait()
    for a in range(2):
        ag_own(a)
        y_sends(a, z, start)
    load[1].wait()
    mp_first(0, rbuf, start)
    for p in range(parts):
        load[4 + p].wait()

    def far_slot(k):
        return lax.rem(k + X, X) - 1

    def r_near(db):
        xb, sub = lax.div(db, 2 * q), lax.rem(db, q)
        return send(ssend.at[:, db], r1buf.at[:, xb, sub], rs1.at[xb, sub], rr1.at[xb, sub], (d, partner))

    def r_far(db):
        xb, sub = lax.div(db, 2 * q), lax.rem(db, q)
        slot = far_slot(chip - xb)
        return send(ssend.at[:, db], r2buf.at[:, slot, sub], rs2.at[xb, sub], rr2.at[slot, sub], (d, xb * 2 + core))

    def r_term(db):
        xb, sub = lax.div(db, 2 * q), lax.rem(db, q)
        mine = lax.rem(lax.div(db, q), 2) == core

        def one(t):
            term = lax.dot_general(
                gbuf[db, :, t], gbuf[d], (((0,), (0,)), ((), ())), preferred_element_type=f32
            )
            for h in range(last_chunks):
                ssend[h, db, t, :] = term[:, h * cw:(h + 1) * cw].astype(bf16)
        tiles(cols, min(256, cols), one)

        def add():
            got = r1buf.at[:, xb, sub]
            send(got, got, rs1.at[0, 0], rr1.at[xb, sub], (d, partner)).wait_recv()
            for h in range(last_chunks):
                ssend[h, db] = (ssend[h, db].astype(f32) + r1buf[h, xb, sub].astype(f32)).astype(bf16)
            when(xb != chip, lambda: r_far(db).start())
        when(jnp.logical_not(mine), lambda: r_near(db).start())
        when(mine, add)

    def rr_term(db):
        rhs = sub_rows(rbuf, db)
        def one(t):
            acc[t, :] += jnp.dot(gbuf[db, t, :], rhs[...], preferred_element_type=f32)
        tiles(rows, tile, one)

    def zero_acc():
        def one(t):
            acc[t, :] = jnp.zeros((tile, cols), f32)
        tiles(rows, tile, one)

    r_term(d)

    def g_step(i):
        s = i + 1
        ag_step(0, s)
        ag_step(1, s, then=2)
        when(s == min(2, last), lambda: mp_relay(0, rbuf))
        at_distance(s, lambda zb: r_term(zb * 2 + y))
    loop(Z - 1, g_step)
    y_sends(2, z, start)
    zero_acc()
    mp_wait(0, rbuf)
    by_distance(lambda zb: rr_term(zb * 2 + y))

    def y_block(zb):
        wait_y(0, zb)
        wait_y(1, zb)
        rr_term(zb * 2 + 1 - y)
    by_distance(y_block)

    def rr_out(t):
        rrbuf[m, t, :] = acc[t, :].astype(bf16)
    tiles(rows, tile, rr_out)
    mp_first(1, rrbuf, start)
    zero_acc()

    owner = lax.div(d, q)
    own_chip = lax.div(owner, 2)
    hd = dp // 2
    pair_off = pl.multiple_of(lax.rem(d, q) * cols, cols)

    def p_send(hb, i, to):
        view_p = pbuf.at[pl.ds(hb * hd, hd)]
        return send(view_p, view_p, ps.at[i], pr.at[hb], (d, to))

    def to_chips(op):
        for k in range(1, X):
            op(p_send(core, 2 + k, lax.rem(chip + k, X) * 2 + core))

    def own_pair():
        def copy(i):
            pbuf[i] = gbuf[i, pl.ds(pair_off, cols), :]
        loop(dp, copy)
        for hb in range(2):
            p_send(hb, hb, partner).start()
        to_chips(start)

    def near_pair():
        for hb in range(2):
            p_send(hb, hb, partner).wait_recv()
        to_chips(start)

    def far_relay():
        p_send(core, 0, partner).wait_recv()
        p_send(core, 0, partner).start()

    def far_pair():
        p_send(1 - core, 0, partner).wait_recv()

    when(m == owner, own_pair)

    def back_term(db, piece, t):
        p, r0, _, c0, w, _ = piece
        off = pl.multiple_of(lax.rem(db, q) * cols + c0, w)
        rhs = rbuf[lax.div(db, q), pl.ds(off, w), :]
        mine = pl.ds(pl.multiple_of(t.start + (p * part + r0), t.size), t.size)
        return lax.dot_general(
            dbuf[mine, :], rhs, (((1,), (1,)), ((), ())), preferred_element_type=f32
        )

    def piece_tiles(piece, fn):
        tiles(piece[2], min(256, piece[2]), fn)

    def by_send(i, zb):
        return send(out_bufs[i].at[zb], y_bufs[i].at[zb], bys.at[i, zb], byr.at[i, zb], (ynbr, m))

    def by_last(i):
        return send(out_bufs[i].at[z, 1 - y], y_bufs[i], bys.at[i, 0], byr.at[i, 0], (ynbr, m))

    def bz_up(i, zb, src):
        return send(src.at[zb], z_bufs[i].at[zb], bzs.at[i, zb], bzr.at[i, zb], (d + 2, m))

    def bz_dn(i, zb, src):
        slot = jnp.where(zb == z - 1, Z, zb)
        return send(src.at[zb], z_bufs[i].at[slot], bzs.at[i, zb], bzr.at[i, slot], (d - 2, m))

    def z_arrivals(i, zb, add):
        def one(slot):
            dst = z_bufs[i].at[slot]
            send(dst, dst, bzs.at[i, 0], bzr.at[i, slot], (ynbr, m)).wait_recv()
            add(slot)
        when(jnp.logical_and(zb >= z, z > 0), lambda: one(zb))
        when(jnp.logical_and(zb < z, z < last), lambda: one(zb))
        when(jnp.logical_and(zb == z, z < last), lambda: one(Z))

    def z_send(i, zb, src):
        when(zb > z, lambda: bz_up(i, zb, src).start())
        when(zb < z, lambda: bz_dn(i, zb, src).start())

    def to_back(piece, t, value):
        p, r0, _, c0, w, _ = piece
        mine = pl.ds(pl.multiple_of(t.start + (p * part + r0), t.size), t.size)
        bbuf[mine, pl.ds(c0, w)] = value.astype(bf16)

    def line_y_first(i, piece, zb):
        c = pl.ds(0, piece[4])
        by_send(i, zb).wait_recv()

        def one(t):
            acc[t, c] = back_term(zb * 2 + y, piece, t) + y_bufs[i][zb, t, :].astype(f32)
        piece_tiles(piece, one)

        def add(slot):
            def more(t):
                acc[t, c] += z_bufs[i][slot, t, :].astype(f32)
            piece_tiles(piece, more)
        z_arrivals(i, zb, add)

        def pack(t):
            y_bufs[i][zb, t, :] = acc[t, c].astype(bf16)
        when(zb != z, lambda: piece_tiles(piece, pack))
        z_send(i, zb, y_bufs[i])
        when(zb == z, lambda: piece_tiles(piece, lambda t: to_back(piece, t, acc[t, c])))

    def line_z_first(i, piece, zb):
        n = piece[2]

        def rows_of(t, yy):
            return pl.ds(pl.multiple_of(t.start + yy * n, t.size), t.size)
        for yy in range(2):
            def one(t, yy=yy):
                acc[rows_of(t, yy), pl.ds(0, piece[4])] = back_term(zb * 2 + yy, piece, t)
            piece_tiles(piece, one)

        def add(slot):
            for yy in range(2):
                def more(t, yy=yy):
                    acc[rows_of(t, yy), pl.ds(0, piece[4])] += z_bufs[i][slot, yy, t, :].astype(f32)
                piece_tiles(piece, more)
        z_arrivals(i, zb, add)
        for yy in range(2):
            def pack(t, yy=yy):
                out_bufs[i][zb, yy, t, :] = acc[rows_of(t, yy), pl.ds(0, piece[4])].astype(bf16)
            piece_tiles(piece, pack)
        z_send(i, zb, out_bufs[i])
        when(zb == z, lambda: by_last(i).start())

    def finish_z_first(i, piece):
        by_last(i).wait_recv()

        def one(t):
            mine = out_bufs[i][z, y, t, :].astype(f32) + y_bufs[i][t, :].astype(f32)
            to_back(piece, t, mine)
        piece_tiles(piece, one)

    def numbered(p):
        return list(enumerate(pieces[p], first_piece[p]))

    def scatter_first(p):
        for i, piece in numbered(p):
            if piece[5] == Z_FIRST:
                continue

            def one_block(zb, i=i, piece=piece):
                def one(t):
                    out_bufs[i][zb, t, :] = back_term(zb * 2 + 1 - y, piece, t).astype(bf16)
                piece_tiles(piece, one)
                by_send(i, zb).start()
            by_distance(one_block, far_first=True)

    def scatter_step(i, piece, s):
        fn = line_z_first if piece[5] == Z_FIRST else line_y_first
        at_distance(s, lambda zb: fn(i, piece, zb))

    mom_tile = min(128, part)

    def m_term(p, db):
        rhs = sub_rows(rrbuf, db)
        def one(t):
            acc[t, :] += lax.dot_general(
                lbuf[p, db, :, t], rhs[...], (((0,), (0,)), ((), ())), preferred_element_type=f32
            )
        tiles(part, tile, one)

    def zero_part():
        def one(t):
            acc[t, :] = jnp.zeros((tile, cols), f32)
        tiles(part, tile, one)

    def moments(p):
        def one(t):
            w = pl.ds(pl.multiple_of(t.start + p * part, mom_tile), mom_tile)
            rot = acc[t, :]
            new1 = decay_moment * mom1[t, :] + (1.0 - decay_moment) * rot
            new2 = decay_moment * mom2[t, :] + (1.0 - decay_moment) * rot * rot
            mom1[t, :] = new1
            mom2[t, :] = new2
            dbuf[w, :] = (new1 / (jnp.sqrt(new2) + epsilon)).astype(bf16)
        tiles(part, mom_tile, one)

    def direction(p):
        def y_part(zb):
            wait_y(2 + p, zb)
            m_term(p, zb * 2 + 1 - y)
        by_distance(y_part)
        for c in mom_loads(p):
            c.wait()
        moments(p)
        for c in mom_stores(p):
            c.start()

    def r_y_terms(near):
        def one(zb):
            db = zb * 2 + 1 - y
            mine = lax.rem(lax.div(db, q), 2) == core
            when(jnp.logical_xor(mine, near), lambda: r_term(db))
        by_distance(one)

    def l_step(i):
        s = i + 1
        when(s == last, lambda: mp_relay(1, rrbuf))
        ag_step(2, s, then=3 if parts > 1 else None)
        when(jnp.logical_and(s == min(2, last), jnp.logical_and(chip == own_chip, m != owner)), near_pair)
        when(s == 1, lambda: r_y_terms(True))
        when(s == min(2, last), lambda: r_y_terms(False))
    loop(Z - 1, l_step)
    if parts > 1:
        y_sends(3, z, start)
    mp_wait(1, rrbuf)
    by_distance(lambda zb: m_term(0, zb * 2 + y))
    direction(0)
    scatter_first(0)

    def r_final():
        for sub in range(q):
            for k in range(1, X):
                got = r2buf.at[:, k - 1, sub]
                send(got, got, rs1.at[0, 0], rr2.at[k - 1, sub], (d, partner)).wait_recv()
            for h in range(last_chunks):
                def one(t, sub=sub, h=h):
                    total = ssend[h, m * q + sub, t, :].astype(f32)
                    for k in range(1, X):
                        total += r2buf[h, k - 1, sub, t, :].astype(f32)
                    where = pl.ds(pl.multiple_of(sub * cols + t.start, 128), 128)
                    c = pl.ds(h * cw, cw)
                    fac_r[where, c] = decay_factor * fac_r[where, c] + (1.0 - decay_factor) * total
                tiles(cols, 128, one)

    def l_scale(t):
        fac_l[t, :] = decay_factor * fac_l[t, :]
    load[2].wait()
    load[3].wait()
    tiles(rows, tile, l_scale)

    def l_term(db):
        def one(t):
            fac_l[t, :] += (1.0 - decay_factor) * lax.dot_general(
                gbuf[db, t, :], pbuf[db], (((1,), (1,)), ((), ())), preferred_element_type=f32
            )
        tiles(rows, tile, one)

    for p in range(1, parts):
        def both(i, p=p):
            s = i + 1
            if p == 1:
                when(jnp.logical_and(s == last, chip != own_chip), far_relay)
            ag_step(2 + p, s, then=3 + p if p + 1 < parts else None)
            for j, piece in numbered(p - 1):
                scatter_step(j, piece, Z - s)
        loop(Z - 1, both)
        if p + 1 < parts:
            y_sends(3 + p, z, start)
        if p == 1:
            r_final()
            store_right.start()
            when(chip != own_chip, far_pair)
            loop(EARLY, l_term)
        for j, piece in numbered(p - 1):
            scatter_step(j, piece, 0)
        zero_part()
        for c in mom_stores(p - 1):
            c.wait()
        for c in mom_loads(p):
            c.start()
        by_distance(lambda zb, p=p: m_term(p, zb * 2 + y))
        direction(p)
        scatter_first(p)
        for j, piece in numbered(p - 1):
            if piece[5] == Z_FIRST:
                finish_z_first(j, piece)

    def r_sent(db):
        mine = lax.rem(lax.div(db, q), 2) == core
        when(jnp.logical_not(mine), lambda: r_near(db).wait_send())
        when(jnp.logical_and(mine, lax.div(db, 2 * q) != chip), lambda: r_far(db).wait_send())
    loop(dp, r_sent)

    def u_near(h, xb, sub):
        db = (xb * 2 + 1 - core) * q + sub
        return send(
            ssend.at[h, db], u1buf.at[h, xb, sub], us1.at[h, xb, sub], ur1.at[h, xb, sub], (d, partner)
        )

    def u_far(h, xb, sub):
        db = (xb * 2 + core) * q + sub
        slot = far_slot(chip - xb)
        return send(
            ssend.at[h, db], u2buf.at[h, slot, sub], us2.at[h, xb, sub], ur2.at[h, slot, sub], (d, xb * 2 + core)
        )

    def u_got(dst, sem):
        send(dst, dst, us1.at[0, 0, 0], sem, (d, partner)).wait_recv()

    def u_dot(h, db):
        c = pl.ds(h * cw, cw)
        total = None
        for p in range(parts):
            term = jnp.dot(lbuf[p, db], bbuf[pl.ds(p * part, part), c], preferred_element_type=f32)
            total = term if total is None else total + term
        return total

    def u_terms(h):
        def near(i):
            xb, sub = lax.rem(chip + 1 + lax.div(i, q), X), lax.rem(i, q)
            db = (xb * 2 + 1 - core) * q + sub
            ssend[h, db] = u_dot(h, db).astype(bf16)
            u_near(h, xb, sub).start()
        loop(X * q, near)

        def far(i):
            xb, sub = lax.rem(chip + 1 + lax.div(i, q), X), lax.rem(i, q)
            db = (xb * 2 + core) * q + sub
            mine = u_dot(h, db)
            u_got(u1buf.at[h, xb, sub], ur1.at[h, xb, sub])
            ssend[h, db] = (mine + u1buf[h, xb, sub].astype(f32)).astype(bf16)
            when(xb != chip, lambda: u_far(h, xb, sub).start())
        loop(X * q, far)

    def u_final(h):
        c = pl.ds(h * cw, cw)
        for sub in range(q):
            for k in range(1, X):
                u_got(u2buf.at[h, k - 1, sub], ur2.at[h, k - 1, sub])

            def one(t, sub=sub):
                total = ssend[h, m * q + sub, t, :].astype(f32)
                for k in range(1, X):
                    total += u2buf[h, k - 1, sub, t, :].astype(f32)
                where = pl.ds(pl.multiple_of(sub * cols + t.start, 128), 128)
                dbuf[where, c] = total.astype(bf16)
            tiles(cols, 128, one)

    done = EARLY
    for tau in range(last_chunks + Z - 1):
        for h, (i, piece) in enumerate(numbered(parts - 1)):
            late = 1 if piece[5] == Z_FIRST else 0
            if 0 <= tau - h <= last:
                scatter_step(i, piece, last - (tau - h))
            if tau - h == last + late:
                if late:
                    finish_z_first(i, piece)
                u_terms(h)
        per = -(-(dp - EARLY) // (last_chunks + Z - 2))
        if done < dp:
            loop(min(per, dp - done), lambda k, done=done: l_term(done + k))
            done = min(done + per, dp)
            if done == dp:
                store_left.start()
    for h in range(last_chunks):
        u_final(h)
    store_update.start()

    for a in range(2 + parts):
        def sent(i, a=a):
            when(jnp.logical_and(z < last, i <= z), lambda: up(a, i).wait_send())
            when(jnp.logical_and(z > 0, i >= z), lambda: dn(a, i).wait_send())
            y_sends(a, i, lambda c: c.wait_send())
        loop(Z, sent)
        when(z > 0, lambda a=a: extra(a, 1).wait_send())
        when(z < last, lambda a=a: extra(a, 0).wait_send())
    mp_sent(0, rbuf)
    mp_sent(1, rrbuf)

    def near_sent():
        to_chips(lambda c: c.wait_send())
    when(chip == own_chip, near_sent)

    def own_sent():
        for hb in range(2):
            p_send(hb, hb, partner).wait_send()
    when(m == owner, own_sent)
    when(chip != own_chip, lambda: p_send(core, 0, partner).wait_send())
    def line_sent(i, piece):
        src = out_bufs[i] if piece[5] == Z_FIRST else y_bufs[i]

        def one(zb):
            if piece[5] == Y_FIRST:
                by_send(i, zb).wait_send()
            when(zb != z, lambda: bz_up(i, zb, src).wait_send())
        loop(Z, one)
        if piece[5] == Z_FIRST:
            by_last(i).wait_send()
    for p in range(parts):
        for i, piece in numbered(p):
            line_sent(i, piece)
    for h in range(last_chunks):
        for sub in range(q):
            for xb in range(X):
                u_near(h, xb, sub).wait_send()
                when(xb != chip, lambda h=h, xb=xb, sub=sub: u_far(h, xb, sub).wait_send())
    for c in mom_stores(parts - 1) + [store_left, store_right, store_update]:
        c.wait()


def write_out(*refs):
    n = (len(refs) - 2) // 3
    ins, outs, bufs, sem_in, sem_out = refs[:n], refs[n:2 * n], refs[2 * n:-2], refs[-2], refs[-1]
    reads = [pltpu.make_async_copy(a, b, sem_in.at[i]) for i, (a, b) in enumerate(zip(ins, bufs))]
    writes = [pltpu.make_async_copy(b, a, sem_out.at[i]) for i, (a, b) in enumerate(zip(outs, bufs))]
    for c in reads:
        c.start()
    for r, w in zip(reads, writes):
        r.wait()
        w.start()
    for w in writes:
        w.wait()


def solution(mesh):
    dp, mp = mesh.shape["dp"], mesh.shape["mp"]
    Z, X = dp // 2, mp // 2

    def per_device(*args):
        _, rows, cols = args[0].shape
        q = rows // cols
        parts = min(PARTS, rows // 128)
        last_chunks = min(LAST, cols // 128)
        part, cw = rows // parts, cols // last_chunks
        pieces = sum(scatter_pieces(rows, cols, parts, last_chunks), [])
        n = len(pieces)
        out_b, y_b, z_b = [], [], []
        for _, _, nr, _, w, kind in pieces:
            lead = (2,) if kind == Z_FIRST else ()
            out_b.append(pltpu.VMEM((Z,) + lead + (nr, w), bf16))
            y_b.append(pltpu.VMEM((nr, w) if lead else (Z, nr, w), bf16))
            z_b.append(pltpu.VMEM((Z + 1,) + lead + (nr, w), bf16))
        flat = [a.reshape(a.shape[1:]) for a in args]
        dma = pltpu.SemaphoreType.DMA
        outs = pl.pallas_call(
            functools.partial(kernel, dp, mp, rows, cols, parts, last_chunks),
            out_shape=[jax.ShapeDtypeStruct((rows, cols), t) for t in (f32, f32, f32, f32, bf16)],
            in_specs=[pl.BlockSpec(memory_space=pl.ANY)] * 7,
            out_specs=[pl.BlockSpec(memory_space=pl.ANY)] * 5,
            scratch_shapes=[
                pltpu.VMEM((dp, rows, cols), bf16),
                pltpu.VMEM((parts, dp, cols, part), bf16),
                pltpu.VMEM((mp, rows, cols), bf16),
                pltpu.VMEM((mp, rows, cols), bf16),
                pltpu.VMEM((dp, cols, cols), bf16),
                pltpu.VMEM((last_chunks, dp, cols, cw), bf16),
                pltpu.VMEM((last_chunks, X, q, cols, cw), bf16),
                pltpu.VMEM((last_chunks, X - 1, q, cols, cw), bf16),
                pltpu.VMEM((last_chunks, X - 1, q, cols, cw), bf16),
                pltpu.VMEM((rows, cols), f32),
                pltpu.VMEM((rows, cols), f32),
                pltpu.VMEM((part, cols), f32),
                pltpu.VMEM((part, cols), f32),
                pltpu.VMEM((rows, cols), f32),
                pltpu.VMEM((rows, cols), bf16),
                pltpu.VMEM((rows, cols), bf16),
                dma((4 + 3 * parts,)),
                dma((3 + 2 * parts,)),
                dma((2 + parts, Z)),
                dma((2 + parts, Z)),
                dma((2 + parts, Z)),
                dma((2 + parts, Z, 2)),
                dma((2 + parts, Z, 2)),
                dma((2 + parts, 2)),
                dma((2 + parts, 2)),
                dma((2, 2 * X)),
                dma((2, mp)),
                dma((X, q)),
                dma((X, q)),
                dma((X, q)),
                dma((X - 1, q)),
                dma((last_chunks, X, q)),
                dma((last_chunks, X, q)),
                dma((last_chunks, X, q)),
                dma((last_chunks, X - 1, q)),
                dma((2 + X,)),
                dma((2,)),
                dma((n, Z)),
                dma((n, Z)),
                dma((n, Z)),
                dma((n, Z + 1)),
            ] + out_b + y_b + z_b,
            compiler_params=pltpu.CompilerParams(
                collective_id=0, has_side_effects=True, vmem_limit_bytes=67043328
            ),
        )(*flat)
        kinds = [jax.ShapeDtypeStruct(o.shape, o.dtype) for o in outs]
        outs = pl.pallas_call(
            write_out,
            out_shape=kinds,
            in_specs=[pl.BlockSpec(memory_space=pl.ANY)] * len(outs),
            out_specs=[pl.BlockSpec(memory_space=pl.ANY)] * len(outs),
            scratch_shapes=[pltpu.VMEM(o.shape, o.dtype) for o in outs] + [dma((len(outs),)), dma((len(outs),))],
            compiler_params=pltpu.CompilerParams(vmem_limit_bytes=67043328),
        )(*outs)
        return tuple(o.reshape((1,) + o.shape) for o in outs)

    return jax.shard_map(
        per_device,
        mesh=mesh,
        in_specs=(P(None, "mp", "dp"),) * 5 + (P(None, "dp", "mp"), P(None, "mp", "dp")),
        out_specs=(P(None, "mp", "dp"),) * 5,
        check_vma=False,
    )
```

```python
import functools

import jax
import jax.numpy as jnp
from jax import lax
from jax.experimental import pallas as pl
from jax.experimental.pallas import tpu as pltpu
from jax.sharding import PartitionSpec as P

decay_moment = 0.95
decay_factor = 0.95
epsilon = 1e-08
bf16, f32 = jnp.bfloat16, jnp.float32
MESH = pl.DeviceIdType.MESH
PARTS, LAST, LAST_Z, EARLY = 2, 4, 1, 4
Y_FIRST, Z_FIRST = 0, 1


def scatter_pieces(rows, cols, parts, last_chunks):
    part = rows // parts
    out = [[] for _ in range(parts)]
    for p in range(parts - 1):
        out[p].append((p, 0, part // 2, 0, cols, Z_FIRST))
        out[p].append((p, part // 2, part // 2, 0, cols, Y_FIRST))
    for h in range(last_chunks):
        cw = cols // last_chunks
        out[parts - 1].append((parts - 1, 0, part, h * cw, cw, Z_FIRST if h < LAST_Z else Y_FIRST))
    return out


def kernel(dp, mp, rows, cols, parts, last_chunks, *refs):
    pieces = scatter_pieces(rows, cols, parts, last_chunks)
    first_piece = [sum(len(x) for x in pieces[:p]) for p in range(parts)]
    n_pieces = sum(len(x) for x in pieces)
    NAMED = len(refs) - 3 * n_pieces
    (grad, first, second, left_f, right_f, left_b, right_b,
     out_first, out_second, out_left, out_right, out_update,
     gbuf, lbuf, rbuf, rrbuf, pbuf, ssend, r1buf, r2buf, u2buf,
     fac_l, fac_r, mom1, mom2, acc, dbuf, bbuf,
     load_sem, store_sem, zs_up, zs_dn, zr, ys, yr, es, er, as_, ar,
     rs1, rr1, rs2, rr2, us1, ur1, us2, ur2, ps, pr, bys, byr, bzs, bzr) = refs[:NAMED]
    out_bufs = refs[NAMED:NAMED + n_pieces]
    y_bufs = refs[NAMED + n_pieces:NAMED + 2 * n_pieces]
    z_bufs = refs[NAMED + 2 * n_pieces:]
    u1buf = r1buf
    Z, q, X = dp // 2, rows // cols, mp // 2
    part, cw = rows // parts, cols // last_chunks
    d, m = lax.axis_index("dp"), lax.axis_index("mp")
    z, y = lax.div(d, 2), lax.rem(d, 2)
    core, chip = lax.rem(m, 2), lax.div(m, 2)
    partner = chip * 2 + (1 - core)
    last = Z - 1
    ynbr = z * 2 + (1 - y)
    tile = min(256, part)

    def send(src, dst, s, r, dev):
        return pltpu.make_async_remote_copy(
            src_ref=src, dst_ref=dst, send_sem=s, recv_sem=r, device_id=dev, device_id_type=MESH
        )

    def when(cond, fn):
        pl.when(cond)(fn)

    def loop(n, fn):
        def body(i, c):
            fn(i)
            return c
        lax.fori_loop(0, n, body, 0)

    def tiles(n, size, fn, base=0):
        loop(n // size, lambda i: fn(pl.ds(pl.multiple_of(base + i * size, size), size)))

    loads = [
        (grad, gbuf.at[d]), (right_b, rbuf.at[m]), (right_f, fac_r), (left_f, fac_l),
    ]
    loads += [(left_b.at[:, pl.ds(p * part, part)], lbuf.at[p, d]) for p in range(parts)]
    load = [pltpu.make_async_copy(a, b, load_sem.at[i]) for i, (a, b) in enumerate(loads)]
    for c in load:
        c.start()

    def part_rows(ref, p):
        return ref.at[pl.ds(p * part, part), :]

    def mom_loads(p):
        n = 4 + parts + 2 * p
        return [
            pltpu.make_async_copy(part_rows(a, p), b, load_sem.at[n + i])
            for i, (a, b) in enumerate([(first, mom1), (second, mom2)])
        ]

    def mom_stores(p):
        return [
            pltpu.make_async_copy(b, part_rows(a, p), store_sem.at[3 + 2 * p + i])
            for i, (a, b) in enumerate([(out_first, mom1), (out_second, mom2)])
        ]

    store_right = pltpu.make_async_copy(fac_r, out_right, store_sem.at[0])
    store_left = pltpu.make_async_copy(fac_l, out_left, store_sem.at[1])
    store_update = pltpu.make_async_copy(dbuf, out_update, store_sem.at[2])
    for c in mom_loads(0):
        c.start()

    barrier = pltpu.get_barrier_semaphore()
    pl.semaphore_signal(barrier, inc=1, device_id=(ynbr, m), device_id_type=MESH)
    when(z > 0, lambda: pl.semaphore_signal(barrier, inc=1, device_id=(d - 2, m), device_id_type=MESH))
    when(z < last, lambda: pl.semaphore_signal(barrier, inc=1, device_id=(d + 2, m), device_id_type=MESH))
    for k in range(1, mp):
        pl.semaphore_signal(barrier, inc=1, device_id=(d, lax.rem(m + k, mp)), device_id_type=MESH)
    along = (z > 0).astype(jnp.int32) + (z < last).astype(jnp.int32)
    pl.semaphore_wait(barrier, mp + along)

    def half(a, b, hb):
        if a < 2:
            return gbuf.at[b, pl.ds(a * (rows // 2) + hb * (rows // 4), rows // 4), :]
        return lbuf.at[a - 2, b, pl.ds(hb * (cols // 2), cols // 2), :]

    def up(a, zb, hb):
        blk = half(a, zb * 2 + y, hb)
        return send(blk, blk, zs_up.at[a, zb, hb], zr.at[a, zb, hb], (d + 2, m))

    def dn(a, zb, hb):
        blk = half(a, zb * 2 + y, hb)
        return send(blk, blk, zs_dn.at[a, zb, hb], zr.at[a, zb, hb], (d - 2, m))

    def ysend(a, zb, hb):
        blk = half(a, zb * 2 + y, hb)
        return send(blk, blk, ys.at[a, zb, hb], yr.at[a, zb, hb], (ynbr, m))

    def yrecv_desc(a, zb, hb):
        blk = half(a, zb * 2 + (1 - y), hb)
        return send(blk, blk, ys.at[a, zb, hb], yr.at[a, zb, hb], (ynbr, m))

    def by_line(a):
        return (0, 1) if a == 1 + parts else (1,)

    def extra(a, k, hb):
        zb = 0 if k == 0 else last
        blk = half(a, zb * 2 + (1 - y), hb)
        return send(blk, blk, es.at[a, k, hb], er.at[a, k, hb], (d + 2, m) if k == 0 else (d - 2, m))

    def over_y(a, zb, hb):
        inner = jnp.logical_and(zb > 0, zb < last)
        return jnp.logical_or(zb == z, inner)

    def y_sends(a, zb, op):
        for hb in (1, 0):
            if hb in by_line(a):
                when(over_y(a, zb, hb), lambda hb=hb: op(ysend(a, zb, hb)))
            else:
                op(ysend(a, zb, hb))

    def start(c):
        c.start()

    def ag_own(a):
        for hb in range(2):
            when(z < last, lambda: up(a, z, hb).start())
            when(z > 0, lambda: dn(a, z, hb).start())

    def ag_step(a, s, then=None):
        below, above = z - s, z + s

        def from_below():
            for hb in range(2):
                up(a, below, hb).wait_recv()
                when(z < last, lambda hb=hb: up(a, below, hb).start())

        def from_above():
            for hb in range(2):
                dn(a, above, hb).wait_recv()
                when(z > 0, lambda hb=hb: dn(a, above, hb).start())

        when(below >= 0, from_below)
        when(above <= last, from_above)
        when(below >= 0, lambda: y_sends(a, below, start))
        when(above <= last, lambda: y_sends(a, above, start))

        def extra_dn():
            for hb in by_line(a):
                when(z == last, lambda hb=hb: yrecv_desc(a, z, hb).wait_recv())
                when(z < last, lambda hb=hb: extra(a, 1, hb).wait_recv())
                extra(a, 1, hb).start()
            if then is not None:
                for hb in range(2):
                    dn(then, z, hb).start()

        def extra_up():
            for hb in by_line(a):
                when(z == 0, lambda hb=hb: yrecv_desc(a, z, hb).wait_recv())
                when(z > 0, lambda hb=hb: extra(a, 0, hb).wait_recv())
                extra(a, 0, hb).start()
            if then is not None:
                for hb in range(2):
                    up(then, z, hb).start()

        when(jnp.logical_and(z == Z - s, z > 0), extra_dn)
        when(jnp.logical_and(z == s - 1, z < last), extra_up)

    def wait_y(a, zb):
        inner = jnp.logical_and(zb > 0, zb < last)
        for hb in range(2):
            if hb in by_line(a):
                when(inner, lambda hb=hb: yrecv_desc(a, zb, hb).wait_recv())
                when(jnp.logical_and(zb == last, z == 0), lambda hb=hb: extra(a, 1, hb).wait_recv())
                when(jnp.logical_and(zb == 0, z == last), lambda hb=hb: extra(a, 0, hb).wait_recv())
            else:
                yrecv_desc(a, zb, hb).wait_recv()

    def at_distance(s, fn):
        def side(j):
            zb = z + (2 * j - 1) * s
            ok = jnp.logical_and(zb >= 0, zb <= last)
            when(jnp.logical_and(ok, jnp.logical_or(s > 0, j == 0)), lambda: fn(zb))
        loop(2, side)

    def by_distance(fn, far_first=False):
        loop(Z, lambda i: at_distance(last - i if far_first else i, fn))

    def sub_rows(ref, db):
        off = pl.multiple_of(lax.rem(db, q) * cols, cols)
        return ref.at[lax.div(db, q), pl.ds(off, cols), :]

    def mp_copy(a, buf, src, k, to):
        return send(buf.at[src], buf.at[src], as_.at[a, k], ar.at[a, src], (d, to))

    def mp_first(a, buf, op):
        for k in range(1, X):
            op(mp_copy(a, buf, m, X + k, lax.rem(chip + k, X) * 2 + core))
        op(mp_copy(a, buf, m, 0, partner))

    def mp_relay(a, buf):
        for k in range(1, X):
            src = lax.rem(chip + k, X) * 2 + core
            mp_copy(a, buf, src, k, partner).wait_recv()
            mp_copy(a, buf, src, k, partner).start()

    def mp_wait(a, buf):
        for k in range(X):
            src = lax.rem(chip + k, X) * 2 + 1 - core
            mp_copy(a, buf, src, k, partner).wait_recv()

    def mp_sent(a, buf):
        mp_first(a, buf, lambda c: c.wait_send())
        for k in range(1, X):
            mp_copy(a, buf, lax.rem(chip + k, X) * 2 + core, k, partner).wait_send()

    load[0].wait()
    for a in range(2):
        ag_own(a)
        y_sends(a, z, start)
    load[1].wait()
    mp_first(0, rbuf, start)
    for p in range(parts):
        load[4 + p].wait()

    def far_slot(k):
        return lax.rem(k + X, X) - 1

    def r_near(db):
        xb, sub = lax.div(db, 2 * q), lax.rem(db, q)
        return send(ssend.at[:, db], r1buf.at[:, xb, sub], rs1.at[xb, sub], rr1.at[xb, sub], (d, partner))

    def r_far(db):
        xb, sub = lax.div(db, 2 * q), lax.rem(db, q)
        slot = far_slot(chip - xb)
        return send(ssend.at[:, db], r2buf.at[:, slot, sub], rs2.at[xb, sub], rr2.at[slot, sub], (d, xb * 2 + core))

    def r_term(db):
        xb, sub = lax.div(db, 2 * q), lax.rem(db, q)
        mine = lax.rem(lax.div(db, q), 2) == core

        def one(t):
            term = lax.dot_general(
                gbuf[db, :, t], gbuf[d], (((0,), (0,)), ((), ())), preferred_element_type=f32
            )
            for h in range(last_chunks):
                ssend[h, db, t, :] = term[:, h * cw:(h + 1) * cw].astype(bf16)
        tiles(cols, min(256, cols), one)

        def add():
            got = r1buf.at[:, xb, sub]
            send(got, got, rs1.at[0, 0], rr1.at[xb, sub], (d, partner)).wait_recv()
            for h in range(last_chunks):
                ssend[h, db] = (ssend[h, db].astype(f32) + r1buf[h, xb, sub].astype(f32)).astype(bf16)
            when(xb != chip, lambda: r_far(db).start())
        when(jnp.logical_not(mine), lambda: r_near(db).start())
        when(mine, add)

    def rr_term(db):
        rhs = sub_rows(rbuf, db)
        def one(t):
            acc[t, :] += jnp.dot(gbuf[db, t, :], rhs[...], preferred_element_type=f32)
        tiles(rows, tile, one)

    def zero_acc():
        def one(t):
            acc[t, :] = jnp.zeros((tile, cols), f32)
        tiles(rows, tile, one)

    r_term(d)

    def g_step(i):
        s = i + 1
        ag_step(0, s)
        ag_step(1, s, then=2)
        when(s == min(2, last), lambda: mp_relay(0, rbuf))
        at_distance(s, lambda zb: r_term(zb * 2 + y))
    loop(Z - 1, g_step)
    y_sends(2, z, start)
    zero_acc()
    mp_wait(0, rbuf)
    by_distance(lambda zb: rr_term(zb * 2 + y))

    def y_block(zb):
        wait_y(0, zb)
        wait_y(1, zb)
        rr_term(zb * 2 + 1 - y)
    by_distance(y_block)

    def rr_out(t):
        rrbuf[m, t, :] = acc[t, :].astype(bf16)
    tiles(rows, tile, rr_out)
    mp_first(1, rrbuf, start)
    zero_acc()

    owner = lax.div(d, q)
    own_chip = lax.div(owner, 2)
    hd = dp // 2
    pair_off = pl.multiple_of(lax.rem(d, q) * cols, cols)

    def p_send(hb, i, to):
        view_p = pbuf.at[pl.ds(hb * hd, hd)]
        return send(view_p, view_p, ps.at[i], pr.at[hb], (d, to))

    def to_chips(op):
        for k in range(1, X):
            op(p_send(core, 2 + k, lax.rem(chip + k, X) * 2 + core))

    def own_pair():
        def copy(i):
            pbuf[i] = gbuf[i, pl.ds(pair_off, cols), :]
        loop(dp, copy)
        for hb in range(2):
            p_send(hb, hb, partner).start()
        to_chips(start)

    def near_pair():
        for hb in range(2):
            p_send(hb, hb, partner).wait_recv()
        to_chips(start)

    def far_relay():
        p_send(core, 0, partner).wait_recv()
        p_send(core, 0, partner).start()

    def far_pair():
        p_send(1 - core, 0, partner).wait_recv()

    when(m == owner, own_pair)

    def back_term(db, piece, t):
        p, r0, _, c0, w, _ = piece
        off = pl.multiple_of(lax.rem(db, q) * cols + c0, w)
        rhs = rbuf[lax.div(db, q), pl.ds(off, w), :]
        mine = pl.ds(pl.multiple_of(t.start + (p * part + r0), t.size), t.size)
        return lax.dot_general(
            dbuf[mine, :], rhs, (((1,), (1,)), ((), ())), preferred_element_type=f32
        )

    def piece_tiles(piece, fn):
        tiles(piece[2], min(256, piece[2]), fn)

    def by_send(i, zb):
        return send(out_bufs[i].at[zb], y_bufs[i].at[zb], bys.at[i, zb], byr.at[i, zb], (ynbr, m))

    def by_last(i):
        return send(out_bufs[i].at[z, 1 - y], y_bufs[i], bys.at[i, 0], byr.at[i, 0], (ynbr, m))

    def bz_up(i, zb, src):
        return send(src.at[zb], z_bufs[i].at[zb], bzs.at[i, zb], bzr.at[i, zb], (d + 2, m))

    def bz_dn(i, zb, src):
        slot = jnp.where(zb == z - 1, Z, zb)
        return send(src.at[zb], z_bufs[i].at[slot], bzs.at[i, zb], bzr.at[i, slot], (d - 2, m))

    def z_arrivals(i, zb, add):
        def one(slot):
            dst = z_bufs[i].at[slot]
            send(dst, dst, bzs.at[i, 0], bzr.at[i, slot], (ynbr, m)).wait_recv()
            add(slot)
        when(jnp.logical_and(zb >= z, z > 0), lambda: one(zb))
        when(jnp.logical_and(zb < z, z < last), lambda: one(zb))
        when(jnp.logical_and(zb == z, z < last), lambda: one(Z))

    def z_send(i, zb, src):
        when(zb > z, lambda: bz_up(i, zb, src).start())
        when(zb < z, lambda: bz_dn(i, zb, src).start())

    def to_back(piece, t, value):
        p, r0, _, c0, w, _ = piece
        mine = pl.ds(pl.multiple_of(t.start + (p * part + r0), t.size), t.size)
        bbuf[mine, pl.ds(c0, w)] = value.astype(bf16)

    def line_y_first(i, piece, zb):
        c = pl.ds(0, piece[4])
        by_send(i, zb).wait_recv()

        def one(t):
            acc[t, c] = back_term(zb * 2 + y, piece, t) + y_bufs[i][zb, t, :].astype(f32)
        piece_tiles(piece, one)

        def add(slot):
            def more(t):
                acc[t, c] += z_bufs[i][slot, t, :].astype(f32)
            piece_tiles(piece, more)
        z_arrivals(i, zb, add)

        def pack(t):
            y_bufs[i][zb, t, :] = acc[t, c].astype(bf16)
        when(zb != z, lambda: piece_tiles(piece, pack))
        z_send(i, zb, y_bufs[i])
        when(zb == z, lambda: piece_tiles(piece, lambda t: to_back(piece, t, acc[t, c])))

    def line_z_first(i, piece, zb):
        n = piece[2]

        def rows_of(t, yy):
            return pl.ds(pl.multiple_of(t.start + yy * n, t.size), t.size)
        for yy in range(2):
            def one(t, yy=yy):
                acc[rows_of(t, yy), pl.ds(0, piece[4])] = back_term(zb * 2 + yy, piece, t)
            piece_tiles(piece, one)

        def add(slot):
            for yy in range(2):
                def more(t, yy=yy):
                    acc[rows_of(t, yy), pl.ds(0, piece[4])] += z_bufs[i][slot, yy, t, :].astype(f32)
                piece_tiles(piece, more)
        z_arrivals(i, zb, add)
        for yy in range(2):
            def pack(t, yy=yy):
                out_bufs[i][zb, yy, t, :] = acc[rows_of(t, yy), pl.ds(0, piece[4])].astype(bf16)
            piece_tiles(piece, pack)
        z_send(i, zb, out_bufs[i])
        when(zb == z, lambda: by_last(i).start())

    def finish_z_first(i, piece):
        by_last(i).wait_recv()

        def one(t):
            mine = out_bufs[i][z, y, t, :].astype(f32) + y_bufs[i][t, :].astype(f32)
            to_back(piece, t, mine)
        piece_tiles(piece, one)

    def numbered(p):
        return list(enumerate(pieces[p], first_piece[p]))

    def scatter_first(p):
        for i, piece in numbered(p):
            if piece[5] == Z_FIRST:
                if p == parts - 1:
                    scatter_step(i, piece, last)
                continue

            def one_block(zb, i=i, piece=piece):
                def one(t):
                    out_bufs[i][zb, t, :] = back_term(zb * 2 + 1 - y, piece, t).astype(bf16)
                piece_tiles(piece, one)
                by_send(i, zb).start()
            by_distance(one_block, far_first=True)

    def scatter_step(i, piece, s):
        fn = line_z_first if piece[5] == Z_FIRST else line_y_first
        at_distance(s, lambda zb: fn(i, piece, zb))

    mom_tile = min(128, part)

    def m_term(p, db):
        rhs = sub_rows(rrbuf, db)
        def one(t):
            acc[t, :] += lax.dot_general(
                lbuf[p, db, :, t], rhs[...], (((0,), (0,)), ((), ())), preferred_element_type=f32
            )
        tiles(part, tile, one)

    def zero_part():
        def one(t):
            acc[t, :] = jnp.zeros((tile, cols), f32)
        tiles(part, tile, one)

    def moments(p):
        def one(t):
            w = pl.ds(pl.multiple_of(t.start + p * part, mom_tile), mom_tile)
            rot = acc[t, :]
            new1 = decay_moment * mom1[t, :] + (1.0 - decay_moment) * rot
            new2 = decay_moment * mom2[t, :] + (1.0 - decay_moment) * rot * rot
            mom1[t, :] = new1
            mom2[t, :] = new2
            dbuf[w, :] = (new1 / (jnp.sqrt(new2) + epsilon)).astype(bf16)
        tiles(part, mom_tile, one)

    def direction(p):
        def y_part(zb):
            wait_y(2 + p, zb)
            m_term(p, zb * 2 + 1 - y)
        by_distance(y_part)
        for c in mom_loads(p):
            c.wait()
        moments(p)
        for c in mom_stores(p):
            c.start()

    def r_y_terms(near):
        def one(zb):
            db = zb * 2 + 1 - y
            mine = lax.rem(lax.div(db, q), 2) == core
            when(jnp.logical_xor(mine, near), lambda: r_term(db))
        by_distance(one)

    def l_step(i):
        s = i + 1
        when(s == last, lambda: mp_relay(1, rrbuf))
        ag_step(2, s, then=3 if parts > 1 else None)
        when(jnp.logical_and(s == min(2, last), jnp.logical_and(chip == own_chip, m != owner)), near_pair)
        when(s == 1, lambda: r_y_terms(True))
        when(s == min(2, last), lambda: r_y_terms(False))
    loop(Z - 1, l_step)
    if parts > 1:
        y_sends(3, z, start)
    mp_wait(1, rrbuf)
    by_distance(lambda zb: m_term(0, zb * 2 + y))
    direction(0)
    scatter_first(0)

    def r_final():
        for sub in range(q):
            for k in range(1, X):
                got = r2buf.at[:, k - 1, sub]
                send(got, got, rs1.at[0, 0], rr2.at[k - 1, sub], (d, partner)).wait_recv()
            for h in range(last_chunks):
                def one(t, sub=sub, h=h):
                    total = ssend[h, m * q + sub, t, :].astype(f32)
                    for k in range(1, X):
                        total += r2buf[h, k - 1, sub, t, :].astype(f32)
                    where = pl.ds(pl.multiple_of(sub * cols + t.start, 128), 128)
                    c = pl.ds(h * cw, cw)
                    fac_r[where, c] = decay_factor * fac_r[where, c] + (1.0 - decay_factor) * total
                tiles(cols, 128, one)

    def l_scale(t):
        fac_l[t, :] = decay_factor * fac_l[t, :]
    load[2].wait()
    load[3].wait()
    tiles(rows, tile, l_scale)

    def l_term(db):
        def one(t):
            fac_l[t, :] += (1.0 - decay_factor) * lax.dot_general(
                gbuf[db, t, :], pbuf[db], (((1,), (1,)), ((), ())), preferred_element_type=f32
            )
        tiles(rows, tile, one)

    for p in range(1, parts):
        def both(i, p=p):
            s = i + 1
            if p == 1:
                when(jnp.logical_and(s == last, chip != own_chip), far_relay)
            ag_step(2 + p, s, then=3 + p if p + 1 < parts else None)
            for j, piece in numbered(p - 1):
                scatter_step(j, piece, Z - s)
        loop(Z - 1, both)
        if p + 1 < parts:
            y_sends(3 + p, z, start)
        if p == 1:
            r_final()
            store_right.start()
            when(chip != own_chip, far_pair)
            when(jnp.logical_or(z == 0, z == last), lambda: loop(EARLY, l_term))
        for j, piece in numbered(p - 1):
            scatter_step(j, piece, 0)
        zero_part()
        for c in mom_stores(p - 1):
            c.wait()
        for c in mom_loads(p):
            c.start()
        by_distance(lambda zb, p=p: m_term(p, zb * 2 + y))
        direction(p)
        scatter_first(p)
        for j, piece in numbered(p - 1):
            if piece[5] == Z_FIRST:
                finish_z_first(j, piece)

    def r_sent(db):
        mine = lax.rem(lax.div(db, q), 2) == core
        when(jnp.logical_not(mine), lambda: r_near(db).wait_send())
        when(jnp.logical_and(mine, lax.div(db, 2 * q) != chip), lambda: r_far(db).wait_send())
    loop(dp, r_sent)

    def u_near(h, xb, sub):
        db = (xb * 2 + 1 - core) * q + sub
        return send(
            ssend.at[h, db], u1buf.at[h, xb, sub], us1.at[h, xb, sub], ur1.at[h, xb, sub], (d, partner)
        )

    def u_far(h, xb, sub):
        db = (xb * 2 + core) * q + sub
        slot = far_slot(chip - xb)
        return send(
            ssend.at[h, db], u2buf.at[h, slot, sub], us2.at[h, xb, sub], ur2.at[h, slot, sub], (d, xb * 2 + core)
        )

    def u_got(dst, sem):
        send(dst, dst, us1.at[0, 0, 0], sem, (d, partner)).wait_recv()

    def u_dot(h, db):
        c = pl.ds(h * cw, cw)
        p = parts - 1
        term = jnp.dot(lbuf[p, db], bbuf[pl.ds(p * part, part), c], preferred_element_type=f32)
        return ssend[h, db].astype(f32) + term

    def u_before():
        def one(db):
            for h0 in range(0, last_chunks, 2):
                c = pl.ds(h0 * cw, 2 * cw)
                total = None
                for p in range(parts - 1):
                    term = jnp.dot(lbuf[p, db], bbuf[pl.ds(p * part, part), c], preferred_element_type=f32)
                    total = term if total is None else total + term
                for h in range(2):
                    ssend[h0 + h, db] = total[:, h * cw:(h + 1) * cw].astype(bf16)
        loop(dp, one)

    def u_terms(h):
        def near(i):
            xb, sub = lax.rem(chip + 1 + lax.div(i, q), X), lax.rem(i, q)
            db = (xb * 2 + 1 - core) * q + sub
            ssend[h, db] = u_dot(h, db).astype(bf16)
            u_near(h, xb, sub).start()
        loop(X * q, near)

        def far(i):
            xb, sub = lax.rem(chip + 1 + lax.div(i, q), X), lax.rem(i, q)
            db = (xb * 2 + core) * q + sub
            mine = u_dot(h, db)
            u_got(u1buf.at[h, xb, sub], ur1.at[h, xb, sub])
            ssend[h, db] = (mine + u1buf[h, xb, sub].astype(f32)).astype(bf16)
            when(xb != chip, lambda: u_far(h, xb, sub).start())
        loop(X * q, far)

    def u_final(h):
        c = pl.ds(h * cw, cw)
        for sub in range(q):
            for k in range(1, X):
                u_got(u2buf.at[h, k - 1, sub], ur2.at[h, k - 1, sub])

            def one(t, sub=sub):
                total = ssend[h, m * q + sub, t, :].astype(f32)
                for k in range(1, X):
                    total += u2buf[h, k - 1, sub, t, :].astype(f32)
                where = pl.ds(pl.multiple_of(sub * cols + t.start, 128), 128)
                dbuf[where, c] = total.astype(bf16)
            tiles(cols, 128, one)

    done = EARLY
    wide = numbered(parts - 1)
    per = -(-(dp - EARLY) // (last_chunks + Z - 2))
    for tau in range(last_chunks + Z - 1):
        for h, (i, piece) in enumerate(wide):
            if 0 <= tau - h < last and not (piece[5] == Z_FIRST and tau == 0):
                scatter_step(i, piece, last - (tau - h))
        if tau == 1:
            u_before()
        if tau == 2:
            when(jnp.logical_and(z > 0, z < last), lambda: loop(EARLY, l_term))
        for h, (i, piece) in enumerate(wide):
            z_first = piece[5] == Z_FIRST
            if tau - h == last:
                scatter_step(i, piece, 0)
                if not z_first:
                    u_terms(h)
            if z_first and tau == min(h + last + 2, last_chunks + Z - 2):
                finish_z_first(i, piece)
                u_terms(h)
        if done < dp:
            loop(min(per, dp - done), lambda k, done=done: l_term(done + k))
            done = min(done + per, dp)
            if done == dp:
                store_left.start()
    for h in range(last_chunks):
        u_final(h)
    store_update.start()

    for a in range(2 + parts):
        def sent(i, a=a):
            for hb in range(2):
                when(jnp.logical_and(z < last, i <= z), lambda: up(a, i, hb).wait_send())
                when(jnp.logical_and(z > 0, i >= z), lambda: dn(a, i, hb).wait_send())
            y_sends(a, i, lambda c: c.wait_send())
        loop(Z, sent)
        for hb in by_line(a):
            when(z > 0, lambda: extra(a, 1, hb).wait_send())
            when(z < last, lambda: extra(a, 0, hb).wait_send())
    mp_sent(0, rbuf)
    mp_sent(1, rrbuf)

    def near_sent():
        to_chips(lambda c: c.wait_send())
    when(chip == own_chip, near_sent)

    def own_sent():
        for hb in range(2):
            p_send(hb, hb, partner).wait_send()
    when(m == owner, own_sent)
    when(chip != own_chip, lambda: p_send(core, 0, partner).wait_send())
    def line_sent(i, piece):
        src = out_bufs[i] if piece[5] == Z_FIRST else y_bufs[i]

        def one(zb):
            if piece[5] == Y_FIRST:
                by_send(i, zb).wait_send()
            when(zb != z, lambda: bz_up(i, zb, src).wait_send())
        loop(Z, one)
        if piece[5] == Z_FIRST:
            by_last(i).wait_send()
    for p in range(parts):
        for i, piece in numbered(p):
            line_sent(i, piece)
    for h in range(last_chunks):
        for sub in range(q):
            for xb in range(X):
                u_near(h, xb, sub).wait_send()
                when(xb != chip, lambda h=h, xb=xb, sub=sub: u_far(h, xb, sub).wait_send())
    for c in mom_stores(parts - 1) + [store_left, store_right, store_update]:
        c.wait()


def write_out(*refs):
    n = (len(refs) - 2) // 3
    ins, outs, bufs, sem_in, sem_out = refs[:n], refs[n:2 * n], refs[2 * n:-2], refs[-2], refs[-1]
    reads = [pltpu.make_async_copy(a, b, sem_in.at[i]) for i, (a, b) in enumerate(zip(ins, bufs))]
    writes = [pltpu.make_async_copy(b, a, sem_out.at[i]) for i, (a, b) in enumerate(zip(outs, bufs))]
    for c in reads:
        c.start()
    for r, w in zip(reads, writes):
        r.wait()
        w.start()
    for w in writes:
        w.wait()


def solution(mesh):
    dp, mp = mesh.shape["dp"], mesh.shape["mp"]
    Z, X = dp // 2, mp // 2

    def per_device(*args):
        _, rows, cols = args[0].shape
        q = rows // cols
        parts = min(PARTS, rows // 128)
        last_chunks = min(LAST, cols // 128)
        part, cw = rows // parts, cols // last_chunks
        pieces = sum(scatter_pieces(rows, cols, parts, last_chunks), [])
        n = len(pieces)
        out_b, y_b, z_b = [], [], []
        for _, _, nr, _, w, kind in pieces:
            lead = (2,) if kind == Z_FIRST else ()
            out_b.append(pltpu.VMEM((Z,) + lead + (nr, w), bf16))
            y_b.append(pltpu.VMEM((nr, w) if lead else (Z, nr, w), bf16))
            z_b.append(pltpu.VMEM((Z + 1,) + lead + (nr, w), bf16))
        flat = [a.reshape(a.shape[1:]) for a in args]
        dma = pltpu.SemaphoreType.DMA
        outs = pl.pallas_call(
            functools.partial(kernel, dp, mp, rows, cols, parts, last_chunks),
            out_shape=[jax.ShapeDtypeStruct((rows, cols), t) for t in (f32, f32, f32, f32, bf16)],
            in_specs=[pl.BlockSpec(memory_space=pl.ANY)] * 7,
            out_specs=[pl.BlockSpec(memory_space=pl.ANY)] * 5,
            scratch_shapes=[
                pltpu.VMEM((dp, rows, cols), bf16),
                pltpu.VMEM((parts, dp, cols, part), bf16),
                pltpu.VMEM((mp, rows, cols), bf16),
                pltpu.VMEM((mp, rows, cols), bf16),
                pltpu.VMEM((dp, cols, cols), bf16),
                pltpu.VMEM((last_chunks, dp, cols, cw), bf16),
                pltpu.VMEM((last_chunks, X, q, cols, cw), bf16),
                pltpu.VMEM((last_chunks, X - 1, q, cols, cw), bf16),
                pltpu.VMEM((last_chunks, X - 1, q, cols, cw), bf16),
                pltpu.VMEM((rows, cols), f32),
                pltpu.VMEM((rows, cols), f32),
                pltpu.VMEM((part, cols), f32),
                pltpu.VMEM((part, cols), f32),
                pltpu.VMEM((rows, cols), f32),
                pltpu.VMEM((rows, cols), bf16),
                pltpu.VMEM((rows, cols), bf16),
                dma((4 + 3 * parts,)),
                dma((3 + 2 * parts,)),
                dma((2 + parts, Z, 2)),
                dma((2 + parts, Z, 2)),
                dma((2 + parts, Z, 2)),
                dma((2 + parts, Z, 2)),
                dma((2 + parts, Z, 2)),
                dma((2 + parts, 2, 2)),
                dma((2 + parts, 2, 2)),
                dma((2, 2 * X)),
                dma((2, mp)),
                dma((X, q)),
                dma((X, q)),
                dma((X, q)),
                dma((X - 1, q)),
                dma((last_chunks, X, q)),
                dma((last_chunks, X, q)),
                dma((last_chunks, X, q)),
                dma((last_chunks, X - 1, q)),
                dma((2 + X,)),
                dma((2,)),
                dma((n, Z)),
                dma((n, Z)),
                dma((n, Z)),
                dma((n, Z + 1)),
            ] + out_b + y_b + z_b,
            compiler_params=pltpu.CompilerParams(
                collective_id=0, has_side_effects=True, vmem_limit_bytes=67043328
            ),
        )(*flat)
        kinds = [jax.ShapeDtypeStruct(o.shape, o.dtype) for o in outs]
        outs = pl.pallas_call(
            write_out,
            out_shape=kinds,
            in_specs=[pl.BlockSpec(memory_space=pl.ANY)] * len(outs),
            out_specs=[pl.BlockSpec(memory_space=pl.ANY)] * len(outs),
            scratch_shapes=[pltpu.VMEM(o.shape, o.dtype) for o in outs] + [dma((len(outs),)), dma((len(outs),))],
            compiler_params=pltpu.CompilerParams(vmem_limit_bytes=67043328),
        )(*outs)
        return tuple(o.reshape((1,) + o.shape) for o in outs)

    return jax.shard_map(
        per_device,
        mesh=mesh,
        in_specs=(P(None, "mp", "dp"),) * 5 + (P(None, "dp", "mp"), P(None, "mp", "dp")),
        out_specs=(P(None, "mp", "dp"),) * 5,
        check_vma=False,
    )
```

```python
import functools

import jax
import jax.numpy as jnp
from jax import lax
from jax.experimental import pallas as pl
from jax.experimental.pallas import tpu as pltpu
from jax.sharding import PartitionSpec as P

decay_moment = 0.95
decay_factor = 0.95
epsilon = 1e-08
bf16, f32 = jnp.bfloat16, jnp.float32
MESH = pl.DeviceIdType.MESH
PARTS, LAST, LAST_Z, EARLY = 2, 4, 1, 4
Y_FIRST, Z_FIRST = 0, 1


def scatter_pieces(rows, cols, parts, last_chunks):
    part = rows // parts
    out = [[] for _ in range(parts)]
    for p in range(parts - 1):
        out[p].append((p, 0, part // 2, 0, cols, Z_FIRST))
        out[p].append((p, part // 2, part // 2, 0, cols, Y_FIRST))
    for h in range(last_chunks):
        cw = cols // last_chunks
        out[parts - 1].append((parts - 1, 0, part, h * cw, cw, Z_FIRST if h < LAST_Z else Y_FIRST))
    return out


def kernel(dp, mp, rows, cols, parts, last_chunks, *refs):
    pieces = scatter_pieces(rows, cols, parts, last_chunks)
    first_piece = [sum(len(x) for x in pieces[:p]) for p in range(parts)]
    n_pieces = sum(len(x) for x in pieces)
    NAMED = len(refs) - 3 * n_pieces
    (grad, first, second, left_f, right_f, left_b, right_b,
     out_first, out_second, out_left, out_right, out_update,
     gbuf, lbuf, rbuf, rrbuf, pbuf, ssend, r1buf, r2buf, u2buf,
     fac_l, fac_r, mom1, mom2, acc, dbuf, bbuf,
     load_sem, store_sem, zs_up, zs_dn, zr, ys, yr, es, er, as_, ar,
     rs1, rr1, rs2, rr2, us1, ur1, us2, ur2, ps, pr, bys, byr, bzs, bzr) = refs[:NAMED]
    out_bufs = refs[NAMED:NAMED + n_pieces]
    y_bufs = refs[NAMED + n_pieces:NAMED + 2 * n_pieces]
    z_bufs = refs[NAMED + 2 * n_pieces:]
    u1buf = r1buf
    Z, q, X = dp // 2, rows // cols, mp // 2
    part, cw = rows // parts, cols // last_chunks
    d, m = lax.axis_index("dp"), lax.axis_index("mp")
    z, y = lax.div(d, 2), lax.rem(d, 2)
    core, chip = lax.rem(m, 2), lax.div(m, 2)
    partner = chip * 2 + (1 - core)
    last = Z - 1
    ynbr = z * 2 + (1 - y)
    tile = min(256, part)

    def send(src, dst, s, r, dev):
        return pltpu.make_async_remote_copy(
            src_ref=src, dst_ref=dst, send_sem=s, recv_sem=r, device_id=dev, device_id_type=MESH
        )

    def when(cond, fn):
        pl.when(cond)(fn)

    def loop(n, fn):
        def body(i, c):
            fn(i)
            return c
        lax.fori_loop(0, n, body, 0)

    def tiles(n, size, fn, base=0):
        loop(n // size, lambda i: fn(pl.ds(pl.multiple_of(base + i * size, size), size)))

    loads = [
        (grad, gbuf.at[d]), (right_b, rbuf.at[m]), (right_f, fac_r), (left_f, fac_l),
    ]
    loads += [(left_b.at[:, pl.ds(p * part, part)], lbuf.at[p, d]) for p in range(parts)]
    load = [pltpu.make_async_copy(a, b, load_sem.at[i]) for i, (a, b) in enumerate(loads)]
    for c in load:
        c.start()

    def part_rows(ref, p):
        return ref.at[pl.ds(p * part, part), :]

    def mom_loads(p):
        n = 4 + parts + 2 * p
        return [
            pltpu.make_async_copy(part_rows(a, p), b, load_sem.at[n + i])
            for i, (a, b) in enumerate([(first, mom1), (second, mom2)])
        ]

    def mom_stores(p):
        return [
            pltpu.make_async_copy(b, part_rows(a, p), store_sem.at[3 + 2 * p + i])
            for i, (a, b) in enumerate([(out_first, mom1), (out_second, mom2)])
        ]

    store_right = pltpu.make_async_copy(fac_r, out_right, store_sem.at[0])
    store_left = pltpu.make_async_copy(fac_l, out_left, store_sem.at[1])
    store_update = pltpu.make_async_copy(dbuf, out_update, store_sem.at[2])
    for c in mom_loads(0):
        c.start()

    barrier = pltpu.get_barrier_semaphore()
    pl.semaphore_signal(barrier, inc=1, device_id=(ynbr, m), device_id_type=MESH)
    when(z > 0, lambda: pl.semaphore_signal(barrier, inc=1, device_id=(d - 2, m), device_id_type=MESH))
    when(z < last, lambda: pl.semaphore_signal(barrier, inc=1, device_id=(d + 2, m), device_id_type=MESH))
    for k in range(1, mp):
        pl.semaphore_signal(barrier, inc=1, device_id=(d, lax.rem(m + k, mp)), device_id_type=MESH)
    along = (z > 0).astype(jnp.int32) + (z < last).astype(jnp.int32)
    pl.semaphore_wait(barrier, mp + along)

    def half(a, b, hb):
        if a < 2:
            return gbuf.at[b, pl.ds(a * (rows // 2) + hb * (rows // 4), rows // 4), :]
        return lbuf.at[a - 2, b, pl.ds(hb * (cols // 2), cols // 2), :]

    def up(a, zb, hb):
        blk = half(a, zb * 2 + y, hb)
        return send(blk, blk, zs_up.at[a, zb, hb], zr.at[a, zb, hb], (d + 2, m))

    def dn(a, zb, hb):
        blk = half(a, zb * 2 + y, hb)
        return send(blk, blk, zs_dn.at[a, zb, hb], zr.at[a, zb, hb], (d - 2, m))

    def ysend(a, zb, hb):
        blk = half(a, zb * 2 + y, hb)
        return send(blk, blk, ys.at[a, zb, hb], yr.at[a, zb, hb], (ynbr, m))

    def yrecv_desc(a, zb, hb):
        blk = half(a, zb * 2 + (1 - y), hb)
        return send(blk, blk, ys.at[a, zb, hb], yr.at[a, zb, hb], (ynbr, m))

    def by_line(a):
        return (1,)

    def extra(a, k, hb):
        zb = 0 if k == 0 else last
        blk = half(a, zb * 2 + (1 - y), hb)
        return send(blk, blk, es.at[a, k, hb], er.at[a, k, hb], (d + 2, m) if k == 0 else (d - 2, m))

    def over_y(a, zb, hb):
        inner = jnp.logical_and(zb > 0, zb < last)
        return jnp.logical_or(zb == z, inner)

    def y_sends(a, zb, op):
        for hb in (1, 0):
            if hb in by_line(a):
                when(over_y(a, zb, hb), lambda hb=hb: op(ysend(a, zb, hb)))
            else:
                op(ysend(a, zb, hb))

    def start(c):
        c.start()

    def ag_own(a):
        for hb in range(2):
            when(z < last, lambda: up(a, z, hb).start())
            when(z > 0, lambda: dn(a, z, hb).start())

    def ag_step(a, s, then=None):
        below, above = z - s, z + s

        def from_below():
            for hb in range(2):
                up(a, below, hb).wait_recv()
                when(z < last, lambda hb=hb: up(a, below, hb).start())

        def from_above():
            for hb in range(2):
                dn(a, above, hb).wait_recv()
                when(z > 0, lambda hb=hb: dn(a, above, hb).start())

        when(below >= 0, from_below)
        when(above <= last, from_above)
        when(below >= 0, lambda: y_sends(a, below, start))
        when(above <= last, lambda: y_sends(a, above, start))

        def extra_dn():
            for hb in by_line(a):
                when(z == last, lambda hb=hb: yrecv_desc(a, z, hb).wait_recv())
                when(z < last, lambda hb=hb: extra(a, 1, hb).wait_recv())
                extra(a, 1, hb).start()
            if then is not None:
                for hb in range(2):
                    dn(then, z, hb).start()

        def extra_up():
            for hb in by_line(a):
                when(z == 0, lambda hb=hb: yrecv_desc(a, z, hb).wait_recv())
                when(z > 0, lambda hb=hb: extra(a, 0, hb).wait_recv())
                extra(a, 0, hb).start()
            if then is not None:
                for hb in range(2):
                    up(then, z, hb).start()

        when(jnp.logical_and(z == Z - s, z > 0), extra_dn)
        when(jnp.logical_and(z == s - 1, z < last), extra_up)

    def wait_y(a, zb):
        inner = jnp.logical_and(zb > 0, zb < last)
        for hb in range(2):
            if hb in by_line(a):
                when(inner, lambda hb=hb: yrecv_desc(a, zb, hb).wait_recv())
                when(jnp.logical_and(zb == last, z == 0), lambda hb=hb: extra(a, 1, hb).wait_recv())
                when(jnp.logical_and(zb == 0, z == last), lambda hb=hb: extra(a, 0, hb).wait_recv())
            else:
                yrecv_desc(a, zb, hb).wait_recv()

    def at_distance(s, fn):
        def side(j):
            zb = z + (2 * j - 1) * s
            ok = jnp.logical_and(zb >= 0, zb <= last)
            when(jnp.logical_and(ok, jnp.logical_or(s > 0, j == 0)), lambda: fn(zb))
        loop(2, side)

    def by_distance(fn, far_first=False):
        loop(Z, lambda i: at_distance(last - i if far_first else i, fn))

    def sub_rows(ref, db):
        off = pl.multiple_of(lax.rem(db, q) * cols, cols)
        return ref.at[lax.div(db, q), pl.ds(off, cols), :]

    def mp_copy(a, buf, src, k, to):
        return send(buf.at[src], buf.at[src], as_.at[a, k], ar.at[a, src], (d, to))

    def mp_first(a, buf, op):
        for k in range(1, X):
            op(mp_copy(a, buf, m, X + k, lax.rem(chip + k, X) * 2 + core))
        op(mp_copy(a, buf, m, 0, partner))

    def mp_relay(a, buf):
        for k in range(1, X):
            src = lax.rem(chip + k, X) * 2 + core
            mp_copy(a, buf, src, k, partner).wait_recv()
            mp_copy(a, buf, src, k, partner).start()

    def mp_wait(a, buf):
        for k in range(X):
            src = lax.rem(chip + k, X) * 2 + 1 - core
            mp_copy(a, buf, src, k, partner).wait_recv()

    def mp_sent(a, buf):
        mp_first(a, buf, lambda c: c.wait_send())
        for k in range(1, X):
            mp_copy(a, buf, lax.rem(chip + k, X) * 2 + core, k, partner).wait_send()

    load[0].wait()
    for a in range(2):
        ag_own(a)
        y_sends(a, z, start)
    load[1].wait()
    mp_first(0, rbuf, start)
    for p in range(parts):
        load[4 + p].wait()

    def far_slot(k):
        return lax.rem(k + X, X) - 1

    def r_near(db):
        xb, sub = lax.div(db, 2 * q), lax.rem(db, q)
        return send(ssend.at[:, db], r1buf.at[:, xb, sub], rs1.at[xb, sub], rr1.at[xb, sub], (d, partner))

    def r_far(db):
        xb, sub = lax.div(db, 2 * q), lax.rem(db, q)
        slot = far_slot(chip - xb)
        return send(ssend.at[:, db], r2buf.at[:, slot, sub], rs2.at[xb, sub], rr2.at[slot, sub], (d, xb * 2 + core))

    def r_term(db):
        xb, sub = lax.div(db, 2 * q), lax.rem(db, q)
        mine = lax.rem(lax.div(db, q), 2) == core

        def one(t):
            term = lax.dot_general(
                gbuf[db, :, t], gbuf[d], (((0,), (0,)), ((), ())), preferred_element_type=f32
            )
            for h in range(last_chunks):
                ssend[h, db, t, :] = term[:, h * cw:(h + 1) * cw].astype(bf16)
        tiles(cols, min(256, cols), one)

        def add():
            got = r1buf.at[:, xb, sub]
            send(got, got, rs1.at[0, 0], rr1.at[xb, sub], (d, partner)).wait_recv()
            for h in range(last_chunks):
                ssend[h, db] = (ssend[h, db].astype(f32) + r1buf[h, xb, sub].astype(f32)).astype(bf16)
            when(xb != chip, lambda: r_far(db).start())
        when(jnp.logical_not(mine), lambda: r_near(db).start())
        when(mine, add)

    def rr_term(db):
        rhs = sub_rows(rbuf, db)
        def one(t):
            acc[t, :] += jnp.dot(gbuf[db, t, :], rhs[...], preferred_element_type=f32)
        tiles(rows, tile, one)

    def zero_acc():
        def one(t):
            acc[t, :] = jnp.zeros((tile, cols), f32)
        tiles(rows, tile, one)

    r_term(d)

    def g_step(i):
        s = i + 1
        ag_step(0, s)
        ag_step(1, s, then=2)
        when(s == min(2, last), lambda: mp_relay(0, rbuf))
        at_distance(s, lambda zb: r_term(zb * 2 + y))
    loop(Z - 1, g_step)
    y_sends(2, z, start)
    zero_acc()
    mp_wait(0, rbuf)
    by_distance(lambda zb: rr_term(zb * 2 + y))

    def y_block(zb):
        wait_y(0, zb)
        wait_y(1, zb)
        rr_term(zb * 2 + 1 - y)
    by_distance(y_block)

    def rr_out(t):
        rrbuf[m, t, :] = acc[t, :].astype(bf16)
    tiles(rows, tile, rr_out)
    mp_first(1, rrbuf, start)
    zero_acc()

    owner = lax.div(d, q)
    own_chip = lax.div(owner, 2)
    hd = dp // 2
    pair_off = pl.multiple_of(lax.rem(d, q) * cols, cols)

    def p_send(hb, i, to):
        view_p = pbuf.at[pl.ds(hb * hd, hd)]
        return send(view_p, view_p, ps.at[i], pr.at[hb], (d, to))

    def to_chips(op):
        for k in range(1, X):
            op(p_send(core, 2 + k, lax.rem(chip + k, X) * 2 + core))

    def own_pair():
        def copy(i):
            pbuf[i] = gbuf[i, pl.ds(pair_off, cols), :]
        loop(dp, copy)
        for hb in range(2):
            p_send(hb, hb, partner).start()
        to_chips(start)

    def near_pair():
        for hb in range(2):
            p_send(hb, hb, partner).wait_recv()
        to_chips(start)

    def far_relay():
        p_send(core, 0, partner).wait_recv()
        p_send(core, 0, partner).start()

    def far_pair():
        p_send(1 - core, 0, partner).wait_recv()

    when(m == owner, own_pair)

    def back_term(db, piece, t):
        p, r0, _, c0, w, _ = piece
        off = pl.multiple_of(lax.rem(db, q) * cols + c0, 128)
        rhs = rbuf[lax.div(db, q), pl.ds(off, w), :]
        mine = pl.ds(pl.multiple_of(t.start + (p * part + r0), t.size), t.size)
        return lax.dot_general(
            dbuf[mine, :], rhs, (((1,), (1,)), ((), ())), preferred_element_type=f32
        )

    def piece_tiles(piece, fn):
        tiles(piece[2], min(256, piece[2]), fn)

    def by_send(i, zb):
        return send(out_bufs[i].at[zb], y_bufs[i].at[zb], bys.at[i, zb], byr.at[i, zb], (ynbr, m))

    def by_last(i):
        return send(out_bufs[i].at[z, 1 - y], y_bufs[i], bys.at[i, 0], byr.at[i, 0], (ynbr, m))

    def bz_up(i, zb, src):
        return send(src.at[zb], z_bufs[i].at[zb], bzs.at[i, zb], bzr.at[i, zb], (d + 2, m))

    def bz_dn(i, zb, src):
        slot = jnp.where(zb == z - 1, Z, zb)
        return send(src.at[zb], z_bufs[i].at[slot], bzs.at[i, zb], bzr.at[i, slot], (d - 2, m))

    def z_arrivals(i, zb, add):
        def one(slot):
            dst = z_bufs[i].at[slot]
            send(dst, dst, bzs.at[i, 0], bzr.at[i, slot], (ynbr, m)).wait_recv()
            add(slot)
        when(jnp.logical_and(zb >= z, z > 0), lambda: one(zb))
        when(jnp.logical_and(zb < z, z < last), lambda: one(zb))
        when(jnp.logical_and(zb == z, z < last), lambda: one(Z))

    def z_send(i, zb, src):
        when(zb > z, lambda: bz_up(i, zb, src).start())
        when(zb < z, lambda: bz_dn(i, zb, src).start())

    def to_back(piece, t, value):
        p, r0, _, c0, w, _ = piece
        mine = pl.ds(pl.multiple_of(t.start + (p * part + r0), t.size), t.size)
        bbuf[mine, pl.ds(c0, w)] = value.astype(bf16)

    def line_y_first(i, piece, zb):
        c = pl.ds(0, piece[4])
        by_send(i, zb).wait_recv()

        def one(t):
            acc[t, c] = back_term(zb * 2 + y, piece, t) + y_bufs[i][zb, t, :].astype(f32)
        piece_tiles(piece, one)

        def add(slot):
            def more(t):
                acc[t, c] += z_bufs[i][slot, t, :].astype(f32)
            piece_tiles(piece, more)
        z_arrivals(i, zb, add)

        def pack(t):
            y_bufs[i][zb, t, :] = acc[t, c].astype(bf16)
        when(zb != z, lambda: piece_tiles(piece, pack))
        z_send(i, zb, y_bufs[i])
        when(zb == z, lambda: piece_tiles(piece, lambda t: to_back(piece, t, acc[t, c])))

    def line_z_first(i, piece, zb):
        n = piece[2]

        def rows_of(t, yy):
            return pl.ds(pl.multiple_of(t.start + yy * n, t.size), t.size)
        for yy in range(2):
            def one(t, yy=yy):
                acc[rows_of(t, yy), pl.ds(0, piece[4])] = back_term(zb * 2 + yy, piece, t)
            piece_tiles(piece, one)

        def add(slot):
            for yy in range(2):
                def more(t, yy=yy):
                    acc[rows_of(t, yy), pl.ds(0, piece[4])] += z_bufs[i][slot, yy, t, :].astype(f32)
                piece_tiles(piece, more)
        z_arrivals(i, zb, add)
        for yy in range(2):
            def pack(t, yy=yy):
                out_bufs[i][zb, yy, t, :] = acc[rows_of(t, yy), pl.ds(0, piece[4])].astype(bf16)
            piece_tiles(piece, pack)
        z_send(i, zb, out_bufs[i])
        when(zb == z, lambda: by_last(i).start())

    def finish_z_first(i, piece):
        by_last(i).wait_recv()

        def one(t):
            mine = out_bufs[i][z, y, t, :].astype(f32) + y_bufs[i][t, :].astype(f32)
            to_back(piece, t, mine)
        piece_tiles(piece, one)

    def numbered(p):
        return list(enumerate(pieces[p], first_piece[p]))

    def scatter_first(p):
        groups = []
        for i, piece in numbered(p):
            if piece[5] == Z_FIRST:
                if p == parts - 1:
                    scatter_step(i, piece, last)
            elif len(groups) > 1 and len(groups[-1]) == 1:
                groups[-1].append((i, piece))
            else:
                groups.append([(i, piece)])
        for group in groups:
            p0, r0, nr, c0, w, kind = group[0][1]
            both = (p0, r0, nr, c0, w * len(group), kind)

            def one_block(zb, group=group, both=both, w=w):
                def one(t):
                    value = back_term(zb * 2 + 1 - y, both, t).astype(bf16)
                    for j, (i, _) in enumerate(group):
                        out_bufs[i][zb, t, :] = value[:, j * w:(j + 1) * w]
                piece_tiles(both, one)
                by_send(group[0][0], zb).start()
            by_distance(one_block, far_first=True)
            for i, _ in group[1:]:
                by_distance(lambda zb, i=i: by_send(i, zb).start(), far_first=True)

    def scatter_step(i, piece, s):
        fn = line_z_first if piece[5] == Z_FIRST else line_y_first
        at_distance(s, lambda zb: fn(i, piece, zb))

    mom_tile = min(128, part)

    def m_term(p, db):
        rhs = sub_rows(rrbuf, db)
        def one(t):
            acc[t, :] += lax.dot_general(
                lbuf[p, db, :, t], rhs[...], (((0,), (0,)), ((), ())), preferred_element_type=f32
            )
        tiles(part, tile, one)

    def zero_part():
        def one(t):
            acc[t, :] = jnp.zeros((tile, cols), f32)
        tiles(part, tile, one)

    def moments(p):
        def one(t):
            w = pl.ds(pl.multiple_of(t.start + p * part, mom_tile), mom_tile)
            rot = acc[t, :]
            new1 = decay_moment * mom1[t, :] + (1.0 - decay_moment) * rot
            new2 = decay_moment * mom2[t, :] + (1.0 - decay_moment) * rot * rot
            mom1[t, :] = new1
            mom2[t, :] = new2
            dbuf[w, :] = (new1 / (jnp.sqrt(new2) + epsilon)).astype(bf16)
        tiles(part, mom_tile, one)

    def direction(p):
        def y_part(zb):
            wait_y(2 + p, zb)
            m_term(p, zb * 2 + 1 - y)
        by_distance(y_part)
        for c in mom_loads(p):
            c.wait()
        moments(p)
        for c in mom_stores(p):
            c.start()

    def r_y_terms(near):
        def one(zb):
            db = zb * 2 + 1 - y
            mine = lax.rem(lax.div(db, q), 2) == core
            when(jnp.logical_xor(mine, near), lambda: r_term(db))
        by_distance(one)

    def l_step(i):
        s = i + 1
        when(s == last, lambda: mp_relay(1, rrbuf))
        ag_step(2, s, then=3 if parts > 1 else None)
        when(jnp.logical_and(s == min(2, last), jnp.logical_and(chip == own_chip, m != owner)), near_pair)
        when(s == 1, lambda: r_y_terms(True))
        when(s == min(2, last), lambda: r_y_terms(False))
    loop(Z - 1, l_step)
    if parts > 1:
        y_sends(3, z, start)
    mp_wait(1, rrbuf)
    by_distance(lambda zb: m_term(0, zb * 2 + y))
    direction(0)
    scatter_first(0)

    def r_final():
        for sub in range(q):
            for k in range(1, X):
                got = r2buf.at[:, k - 1, sub]
                send(got, got, rs1.at[0, 0], rr2.at[k - 1, sub], (d, partner)).wait_recv()
            for h in range(last_chunks):
                def one(t, sub=sub, h=h):
                    total = ssend[h, m * q + sub, t, :].astype(f32)
                    for k in range(1, X):
                        total += r2buf[h, k - 1, sub, t, :].astype(f32)
                    where = pl.ds(pl.multiple_of(sub * cols + t.start, 128), 128)
                    c = pl.ds(h * cw, cw)
                    fac_r[where, c] = decay_factor * fac_r[where, c] + (1.0 - decay_factor) * total
                tiles(cols, 128, one)

    def l_scale(t):
        fac_l[t, :] = decay_factor * fac_l[t, :]
    load[2].wait()
    load[3].wait()
    tiles(rows, tile, l_scale)

    def l_term(db):
        def one(t):
            fac_l[t, :] += (1.0 - decay_factor) * lax.dot_general(
                gbuf[db, t, :], pbuf[db], (((1,), (1,)), ((), ())), preferred_element_type=f32
            )
        tiles(rows, tile, one)

    for p in range(1, parts):
        def both(i, p=p):
            s = i + 1
            if p == 1:
                when(jnp.logical_and(s == last, chip != own_chip), far_relay)
            ag_step(2 + p, s, then=3 + p if p + 1 < parts else None)
            for j, piece in numbered(p - 1):
                scatter_step(j, piece, Z - s)
        loop(Z - 1, both)
        if p + 1 < parts:
            y_sends(3 + p, z, start)
        if p == 1:
            r_final()
            store_right.start()
            when(chip != own_chip, far_pair)
            when(jnp.logical_or(z == 0, z == last), lambda: loop(EARLY, l_term))
        for j, piece in numbered(p - 1):
            scatter_step(j, piece, 0)
        zero_part()
        for c in mom_stores(p - 1):
            c.wait()
        for c in mom_loads(p):
            c.start()
        by_distance(lambda zb, p=p: m_term(p, zb * 2 + y))
        direction(p)
        scatter_first(p)
        for j, piece in numbered(p - 1):
            if piece[5] == Z_FIRST:
                finish_z_first(j, piece)

    def r_sent(db):
        mine = lax.rem(lax.div(db, q), 2) == core
        when(jnp.logical_not(mine), lambda: r_near(db).wait_send())
        when(jnp.logical_and(mine, lax.div(db, 2 * q) != chip), lambda: r_far(db).wait_send())
    loop(dp, r_sent)

    def u_near(h, xb, sub):
        db = (xb * 2 + 1 - core) * q + sub
        return send(
            ssend.at[h, db], u1buf.at[h, xb, sub], us1.at[h, xb, sub], ur1.at[h, xb, sub], (d, partner)
        )

    def u_far(h, xb, sub):
        db = (xb * 2 + core) * q + sub
        slot = far_slot(chip - xb)
        return send(
            ssend.at[h, db], u2buf.at[h, slot, sub], us2.at[h, xb, sub], ur2.at[h, slot, sub], (d, xb * 2 + core)
        )

    def u_got(dst, sem):
        send(dst, dst, us1.at[0, 0, 0], sem, (d, partner)).wait_recv()

    def u_dot(h, db):
        c = pl.ds(h * cw, cw)
        p = parts - 1
        term = jnp.dot(lbuf[p, db], bbuf[pl.ds(p * part, part), c], preferred_element_type=f32)
        return ssend[h, db].astype(f32) + term

    def u_before():
        def one(db):
            for h0 in range(0, last_chunks, 2):
                c = pl.ds(h0 * cw, 2 * cw)
                total = None
                for p in range(parts - 1):
                    term = jnp.dot(lbuf[p, db], bbuf[pl.ds(p * part, part), c], preferred_element_type=f32)
                    total = term if total is None else total + term
                for h in range(2):
                    ssend[h0 + h, db] = total[:, h * cw:(h + 1) * cw].astype(bf16)
        loop(dp, one)

    def u_terms(h):
        def near(i):
            xb, sub = lax.rem(chip + 1 + lax.div(i, q), X), lax.rem(i, q)
            db = (xb * 2 + 1 - core) * q + sub
            ssend[h, db] = u_dot(h, db).astype(bf16)
            u_near(h, xb, sub).start()
        loop(X * q, near)

        def far(i):
            xb, sub = lax.rem(chip + 1 + lax.div(i, q), X), lax.rem(i, q)
            db = (xb * 2 + core) * q + sub
            mine = u_dot(h, db)
            u_got(u1buf.at[h, xb, sub], ur1.at[h, xb, sub])
            ssend[h, db] = (mine + u1buf[h, xb, sub].astype(f32)).astype(bf16)
            when(xb != chip, lambda: u_far(h, xb, sub).start())
        loop(X * q, far)

    def u_final(h):
        c = pl.ds(h * cw, cw)
        for sub in range(q):
            for k in range(1, X):
                u_got(u2buf.at[h, k - 1, sub], ur2.at[h, k - 1, sub])

            def one(t, sub=sub):
                total = ssend[h, m * q + sub, t, :].astype(f32)
                for k in range(1, X):
                    total += u2buf[h, k - 1, sub, t, :].astype(f32)
                where = pl.ds(pl.multiple_of(sub * cols + t.start, 128), 128)
                dbuf[where, c] = total.astype(bf16)
            tiles(cols, 128, one)

    done = EARLY
    wide = numbered(parts - 1)
    steady = [i for i, piece in wide if piece[5] == Y_FIRST]
    taus = len(steady) + Z - 1
    per = -(-(dp - EARLY) // (taus - 1))

    def when_due(i, piece, t):
        if piece[5] == Y_FIRST:
            return steady.index(i) + last - t
        return ((last - t) * (taus - 3) * 2 + last) // (2 * last)

    for tau in range(taus):
        for h, (i, piece) in enumerate(wide):
            for t in range(last, 0, -1):
                if when_due(i, piece, t) == tau and not (piece[5] == Z_FIRST and t == last):
                    scatter_step(i, piece, t)
        if tau == 1:
            u_before()
        if tau == 2:
            when(jnp.logical_and(z > 0, z < last), lambda: loop(EARLY, l_term))
        for h, (i, piece) in enumerate(wide):
            z_first = piece[5] == Z_FIRST
            if z_first and tau == when_due(i, piece, 0) + 1:
                finish_z_first(i, piece)
                u_terms(h)
            if when_due(i, piece, 0) == tau:
                scatter_step(i, piece, 0)
                if not z_first:
                    u_terms(h)
        if done < dp:
            loop(min(per, dp - done), lambda k, done=done: l_term(done + k))
            done = min(done + per, dp)
            if done == dp:
                store_left.start()
    for h in range(last_chunks):
        u_final(h)
    store_update.start()

    for a in range(2 + parts):
        def sent(i, a=a):
            for hb in range(2):
                when(jnp.logical_and(z < last, i <= z), lambda: up(a, i, hb).wait_send())
                when(jnp.logical_and(z > 0, i >= z), lambda: dn(a, i, hb).wait_send())
            y_sends(a, i, lambda c: c.wait_send())
        loop(Z, sent)
        for hb in by_line(a):
            when(z > 0, lambda: extra(a, 1, hb).wait_send())
            when(z < last, lambda: extra(a, 0, hb).wait_send())
    mp_sent(0, rbuf)
    mp_sent(1, rrbuf)

    def near_sent():
        to_chips(lambda c: c.wait_send())
    when(chip == own_chip, near_sent)

    def own_sent():
        for hb in range(2):
            p_send(hb, hb, partner).wait_send()
    when(m == owner, own_sent)
    when(chip != own_chip, lambda: p_send(core, 0, partner).wait_send())
    def line_sent(i, piece):
        src = out_bufs[i] if piece[5] == Z_FIRST else y_bufs[i]

        def one(zb):
            if piece[5] == Y_FIRST:
                by_send(i, zb).wait_send()
            when(zb != z, lambda: bz_up(i, zb, src).wait_send())
        loop(Z, one)
        if piece[5] == Z_FIRST:
            by_last(i).wait_send()
    for p in range(parts):
        for i, piece in numbered(p):
            line_sent(i, piece)
    for h in range(last_chunks):
        for sub in range(q):
            for xb in range(X):
                u_near(h, xb, sub).wait_send()
                when(xb != chip, lambda h=h, xb=xb, sub=sub: u_far(h, xb, sub).wait_send())
    for c in mom_stores(parts - 1) + [store_left, store_right, store_update]:
        c.wait()


def write_out(*refs):
    n = (len(refs) - 2) // 3
    ins, outs, bufs, sem_in, sem_out = refs[:n], refs[n:2 * n], refs[2 * n:-2], refs[-2], refs[-1]
    reads = [pltpu.make_async_copy(a, b, sem_in.at[i]) for i, (a, b) in enumerate(zip(ins, bufs))]
    writes = [pltpu.make_async_copy(b, a, sem_out.at[i]) for i, (a, b) in enumerate(zip(outs, bufs))]
    for c in reads:
        c.start()
    for r, w in zip(reads, writes):
        r.wait()
        w.start()
    for w in writes:
        w.wait()


def solution(mesh):
    dp, mp = mesh.shape["dp"], mesh.shape["mp"]
    Z, X = dp // 2, mp // 2

    def per_device(*args):
        _, rows, cols = args[0].shape
        q = rows // cols
        parts = min(PARTS, rows // 128)
        last_chunks = min(LAST, cols // 128)
        part, cw = rows // parts, cols // last_chunks
        pieces = sum(scatter_pieces(rows, cols, parts, last_chunks), [])
        n = len(pieces)
        out_b, y_b, z_b = [], [], []
        for _, _, nr, _, w, kind in pieces:
            lead = (2,) if kind == Z_FIRST else ()
            out_b.append(pltpu.VMEM((Z,) + lead + (nr, w), bf16))
            y_b.append(pltpu.VMEM((nr, w) if lead else (Z, nr, w), bf16))
            z_b.append(pltpu.VMEM((Z + 1,) + lead + (nr, w), bf16))
        flat = [a.reshape(a.shape[1:]) for a in args]
        dma = pltpu.SemaphoreType.DMA
        outs = pl.pallas_call(
            functools.partial(kernel, dp, mp, rows, cols, parts, last_chunks),
            out_shape=[jax.ShapeDtypeStruct((rows, cols), t) for t in (f32, f32, f32, f32, bf16)],
            in_specs=[pl.BlockSpec(memory_space=pl.ANY)] * 7,
            out_specs=[pl.BlockSpec(memory_space=pl.ANY)] * 5,
            scratch_shapes=[
                pltpu.VMEM((dp, rows, cols), bf16),
                pltpu.VMEM((parts, dp, cols, part), bf16),
                pltpu.VMEM((mp, rows, cols), bf16),
                pltpu.VMEM((mp, rows, cols), bf16),
                pltpu.VMEM((dp, cols, cols), bf16),
                pltpu.VMEM((last_chunks, dp, cols, cw), bf16),
                pltpu.VMEM((last_chunks, X, q, cols, cw), bf16),
                pltpu.VMEM((last_chunks, X - 1, q, cols, cw), bf16),
                pltpu.VMEM((last_chunks, X - 1, q, cols, cw), bf16),
                pltpu.VMEM((rows, cols), f32),
                pltpu.VMEM((rows, cols), f32),
                pltpu.VMEM((part, cols), f32),
                pltpu.VMEM((part, cols), f32),
                pltpu.VMEM((rows, cols), f32),
                pltpu.VMEM((rows, cols), bf16),
                pltpu.VMEM((rows, cols), bf16),
                dma((4 + 3 * parts,)),
                dma((3 + 2 * parts,)),
                dma((2 + parts, Z, 2)),
                dma((2 + parts, Z, 2)),
                dma((2 + parts, Z, 2)),
                dma((2 + parts, Z, 2)),
                dma((2 + parts, Z, 2)),
                dma((2 + parts, 2, 2)),
                dma((2 + parts, 2, 2)),
                dma((2, 2 * X)),
                dma((2, mp)),
                dma((X, q)),
                dma((X, q)),
                dma((X, q)),
                dma((X - 1, q)),
                dma((last_chunks, X, q)),
                dma((last_chunks, X, q)),
                dma((last_chunks, X, q)),
                dma((last_chunks, X - 1, q)),
                dma((2 + X,)),
                dma((2,)),
                dma((n, Z)),
                dma((n, Z)),
                dma((n, Z)),
                dma((n, Z + 1)),
            ] + out_b + y_b + z_b,
            compiler_params=pltpu.CompilerParams(
                collective_id=0, has_side_effects=True, vmem_limit_bytes=67043328
            ),
        )(*flat)
        kinds = [jax.ShapeDtypeStruct(o.shape, o.dtype) for o in outs]
        outs = pl.pallas_call(
            write_out,
            out_shape=kinds,
            in_specs=[pl.BlockSpec(memory_space=pl.ANY)] * len(outs),
            out_specs=[pl.BlockSpec(memory_space=pl.ANY)] * len(outs),
            scratch_shapes=[pltpu.VMEM(o.shape, o.dtype) for o in outs] + [dma((len(outs),)), dma((len(outs),))],
            compiler_params=pltpu.CompilerParams(vmem_limit_bytes=67043328),
        )(*outs)
        return tuple(o.reshape((1,) + o.shape) for o in outs)

    return jax.shard_map(
        per_device,
        mesh=mesh,
        in_specs=(P(None, "mp", "dp"),) * 5 + (P(None, "dp", "mp"), P(None, "mp", "dp")),
        out_specs=(P(None, "mp", "dp"),) * 5,
        check_vma=False,
    )
```

```python
import functools

import jax
import jax.numpy as jnp
from jax import lax
from jax.experimental import pallas as pl
from jax.experimental.pallas import tpu as pltpu
from jax.sharding import PartitionSpec as P

decay_moment = 0.95
decay_factor = 0.95
epsilon = 1e-08
bf16, f32 = jnp.bfloat16, jnp.float32
MESH = pl.DeviceIdType.MESH
PARTS, LAST, LAST_Z, EARLY = 2, 4, 1, 4
Y_FIRST, Z_FIRST = 0, 1
PIECE_US, HOP_US, CHAIN_US, Z_HOP_US, L_FROM = 11, 3, 8, 8, 3


def scatter_pieces(rows, cols, parts, last_chunks):
    part = rows // parts
    out = [[] for _ in range(parts)]
    for p in range(parts - 1):
        out[p].append((p, 0, part // 2, 0, cols, Z_FIRST))
        out[p].append((p, part // 2, part // 2, 0, cols, Y_FIRST))
    for h in range(last_chunks):
        cw = cols // last_chunks
        out[parts - 1].append((parts - 1, 0, part, h * cw, cw, Z_FIRST if h < LAST_Z else Y_FIRST))
    return out


def kernel(dp, mp, rows, cols, parts, last_chunks, *refs):
    pieces = scatter_pieces(rows, cols, parts, last_chunks)
    first_piece = [sum(len(x) for x in pieces[:p]) for p in range(parts)]
    n_pieces = sum(len(x) for x in pieces)
    NAMED = len(refs) - 3 * n_pieces
    (grad, first, second, left_f, right_f, left_b, right_b,
     out_first, out_second, out_left, out_right, out_update,
     gbuf, lbuf, rbuf, rrbuf, pbuf, ssend, r1buf, r2buf, u2buf,
     fac_l, fac_r, mom1, mom2, acc, dbuf, bbuf,
     load_sem, store_sem, zs_up, zs_dn, zr, ys, yr, es, er, as_, ar,
     rs1, rr1, rs2, rr2, us1, ur1, us2, ur2, ps, pr, bys, byr, bzs, bzr) = refs[:NAMED]
    out_bufs = refs[NAMED:NAMED + n_pieces]
    y_bufs = refs[NAMED + n_pieces:NAMED + 2 * n_pieces]
    z_bufs = refs[NAMED + 2 * n_pieces:]
    u1buf = r1buf
    Z, q, X = dp // 2, rows // cols, mp // 2
    part, cw = rows // parts, cols // last_chunks
    d, m = lax.axis_index("dp"), lax.axis_index("mp")
    z, y = lax.div(d, 2), lax.rem(d, 2)
    core, chip = lax.rem(m, 2), lax.div(m, 2)
    partner = chip * 2 + (1 - core)
    last = Z - 1
    ynbr = z * 2 + (1 - y)
    tile = min(256, part)

    def send(src, dst, s, r, dev):
        return pltpu.make_async_remote_copy(
            src_ref=src, dst_ref=dst, send_sem=s, recv_sem=r, device_id=dev, device_id_type=MESH
        )

    def when(cond, fn):
        pl.when(cond)(fn)

    def loop(n, fn):
        def body(i, c):
            fn(i)
            return c
        lax.fori_loop(0, n, body, 0)

    def tiles(n, size, fn, base=0):
        loop(n // size, lambda i: fn(pl.ds(pl.multiple_of(base + i * size, size), size)))

    loads = [
        (grad, gbuf.at[d]), (right_b, rbuf.at[m]), (right_f, fac_r), (left_f, fac_l),
    ]
    loads += [(left_b.at[:, pl.ds(p * part, part)], lbuf.at[p, d]) for p in range(parts)]
    load = [pltpu.make_async_copy(a, b, load_sem.at[i]) for i, (a, b) in enumerate(loads)]
    for c in load:
        c.start()

    def part_rows(ref, p):
        return ref.at[pl.ds(p * part, part), :]

    def mom_loads(p):
        n = 4 + parts + 2 * p
        return [
            pltpu.make_async_copy(part_rows(a, p), b, load_sem.at[n + i])
            for i, (a, b) in enumerate([(first, mom1), (second, mom2)])
        ]

    def mom_stores(p):
        return [
            pltpu.make_async_copy(b, part_rows(a, p), store_sem.at[3 + 2 * p + i])
            for i, (a, b) in enumerate([(out_first, mom1), (out_second, mom2)])
        ]

    store_right = pltpu.make_async_copy(fac_r, out_right, store_sem.at[0])
    store_left = pltpu.make_async_copy(fac_l, out_left, store_sem.at[1])
    store_update = pltpu.make_async_copy(dbuf, out_update, store_sem.at[2])
    for c in mom_loads(0):
        c.start()

    barrier = pltpu.get_barrier_semaphore()
    pl.semaphore_signal(barrier, inc=1, device_id=(ynbr, m), device_id_type=MESH)
    when(z > 0, lambda: pl.semaphore_signal(barrier, inc=1, device_id=(d - 2, m), device_id_type=MESH))
    when(z < last, lambda: pl.semaphore_signal(barrier, inc=1, device_id=(d + 2, m), device_id_type=MESH))
    for k in range(1, mp):
        pl.semaphore_signal(barrier, inc=1, device_id=(d, lax.rem(m + k, mp)), device_id_type=MESH)
    along = (z > 0).astype(jnp.int32) + (z < last).astype(jnp.int32)
    pl.semaphore_wait(barrier, mp + along)

    def half(a, b, hb):
        if a < 2:
            return gbuf.at[b, pl.ds(a * (rows // 2) + hb * (rows // 4), rows // 4), :]
        return lbuf.at[a - 2, b, pl.ds(hb * (cols // 2), cols // 2), :]

    def up(a, zb, hb):
        blk = half(a, zb * 2 + y, hb)
        return send(blk, blk, zs_up.at[a, zb, hb], zr.at[a, zb, hb], (d + 2, m))

    def dn(a, zb, hb):
        blk = half(a, zb * 2 + y, hb)
        return send(blk, blk, zs_dn.at[a, zb, hb], zr.at[a, zb, hb], (d - 2, m))

    def ysend(a, zb, hb):
        blk = half(a, zb * 2 + y, hb)
        return send(blk, blk, ys.at[a, zb, hb], yr.at[a, zb, hb], (ynbr, m))

    def yrecv_desc(a, zb, hb):
        blk = half(a, zb * 2 + (1 - y), hb)
        return send(blk, blk, ys.at[a, zb, hb], yr.at[a, zb, hb], (ynbr, m))

    def by_line(a):
        return (1,)

    def extra(a, k, hb):
        zb = 0 if k == 0 else last
        blk = half(a, zb * 2 + (1 - y), hb)
        return send(blk, blk, es.at[a, k, hb], er.at[a, k, hb], (d + 2, m) if k == 0 else (d - 2, m))

    def over_y(a, zb, hb):
        inner = jnp.logical_and(zb > 0, zb < last)
        return jnp.logical_or(zb == z, inner)

    def y_half(a, zb, hb, op):
        if hb in by_line(a):
            when(over_y(a, zb, hb), lambda: op(ysend(a, zb, hb)))
        else:
            op(ysend(a, zb, hb))

    def y_sends(a, zb, op):
        for hb in (1, 0):
            y_half(a, zb, hb, op)

    def start(c):
        c.start()

    def ag_own(a):
        for hb in range(2):
            when(z < last, lambda: up(a, z, hb).start())
            when(z > 0, lambda: dn(a, z, hb).start())

    def ag_step(a, s, then=None):
        below, above = z - s, z + s

        def from_below():
            for hb in range(2):
                up(a, below, hb).wait_recv()
                when(z < last, lambda hb=hb: up(a, below, hb).start())
                y_half(a, below, hb, start)

        def from_above():
            for hb in range(2):
                dn(a, above, hb).wait_recv()
                when(z > 0, lambda hb=hb: dn(a, above, hb).start())
                y_half(a, above, hb, start)

        when(below >= 0, from_below)
        when(above <= last, from_above)

        def extra_dn():
            for hb in by_line(a):
                when(z == last, lambda hb=hb: yrecv_desc(a, z, hb).wait_recv())
                when(z < last, lambda hb=hb: extra(a, 1, hb).wait_recv())
                extra(a, 1, hb).start()
            if then is not None:
                for hb in range(2):
                    dn(then, z, hb).start()

        def extra_up():
            for hb in by_line(a):
                when(z == 0, lambda hb=hb: yrecv_desc(a, z, hb).wait_recv())
                when(z > 0, lambda hb=hb: extra(a, 0, hb).wait_recv())
                extra(a, 0, hb).start()
            if then is not None:
                for hb in range(2):
                    up(then, z, hb).start()

        when(jnp.logical_and(z == Z - s, z > 0), extra_dn)
        when(jnp.logical_and(z == s - 1, z < last), extra_up)

    def wait_y(a, zb):
        inner = jnp.logical_and(zb > 0, zb < last)
        for hb in range(2):
            if hb in by_line(a):
                when(inner, lambda hb=hb: yrecv_desc(a, zb, hb).wait_recv())
                when(jnp.logical_and(zb == last, z == 0), lambda hb=hb: extra(a, 1, hb).wait_recv())
                when(jnp.logical_and(zb == 0, z == last), lambda hb=hb: extra(a, 0, hb).wait_recv())
            else:
                yrecv_desc(a, zb, hb).wait_recv()

    def at_distance(s, fn):
        def side(j):
            zb = z + (2 * j - 1) * s
            ok = jnp.logical_and(zb >= 0, zb <= last)
            when(jnp.logical_and(ok, jnp.logical_or(s > 0, j == 0)), lambda: fn(zb))
        loop(2, side)

    def by_distance(fn, far_first=False):
        loop(Z, lambda i: at_distance(last - i if far_first else i, fn))

    def sub_rows(ref, db):
        off = pl.multiple_of(lax.rem(db, q) * cols, cols)
        return ref.at[lax.div(db, q), pl.ds(off, cols), :]

    def mp_copy(a, buf, src, k, to):
        return send(buf.at[src], buf.at[src], as_.at[a, k], ar.at[a, src], (d, to))

    def mp_first(a, buf, op):
        for k in range(1, X):
            op(mp_copy(a, buf, m, X + k, lax.rem(chip + k, X) * 2 + core))
        op(mp_copy(a, buf, m, 0, partner))

    def mp_relay(a, buf):
        for k in range(1, X):
            src = lax.rem(chip + k, X) * 2 + core
            mp_copy(a, buf, src, k, partner).wait_recv()
            mp_copy(a, buf, src, k, partner).start()

    def mp_wait(a, buf):
        for k in range(X):
            src = lax.rem(chip + k, X) * 2 + 1 - core
            mp_copy(a, buf, src, k, partner).wait_recv()

    def mp_sent(a, buf):
        mp_first(a, buf, lambda c: c.wait_send())
        for k in range(1, X):
            mp_copy(a, buf, lax.rem(chip + k, X) * 2 + core, k, partner).wait_send()

    load[0].wait()
    for a in range(2):
        ag_own(a)
        y_sends(a, z, start)
    load[1].wait()
    mp_first(0, rbuf, start)
    for p in range(parts):
        load[4 + p].wait()

    def far_slot(k):
        return lax.rem(k + X, X) - 1

    def r_near(db):
        xb, sub = lax.div(db, 2 * q), lax.rem(db, q)
        return send(ssend.at[:, db], r1buf.at[:, xb, sub], rs1.at[xb, sub], rr1.at[xb, sub], (d, partner))

    def r_far(db):
        xb, sub = lax.div(db, 2 * q), lax.rem(db, q)
        slot = far_slot(chip - xb)
        return send(ssend.at[:, db], r2buf.at[:, slot, sub], rs2.at[xb, sub], rr2.at[slot, sub], (d, xb * 2 + core))

    def r_term(db):
        xb, sub = lax.div(db, 2 * q), lax.rem(db, q)
        mine = lax.rem(lax.div(db, q), 2) == core

        def one(t):
            term = lax.dot_general(
                gbuf[db, :, t], gbuf[d], (((0,), (0,)), ((), ())), preferred_element_type=f32
            )
            for h in range(last_chunks):
                ssend[h, db, t, :] = term[:, h * cw:(h + 1) * cw].astype(bf16)
        tiles(cols, min(256, cols), one)

        def add():
            got = r1buf.at[:, xb, sub]
            send(got, got, rs1.at[0, 0], rr1.at[xb, sub], (d, partner)).wait_recv()
            for h in range(last_chunks):
                ssend[h, db] = (ssend[h, db].astype(f32) + r1buf[h, xb, sub].astype(f32)).astype(bf16)
            when(xb != chip, lambda: r_far(db).start())
        when(jnp.logical_not(mine), lambda: r_near(db).start())
        when(mine, add)

    def rr_term(db):
        rhs = sub_rows(rbuf, db)
        def one(t):
            acc[t, :] += jnp.dot(gbuf[db, t, :], rhs[...], preferred_element_type=f32)
        tiles(rows, tile, one)

    def zero_acc():
        def one(t):
            acc[t, :] = jnp.zeros((tile, cols), f32)
        tiles(rows, tile, one)

    r_term(d)

    def g_step(i):
        s = i + 1
        ag_step(0, s)
        ag_step(1, s, then=2)
        when(s == min(2, last), lambda: mp_relay(0, rbuf))
        at_distance(s, lambda zb: r_term(zb * 2 + y))
    loop(Z - 1, g_step)
    y_sends(2, z, start)
    zero_acc()
    mp_wait(0, rbuf)
    by_distance(lambda zb: rr_term(zb * 2 + y))

    def y_block(zb):
        wait_y(0, zb)
        wait_y(1, zb)
        rr_term(zb * 2 + 1 - y)
    by_distance(y_block)

    def rr_out(t):
        rrbuf[m, t, :] = acc[t, :].astype(bf16)
    tiles(rows, tile, rr_out)
    mp_first(1, rrbuf, start)
    zero_acc()

    owner = lax.div(d, q)
    own_chip = lax.div(owner, 2)
    hd = dp // 2
    pair_off = pl.multiple_of(lax.rem(d, q) * cols, cols)

    def p_send(hb, i, to):
        view_p = pbuf.at[pl.ds(hb * hd, hd)]
        return send(view_p, view_p, ps.at[i], pr.at[hb], (d, to))

    def to_chips(op):
        for k in range(1, X):
            op(p_send(core, 2 + k, lax.rem(chip + k, X) * 2 + core))

    def own_pair():
        def copy(i):
            pbuf[i] = gbuf[i, pl.ds(pair_off, cols), :]
        loop(dp, copy)
        for hb in range(2):
            p_send(hb, hb, partner).start()
        to_chips(start)

    def near_pair():
        for hb in range(2):
            p_send(hb, hb, partner).wait_recv()
        to_chips(start)

    def far_relay():
        p_send(core, 0, partner).wait_recv()
        p_send(core, 0, partner).start()

    def far_pair():
        p_send(1 - core, 0, partner).wait_recv()

    when(m == owner, own_pair)

    def back_term(db, piece, t):
        p, r0, _, c0, w, _ = piece
        off = pl.multiple_of(lax.rem(db, q) * cols + c0, 128)
        rhs = rbuf[lax.div(db, q), pl.ds(off, w), :]
        mine = pl.ds(pl.multiple_of(t.start + (p * part + r0), t.size), t.size)
        return lax.dot_general(
            dbuf[mine, :], rhs, (((1,), (1,)), ((), ())), preferred_element_type=f32
        )

    def piece_tiles(piece, fn):
        tiles(piece[2], min(256, piece[2]), fn)

    def by_send(i, zb):
        return send(out_bufs[i].at[zb], y_bufs[i].at[zb], bys.at[i, zb], byr.at[i, zb], (ynbr, m))

    def by_last(i):
        return send(out_bufs[i].at[z, 1 - y], y_bufs[i], bys.at[i, 0], byr.at[i, 0], (ynbr, m))

    def bz_up(i, zb, src):
        return send(src.at[zb], z_bufs[i].at[zb], bzs.at[i, zb], bzr.at[i, zb], (d + 2, m))

    def bz_dn(i, zb, src):
        slot = jnp.where(zb == z - 1, Z, zb)
        return send(src.at[zb], z_bufs[i].at[slot], bzs.at[i, zb], bzr.at[i, slot], (d - 2, m))

    def z_arrivals(i, zb, add):
        def one(slot):
            dst = z_bufs[i].at[slot]
            send(dst, dst, bzs.at[i, 0], bzr.at[i, slot], (ynbr, m)).wait_recv()
            add(slot)
        when(jnp.logical_and(zb >= z, z > 0), lambda: one(zb))
        when(jnp.logical_and(zb < z, z < last), lambda: one(zb))
        when(jnp.logical_and(zb == z, z < last), lambda: one(Z))

    def z_send(i, zb, src):
        when(zb > z, lambda: bz_up(i, zb, src).start())
        when(zb < z, lambda: bz_dn(i, zb, src).start())

    def to_back(piece, t, value):
        p, r0, _, c0, w, _ = piece
        mine = pl.ds(pl.multiple_of(t.start + (p * part + r0), t.size), t.size)
        bbuf[mine, pl.ds(c0, w)] = value.astype(bf16)

    def line_y_first(i, piece, zb):
        c = pl.ds(0, piece[4])
        by_send(i, zb).wait_recv()

        def one(t):
            acc[t, c] = back_term(zb * 2 + y, piece, t) + y_bufs[i][zb, t, :].astype(f32)
        piece_tiles(piece, one)

        def add(slot):
            def more(t):
                acc[t, c] += z_bufs[i][slot, t, :].astype(f32)
            piece_tiles(piece, more)
        z_arrivals(i, zb, add)

        def pack(t):
            y_bufs[i][zb, t, :] = acc[t, c].astype(bf16)
        when(zb != z, lambda: piece_tiles(piece, pack))
        z_send(i, zb, y_bufs[i])
        when(zb == z, lambda: piece_tiles(piece, lambda t: to_back(piece, t, acc[t, c])))

    def line_z_first(i, piece, zb):
        n = piece[2]

        def rows_of(t, yy):
            return pl.ds(pl.multiple_of(t.start + yy * n, t.size), t.size)
        for yy in range(2):
            def one(t, yy=yy):
                acc[rows_of(t, yy), pl.ds(0, piece[4])] = back_term(zb * 2 + yy, piece, t)
            piece_tiles(piece, one)

        def add(slot):
            for yy in range(2):
                def more(t, yy=yy):
                    acc[rows_of(t, yy), pl.ds(0, piece[4])] += z_bufs[i][slot, yy, t, :].astype(f32)
                piece_tiles(piece, more)
        z_arrivals(i, zb, add)
        for yy in range(2):
            def pack(t, yy=yy):
                out_bufs[i][zb, yy, t, :] = acc[rows_of(t, yy), pl.ds(0, piece[4])].astype(bf16)
            piece_tiles(piece, pack)
        z_send(i, zb, out_bufs[i])
        when(zb == z, lambda: by_last(i).start())

    def finish_z_first(i, piece):
        by_last(i).wait_recv()

        def one(t):
            mine = out_bufs[i][z, y, t, :].astype(f32) + y_bufs[i][t, :].astype(f32)
            to_back(piece, t, mine)
        piece_tiles(piece, one)

    def numbered(p):
        return list(enumerate(pieces[p], first_piece[p]))

    def scatter_first(p):
        groups = []
        for i, piece in numbered(p):
            if piece[5] == Z_FIRST:
                if p == parts - 1:
                    scatter_step(i, piece, last)
            elif len(groups) > 1 and len(groups[-1]) == 1:
                groups[-1].append((i, piece))
            else:
                groups.append([(i, piece)])
        for group in groups:
            p0, r0, nr, c0, w, kind = group[0][1]
            both = (p0, r0, nr, c0, w * len(group), kind)

            def one_block(zb, group=group, both=both, w=w):
                def one(t):
                    value = back_term(zb * 2 + 1 - y, both, t).astype(bf16)
                    for j, (i, _) in enumerate(group):
                        out_bufs[i][zb, t, :] = value[:, j * w:(j + 1) * w]
                piece_tiles(both, one)
                by_send(group[0][0], zb).start()
            by_distance(one_block, far_first=True)
            for i, _ in group[1:]:
                by_distance(lambda zb, i=i: by_send(i, zb).start(), far_first=True)

    def scatter_step(i, piece, s):
        fn = line_z_first if piece[5] == Z_FIRST else line_y_first
        at_distance(s, lambda zb: fn(i, piece, zb))

    mom_tile = min(128, part)

    def m_term(p, db):
        rhs = sub_rows(rrbuf, db)
        def one(t):
            acc[t, :] += lax.dot_general(
                lbuf[p, db, :, t], rhs[...], (((0,), (0,)), ((), ())), preferred_element_type=f32
            )
        tiles(part, tile, one)

    def zero_part():
        def one(t):
            acc[t, :] = jnp.zeros((tile, cols), f32)
        tiles(part, tile, one)

    def moments(p):
        def one(t):
            w = pl.ds(pl.multiple_of(t.start + p * part, mom_tile), mom_tile)
            rot = acc[t, :]
            new1 = decay_moment * mom1[t, :] + (1.0 - decay_moment) * rot
            new2 = decay_moment * mom2[t, :] + (1.0 - decay_moment) * rot * rot
            mom1[t, :] = new1
            mom2[t, :] = new2
            dbuf[w, :] = (new1 / (jnp.sqrt(new2) + epsilon)).astype(bf16)
        tiles(part, mom_tile, one)

    def direction(p):
        def y_part(zb):
            wait_y(2 + p, zb)
            m_term(p, zb * 2 + 1 - y)
        by_distance(y_part)
        for c in mom_loads(p):
            c.wait()
        moments(p)
        for c in mom_stores(p):
            c.start()

    def r_y_terms(near):
        def one(zb):
            db = zb * 2 + 1 - y
            mine = lax.rem(lax.div(db, q), 2) == core
            when(jnp.logical_xor(mine, near), lambda: r_term(db))
        by_distance(one)

    def l_step(i):
        s = i + 1
        when(s == last, lambda: mp_relay(1, rrbuf))
        ag_step(2, s, then=3 if parts > 1 else None)
        when(jnp.logical_and(s == min(2, last), jnp.logical_and(chip == own_chip, m != owner)), near_pair)
        when(s == 1, lambda: r_y_terms(True))
        when(s == min(2, last), lambda: r_y_terms(False))
    loop(Z - 1, l_step)
    if parts > 1:
        y_sends(3, z, start)
    mp_wait(1, rrbuf)
    by_distance(lambda zb: m_term(0, zb * 2 + y))
    direction(0)
    scatter_first(0)

    def r_final():
        for sub in range(q):
            for k in range(1, X):
                got = r2buf.at[:, k - 1, sub]
                send(got, got, rs1.at[0, 0], rr2.at[k - 1, sub], (d, partner)).wait_recv()
            for h in range(last_chunks):
                def one(t, sub=sub, h=h):
                    total = ssend[h, m * q + sub, t, :].astype(f32)
                    for k in range(1, X):
                        total += r2buf[h, k - 1, sub, t, :].astype(f32)
                    where = pl.ds(pl.multiple_of(sub * cols + t.start, 128), 128)
                    c = pl.ds(h * cw, cw)
                    fac_r[where, c] = decay_factor * fac_r[where, c] + (1.0 - decay_factor) * total
                tiles(cols, 128, one)

    def l_scale(t):
        fac_l[t, :] = decay_factor * fac_l[t, :]
    load[2].wait()
    load[3].wait()
    tiles(rows, tile, l_scale)

    def l_term(db):
        def one(t):
            fac_l[t, :] += (1.0 - decay_factor) * lax.dot_general(
                gbuf[db, t, :], pbuf[db], (((1,), (1,)), ((), ())), preferred_element_type=f32
            )
        tiles(rows, tile, one)

    for p in range(1, parts):
        def both(i, p=p):
            s = i + 1
            for j, piece in numbered(p - 1):
                scatter_step(j, piece, Z - s)
            ag_step(2 + p, s, then=3 + p if p + 1 < parts else None)
            if p == 1:
                when(jnp.logical_and(s == last, chip != own_chip), far_relay)
        loop(Z - 1, both)
        if p + 1 < parts:
            y_sends(3 + p, z, start)
        if p == 1:
            r_final()
            store_right.start()
            when(chip != own_chip, far_pair)
            loop(EARLY, l_term)
        for j, piece in numbered(p - 1):
            scatter_step(j, piece, 0)
        zero_part()
        for c in mom_stores(p - 1):
            c.wait()
        for c in mom_loads(p):
            c.start()
        by_distance(lambda zb, p=p: m_term(p, zb * 2 + y))
        direction(p)
        scatter_first(p)
        for j, piece in numbered(p - 1):
            if piece[5] == Z_FIRST:
                finish_z_first(j, piece)

    def r_sent(db):
        mine = lax.rem(lax.div(db, q), 2) == core
        when(jnp.logical_not(mine), lambda: r_near(db).wait_send())
        when(jnp.logical_and(mine, lax.div(db, 2 * q) != chip), lambda: r_far(db).wait_send())
    loop(dp, r_sent)

    def u_near(h, xb, sub):
        db = (xb * 2 + 1 - core) * q + sub
        return send(
            ssend.at[h, db], u1buf.at[h, xb, sub], us1.at[h, xb, sub], ur1.at[h, xb, sub], (d, partner)
        )

    def u_far(h, xb, sub):
        db = (xb * 2 + core) * q + sub
        slot = far_slot(chip - xb)
        return send(
            ssend.at[h, db], u2buf.at[h, slot, sub], us2.at[h, xb, sub], ur2.at[h, slot, sub], (d, xb * 2 + core)
        )

    def u_got(dst, sem):
        send(dst, dst, us1.at[0, 0, 0], sem, (d, partner)).wait_recv()

    def u_dot(h, db):
        c = pl.ds(h * cw, cw)
        p = parts - 1
        term = jnp.dot(lbuf[p, db], bbuf[pl.ds(p * part, part), c], preferred_element_type=f32)
        return ssend[h, db].astype(f32) + term

    def u_before():
        def one(db):
            for h0 in range(0, last_chunks, 2):
                c = pl.ds(h0 * cw, 2 * cw)
                total = None
                for p in range(parts - 1):
                    term = jnp.dot(lbuf[p, db], bbuf[pl.ds(p * part, part), c], preferred_element_type=f32)
                    total = term if total is None else total + term
                for h in range(2):
                    ssend[h0 + h, db] = total[:, h * cw:(h + 1) * cw].astype(bf16)
        loop(dp, one)

    def u_terms(h):
        def near(i):
            xb, sub = lax.rem(chip + 1 + lax.div(i, q), X), lax.rem(i, q)
            db = (xb * 2 + 1 - core) * q + sub
            ssend[h, db] = u_dot(h, db).astype(bf16)
            u_near(h, xb, sub).start()
        loop(X * q, near)

        def far(i):
            xb, sub = lax.rem(chip + 1 + lax.div(i, q), X), lax.rem(i, q)
            db = (xb * 2 + core) * q + sub
            mine = u_dot(h, db)
            u_got(u1buf.at[h, xb, sub], ur1.at[h, xb, sub])
            ssend[h, db] = (mine + u1buf[h, xb, sub].astype(f32)).astype(bf16)
            when(xb != chip, lambda: u_far(h, xb, sub).start())
        loop(X * q, far)

    def u_final(h):
        c = pl.ds(h * cw, cw)
        for sub in range(q):
            for k in range(1, X):
                u_got(u2buf.at[h, k - 1, sub], ur2.at[h, k - 1, sub])

            def one(t, sub=sub):
                total = ssend[h, m * q + sub, t, :].astype(f32)
                for k in range(1, X):
                    total += u2buf[h, k - 1, sub, t, :].astype(f32)
                where = pl.ds(pl.multiple_of(sub * cols + t.start, 128), 128)
                dbuf[where, c] = total.astype(bf16)
            tiles(cols, 128, one)

    steps, k = [], 0
    for h, (i, piece) in enumerate(numbered(parts - 1)):
        for t in range(last, -1, -1):
            if piece[5] == Y_FIRST:
                due = PIECE_US * k + HOP_US * (last - t) + 5 + (CHAIN_US if t == 0 else 0)
            else:
                due = Z_HOP_US * (last - t)
            if piece[5] == Y_FIRST or t < last:
                steps.append((due, len(steps), h, i, piece, t))
        if piece[5] == Z_FIRST:
            steps.append((Z_HOP_US * last + 10, len(steps), h, i, piece, -1))
        else:
            k += 1
    steps.sort(key=lambda e: e[:2])
    u_before()
    done = EARLY
    for n, (_, _, h, i, piece, t) in enumerate(steps):
        if t >= 0:
            scatter_step(i, piece, t)
        else:
            finish_z_first(i, piece)
        if t == (-1 if piece[5] == Z_FIRST else 0):
            u_terms(h)
        if n >= L_FROM and done < dp:
            l_term(done)
            done += 1
            if done == dp:
                store_left.start()
    if done < dp:
        loop(dp - done, lambda k, done=done: l_term(done + k))
        store_left.start()
    for h in range(last_chunks):
        u_final(h)
    store_update.start()

    for a in range(2 + parts):
        def sent(i, a=a):
            for hb in range(2):
                when(jnp.logical_and(z < last, i <= z), lambda: up(a, i, hb).wait_send())
                when(jnp.logical_and(z > 0, i >= z), lambda: dn(a, i, hb).wait_send())
            y_sends(a, i, lambda c: c.wait_send())
        loop(Z, sent)
        for hb in by_line(a):
            when(z > 0, lambda: extra(a, 1, hb).wait_send())
            when(z < last, lambda: extra(a, 0, hb).wait_send())
    mp_sent(0, rbuf)
    mp_sent(1, rrbuf)

    def near_sent():
        to_chips(lambda c: c.wait_send())
    when(chip == own_chip, near_sent)

    def own_sent():
        for hb in range(2):
            p_send(hb, hb, partner).wait_send()
    when(m == owner, own_sent)
    when(chip != own_chip, lambda: p_send(core, 0, partner).wait_send())
    def line_sent(i, piece):
        src = out_bufs[i] if piece[5] == Z_FIRST else y_bufs[i]

        def one(zb):
            if piece[5] == Y_FIRST:
                by_send(i, zb).wait_send()
            when(zb != z, lambda: bz_up(i, zb, src).wait_send())
        loop(Z, one)
        if piece[5] == Z_FIRST:
            by_last(i).wait_send()
    for p in range(parts):
        for i, piece in numbered(p):
            line_sent(i, piece)
    for h in range(last_chunks):
        for sub in range(q):
            for xb in range(X):
                u_near(h, xb, sub).wait_send()
                when(xb != chip, lambda h=h, xb=xb, sub=sub: u_far(h, xb, sub).wait_send())
    for c in mom_stores(parts - 1) + [store_left, store_right, store_update]:
        c.wait()


def write_out(*refs):
    n = (len(refs) - 2) // 3
    ins, outs, bufs, sem_in, sem_out = refs[:n], refs[n:2 * n], refs[2 * n:-2], refs[-2], refs[-1]
    reads = [pltpu.make_async_copy(a, b, sem_in.at[i]) for i, (a, b) in enumerate(zip(ins, bufs))]
    writes = [pltpu.make_async_copy(b, a, sem_out.at[i]) for i, (a, b) in enumerate(zip(outs, bufs))]
    for c in reads:
        c.start()
    for r, w in zip(reads, writes):
        r.wait()
        w.start()
    for w in writes:
        w.wait()


def solution(mesh):
    dp, mp = mesh.shape["dp"], mesh.shape["mp"]
    Z, X = dp // 2, mp // 2

    def per_device(*args):
        _, rows, cols = args[0].shape
        q = rows // cols
        parts = min(PARTS, rows // 128)
        last_chunks = min(LAST, cols // 128)
        part, cw = rows // parts, cols // last_chunks
        pieces = sum(scatter_pieces(rows, cols, parts, last_chunks), [])
        n = len(pieces)
        out_b, y_b, z_b = [], [], []
        for _, _, nr, _, w, kind in pieces:
            lead = (2,) if kind == Z_FIRST else ()
            out_b.append(pltpu.VMEM((Z,) + lead + (nr, w), bf16))
            y_b.append(pltpu.VMEM((nr, w) if lead else (Z, nr, w), bf16))
            z_b.append(pltpu.VMEM((Z + 1,) + lead + (nr, w), bf16))
        flat = [a.reshape(a.shape[1:]) for a in args]
        dma = pltpu.SemaphoreType.DMA
        outs = pl.pallas_call(
            functools.partial(kernel, dp, mp, rows, cols, parts, last_chunks),
            out_shape=[jax.ShapeDtypeStruct((rows, cols), t) for t in (f32, f32, f32, f32, bf16)],
            in_specs=[pl.BlockSpec(memory_space=pl.ANY)] * 7,
            out_specs=[pl.BlockSpec(memory_space=pl.ANY)] * 5,
            scratch_shapes=[
                pltpu.VMEM((dp, rows, cols), bf16),
                pltpu.VMEM((parts, dp, cols, part), bf16),
                pltpu.VMEM((mp, rows, cols), bf16),
                pltpu.VMEM((mp, rows, cols), bf16),
                pltpu.VMEM((dp, cols, cols), bf16),
                pltpu.VMEM((last_chunks, dp, cols, cw), bf16),
                pltpu.VMEM((last_chunks, X, q, cols, cw), bf16),
                pltpu.VMEM((last_chunks, X - 1, q, cols, cw), bf16),
                pltpu.VMEM((last_chunks, X - 1, q, cols, cw), bf16),
                pltpu.VMEM((rows, cols), f32),
                pltpu.VMEM((rows, cols), f32),
                pltpu.VMEM((part, cols), f32),
                pltpu.VMEM((part, cols), f32),
                pltpu.VMEM((rows, cols), f32),
                pltpu.VMEM((rows, cols), bf16),
                pltpu.VMEM((rows, cols), bf16),
                dma((4 + 3 * parts,)),
                dma((3 + 2 * parts,)),
                dma((2 + parts, Z, 2)),
                dma((2 + parts, Z, 2)),
                dma((2 + parts, Z, 2)),
                dma((2 + parts, Z, 2)),
                dma((2 + parts, Z, 2)),
                dma((2 + parts, 2, 2)),
                dma((2 + parts, 2, 2)),
                dma((2, 2 * X)),
                dma((2, mp)),
                dma((X, q)),
                dma((X, q)),
                dma((X, q)),
                dma((X - 1, q)),
                dma((last_chunks, X, q)),
                dma((last_chunks, X, q)),
                dma((last_chunks, X, q)),
                dma((last_chunks, X - 1, q)),
                dma((2 + X,)),
                dma((2,)),
                dma((n, Z)),
                dma((n, Z)),
                dma((n, Z)),
                dma((n, Z + 1)),
            ] + out_b + y_b + z_b,
            compiler_params=pltpu.CompilerParams(
                collective_id=0, has_side_effects=True, vmem_limit_bytes=67043328
            ),
        )(*flat)
        kinds = [jax.ShapeDtypeStruct(o.shape, o.dtype) for o in outs]
        outs = pl.pallas_call(
            write_out,
            out_shape=kinds,
            in_specs=[pl.BlockSpec(memory_space=pl.ANY)] * len(outs),
            out_specs=[pl.BlockSpec(memory_space=pl.ANY)] * len(outs),
            scratch_shapes=[pltpu.VMEM(o.shape, o.dtype) for o in outs] + [dma((len(outs),)), dma((len(outs),))],
            compiler_params=pltpu.CompilerParams(vmem_limit_bytes=67043328),
        )(*outs)
        return tuple(o.reshape((1,) + o.shape) for o in outs)

    return jax.shard_map(
        per_device,
        mesh=mesh,
        in_specs=(P(None, "mp", "dp"),) * 5 + (P(None, "dp", "mp"), P(None, "mp", "dp")),
        out_specs=(P(None, "mp", "dp"),) * 5,
        check_vma=False,
    )
```

```python
import functools

import jax
import jax.numpy as jnp
from jax import lax
from jax.experimental import pallas as pl
from jax.experimental.pallas import tpu as pltpu
from jax.sharding import PartitionSpec as P

decay_moment = 0.95
decay_factor = 0.95
epsilon = 1e-08
bf16, f32 = jnp.bfloat16, jnp.float32
MESH = pl.DeviceIdType.MESH
PARTS, LAST, LAST_Z, EARLY = 2, 4, 1, 4
Y_FIRST, Z_FIRST = 0, 1
PIECE_US, HOP_US, CHAIN_US, Z_HOP_US, L_FROM, U_AT = 11, 3, 8, 8, 3, 2


def scatter_pieces(rows, cols, parts, last_chunks):
    part = rows // parts
    out = [[] for _ in range(parts)]
    for p in range(parts - 1):
        out[p].append((p, 0, part // 2, 0, cols, Z_FIRST))
        out[p].append((p, part // 2, part // 2, 0, cols, Y_FIRST))
    for h in range(last_chunks):
        cw = cols // last_chunks
        out[parts - 1].append((parts - 1, 0, part, h * cw, cw, Z_FIRST if h < LAST_Z else Y_FIRST))
    return out


def kernel(dp, mp, rows, cols, parts, last_chunks, *refs):
    pieces = scatter_pieces(rows, cols, parts, last_chunks)
    first_piece = [sum(len(x) for x in pieces[:p]) for p in range(parts)]
    n_pieces = sum(len(x) for x in pieces)
    NAMED = len(refs) - 3 * n_pieces
    (grad, first, second, left_f, right_f, left_b, right_b,
     out_first, out_second, out_left, out_right, out_update,
     gbuf, lbuf, rbuf, rrbuf, pbuf, ssend, r1buf, r2buf, u2buf,
     fac_l, fac_r, mom1, mom2, acc, dbuf, bbuf,
     load_sem, store_sem, zs_up, zs_dn, zr, ys, yr, es, er, as_, ar,
     rs1, rr1, rs2, rr2, us1, ur1, us2, ur2, ps, pr, bys, byr, bzs, bzr) = refs[:NAMED]
    out_bufs = refs[NAMED:NAMED + n_pieces]
    y_bufs = refs[NAMED + n_pieces:NAMED + 2 * n_pieces]
    z_bufs = refs[NAMED + 2 * n_pieces:]
    u1buf = r1buf
    Z, q, X = dp // 2, rows // cols, mp // 2
    part, cw = rows // parts, cols // last_chunks
    d, m = lax.axis_index("dp"), lax.axis_index("mp")
    z, y = lax.div(d, 2), lax.rem(d, 2)
    core, chip = lax.rem(m, 2), lax.div(m, 2)
    partner = chip * 2 + (1 - core)
    last = Z - 1
    ynbr = z * 2 + (1 - y)
    tile = min(256, part)

    def send(src, dst, s, r, dev):
        return pltpu.make_async_remote_copy(
            src_ref=src, dst_ref=dst, send_sem=s, recv_sem=r, device_id=dev, device_id_type=MESH
        )

    def when(cond, fn):
        pl.when(cond)(fn)

    def loop(n, fn):
        def body(i, c):
            fn(i)
            return c
        lax.fori_loop(0, n, body, 0)

    def tiles(n, size, fn, base=0):
        loop(n // size, lambda i: fn(pl.ds(pl.multiple_of(base + i * size, size), size)))

    loads = [
        (grad, gbuf.at[d]), (right_b, rbuf.at[m]), (right_f, fac_r), (left_f, fac_l),
    ]
    loads += [(left_b.at[:, pl.ds(p * part, part)], lbuf.at[p, d]) for p in range(parts)]
    load = [pltpu.make_async_copy(a, b, load_sem.at[i]) for i, (a, b) in enumerate(loads)]
    for c in load:
        c.start()

    def part_rows(ref, p):
        return ref.at[pl.ds(p * part, part), :]

    def mom_loads(p):
        n = 4 + parts + 2 * p
        return [
            pltpu.make_async_copy(part_rows(a, p), b, load_sem.at[n + i])
            for i, (a, b) in enumerate([(first, mom1), (second, mom2)])
        ]

    def mom_stores(p):
        return [
            pltpu.make_async_copy(b, part_rows(a, p), store_sem.at[3 + 2 * p + i])
            for i, (a, b) in enumerate([(out_first, mom1), (out_second, mom2)])
        ]

    store_right = pltpu.make_async_copy(fac_r, out_right, store_sem.at[0])
    store_left = pltpu.make_async_copy(fac_l, out_left, store_sem.at[1])
    store_update = pltpu.make_async_copy(dbuf, out_update, store_sem.at[2])
    for c in mom_loads(0):
        c.start()

    barrier = pltpu.get_barrier_semaphore()
    pl.semaphore_signal(barrier, inc=1, device_id=(ynbr, m), device_id_type=MESH)
    when(z > 0, lambda: pl.semaphore_signal(barrier, inc=1, device_id=(d - 2, m), device_id_type=MESH))
    when(z < last, lambda: pl.semaphore_signal(barrier, inc=1, device_id=(d + 2, m), device_id_type=MESH))
    for k in range(1, mp):
        pl.semaphore_signal(barrier, inc=1, device_id=(d, lax.rem(m + k, mp)), device_id_type=MESH)
    along = (z > 0).astype(jnp.int32) + (z < last).astype(jnp.int32)
    pl.semaphore_wait(barrier, mp + along)

    def half(a, b, hb):
        if a < 2:
            return gbuf.at[b, pl.ds(a * (rows // 2) + hb * (rows // 4), rows // 4), :]
        return lbuf.at[a - 2, b, pl.ds(hb * (cols // 2), cols // 2), :]

    def up(a, zb, hb):
        blk = half(a, zb * 2 + y, hb)
        return send(blk, blk, zs_up.at[a, zb, hb], zr.at[a, zb, hb], (d + 2, m))

    def dn(a, zb, hb):
        blk = half(a, zb * 2 + y, hb)
        return send(blk, blk, zs_dn.at[a, zb, hb], zr.at[a, zb, hb], (d - 2, m))

    def ysend(a, zb, hb):
        blk = half(a, zb * 2 + y, hb)
        return send(blk, blk, ys.at[a, zb, hb], yr.at[a, zb, hb], (ynbr, m))

    def yrecv_desc(a, zb, hb):
        blk = half(a, zb * 2 + (1 - y), hb)
        return send(blk, blk, ys.at[a, zb, hb], yr.at[a, zb, hb], (ynbr, m))

    def by_line(a):
        return (1,)

    def extra(a, k, hb):
        zb = 0 if k == 0 else last
        blk = half(a, zb * 2 + (1 - y), hb)
        return send(blk, blk, es.at[a, k, hb], er.at[a, k, hb], (d + 2, m) if k == 0 else (d - 2, m))

    def over_y(a, zb, hb):
        inner = jnp.logical_and(zb > 0, zb < last)
        return jnp.logical_or(zb == z, inner)

    def y_half(a, zb, hb, op):
        if hb in by_line(a):
            when(over_y(a, zb, hb), lambda: op(ysend(a, zb, hb)))
        else:
            op(ysend(a, zb, hb))

    def y_sends(a, zb, op):
        for hb in (1, 0):
            y_half(a, zb, hb, op)

    def start(c):
        c.start()

    def ag_own(a):
        for hb in range(2):
            when(z < last, lambda: up(a, z, hb).start())
            when(z > 0, lambda: dn(a, z, hb).start())

    def ag_step(a, s, then=None):
        below, above = z - s, z + s

        def from_below():
            for hb in range(2):
                up(a, below, hb).wait_recv()
                when(z < last, lambda hb=hb: up(a, below, hb).start())
                y_half(a, below, hb, start)

        def from_above():
            for hb in range(2):
                dn(a, above, hb).wait_recv()
                when(z > 0, lambda hb=hb: dn(a, above, hb).start())
                y_half(a, above, hb, start)

        when(below >= 0, from_below)
        when(above <= last, from_above)

        def extra_dn():
            for hb in by_line(a):
                when(z == last, lambda hb=hb: yrecv_desc(a, z, hb).wait_recv())
                when(z < last, lambda hb=hb: extra(a, 1, hb).wait_recv())
                extra(a, 1, hb).start()
            if then is not None:
                for hb in range(2):
                    dn(then, z, hb).start()

        def extra_up():
            for hb in by_line(a):
                when(z == 0, lambda hb=hb: yrecv_desc(a, z, hb).wait_recv())
                when(z > 0, lambda hb=hb: extra(a, 0, hb).wait_recv())
                extra(a, 0, hb).start()
            if then is not None:
                for hb in range(2):
                    up(then, z, hb).start()

        when(jnp.logical_and(z == Z - s, z > 0), extra_dn)
        when(jnp.logical_and(z == s - 1, z < last), extra_up)

    def wait_y(a, zb):
        inner = jnp.logical_and(zb > 0, zb < last)
        for hb in range(2):
            if hb in by_line(a):
                when(inner, lambda hb=hb: yrecv_desc(a, zb, hb).wait_recv())
                when(jnp.logical_and(zb == last, z == 0), lambda hb=hb: extra(a, 1, hb).wait_recv())
                when(jnp.logical_and(zb == 0, z == last), lambda hb=hb: extra(a, 0, hb).wait_recv())
            else:
                yrecv_desc(a, zb, hb).wait_recv()

    def at_distance(s, fn):
        def side(j):
            zb = z + (2 * j - 1) * s
            ok = jnp.logical_and(zb >= 0, zb <= last)
            when(jnp.logical_and(ok, jnp.logical_or(s > 0, j == 0)), lambda: fn(zb))
        loop(2, side)

    def by_distance(fn, far_first=False):
        loop(Z, lambda i: at_distance(last - i if far_first else i, fn))

    def sub_rows(ref, db):
        off = pl.multiple_of(lax.rem(db, q) * cols, cols)
        return ref.at[lax.div(db, q), pl.ds(off, cols), :]

    def mp_copy(a, buf, src, k, to):
        return send(buf.at[src], buf.at[src], as_.at[a, k], ar.at[a, src], (d, to))

    def mp_first(a, buf, op):
        for k in range(1, X):
            op(mp_copy(a, buf, m, X + k, lax.rem(chip + k, X) * 2 + core))
        op(mp_copy(a, buf, m, 0, partner))

    def mp_relay(a, buf):
        for k in range(1, X):
            src = lax.rem(chip + k, X) * 2 + core
            mp_copy(a, buf, src, k, partner).wait_recv()
            mp_copy(a, buf, src, k, partner).start()

    def mp_wait(a, buf):
        for k in range(X):
            src = lax.rem(chip + k, X) * 2 + 1 - core
            mp_copy(a, buf, src, k, partner).wait_recv()

    def mp_sent(a, buf):
        mp_first(a, buf, lambda c: c.wait_send())
        for k in range(1, X):
            mp_copy(a, buf, lax.rem(chip + k, X) * 2 + core, k, partner).wait_send()

    load[0].wait()
    for a in range(2):
        ag_own(a)
        y_sends(a, z, start)
    load[1].wait()
    mp_first(0, rbuf, start)
    for p in range(parts):
        load[4 + p].wait()

    def far_slot(k):
        return lax.rem(k + X, X) - 1

    def r_near(db):
        xb, sub = lax.div(db, 2 * q), lax.rem(db, q)
        return send(ssend.at[:, db], r1buf.at[:, xb, sub], rs1.at[xb, sub], rr1.at[xb, sub], (d, partner))

    def r_far(db):
        xb, sub = lax.div(db, 2 * q), lax.rem(db, q)
        slot = far_slot(chip - xb)
        return send(ssend.at[:, db], r2buf.at[:, slot, sub], rs2.at[xb, sub], rr2.at[slot, sub], (d, xb * 2 + core))

    def r_term(db):
        xb, sub = lax.div(db, 2 * q), lax.rem(db, q)
        mine = lax.rem(lax.div(db, q), 2) == core

        def one(t):
            term = lax.dot_general(
                gbuf[db, :, t], gbuf[d], (((0,), (0,)), ((), ())), preferred_element_type=f32
            )
            for h in range(last_chunks):
                ssend[h, db, t, :] = term[:, h * cw:(h + 1) * cw].astype(bf16)
        tiles(cols, min(256, cols), one)

        def add():
            got = r1buf.at[:, xb, sub]
            send(got, got, rs1.at[0, 0], rr1.at[xb, sub], (d, partner)).wait_recv()
            for h in range(last_chunks):
                ssend[h, db] = (ssend[h, db].astype(f32) + r1buf[h, xb, sub].astype(f32)).astype(bf16)
            when(xb != chip, lambda: r_far(db).start())
        when(jnp.logical_not(mine), lambda: r_near(db).start())
        when(mine, add)

    def rr_term(db):
        rhs = sub_rows(rbuf, db)
        def one(t):
            acc[t, :] += jnp.dot(gbuf[db, t, :], rhs[...], preferred_element_type=f32)
        tiles(rows, tile, one)

    def zero_acc():
        def one(t):
            acc[t, :] = jnp.zeros((tile, cols), f32)
        tiles(rows, tile, one)

    r_term(d)

    def g_step(i):
        s = i + 1
        ag_step(0, s)
        ag_step(1, s, then=2)
        when(s == min(2, last), lambda: mp_relay(0, rbuf))
        at_distance(s, lambda zb: r_term(zb * 2 + y))
    loop(Z - 1, g_step)
    y_sends(2, z, start)
    zero_acc()
    mp_wait(0, rbuf)
    by_distance(lambda zb: rr_term(zb * 2 + y))

    def y_block(zb):
        wait_y(0, zb)
        wait_y(1, zb)
        rr_term(zb * 2 + 1 - y)
    by_distance(y_block)

    def rr_out(t):
        rrbuf[m, t, :] = acc[t, :].astype(bf16)
    tiles(rows, tile, rr_out)
    mp_first(1, rrbuf, start)
    zero_acc()

    owner = lax.div(d, q)
    own_chip = lax.div(owner, 2)
    hd = dp // 2
    pair_off = pl.multiple_of(lax.rem(d, q) * cols, cols)

    def p_send(hb, i, to):
        view_p = pbuf.at[pl.ds(hb * hd, hd)]
        return send(view_p, view_p, ps.at[i], pr.at[hb], (d, to))

    def to_chips(op):
        for k in range(1, X):
            op(p_send(core, 2 + k, lax.rem(chip + k, X) * 2 + core))

    def own_pair():
        def copy(i):
            pbuf[i] = gbuf[i, pl.ds(pair_off, cols), :]
        loop(dp, copy)
        for hb in range(2):
            p_send(hb, hb, partner).start()
        to_chips(start)

    def near_pair():
        for hb in range(2):
            p_send(hb, hb, partner).wait_recv()
        to_chips(start)

    def far_relay():
        p_send(core, 0, partner).wait_recv()
        p_send(core, 0, partner).start()

    def far_pair():
        p_send(1 - core, 0, partner).wait_recv()

    when(m == owner, own_pair)

    def back_term(db, piece, t):
        p, r0, _, c0, w, _ = piece
        off = pl.multiple_of(lax.rem(db, q) * cols + c0, 128)
        rhs = rbuf[lax.div(db, q), pl.ds(off, w), :]
        mine = pl.ds(pl.multiple_of(t.start + (p * part + r0), t.size), t.size)
        return lax.dot_general(
            dbuf[mine, :], rhs, (((1,), (1,)), ((), ())), preferred_element_type=f32
        )

    def piece_tiles(piece, fn):
        tiles(piece[2], min(256, piece[2]), fn)

    def by_send(i, zb):
        return send(out_bufs[i].at[zb], y_bufs[i].at[zb], bys.at[i, zb], byr.at[i, zb], (ynbr, m))

    def by_last(i):
        return send(out_bufs[i].at[z, 1 - y], y_bufs[i], bys.at[i, 0], byr.at[i, 0], (ynbr, m))

    def bz_up(i, zb, src):
        return send(src.at[zb], z_bufs[i].at[zb], bzs.at[i, zb], bzr.at[i, zb], (d + 2, m))

    def bz_dn(i, zb, src):
        slot = jnp.where(zb == z - 1, Z, zb)
        return send(src.at[zb], z_bufs[i].at[slot], bzs.at[i, zb], bzr.at[i, slot], (d - 2, m))

    def z_arrivals(i, zb, add):
        def one(slot):
            dst = z_bufs[i].at[slot]
            send(dst, dst, bzs.at[i, 0], bzr.at[i, slot], (ynbr, m)).wait_recv()
            add(slot)
        when(jnp.logical_and(zb >= z, z > 0), lambda: one(zb))
        when(jnp.logical_and(zb < z, z < last), lambda: one(zb))
        when(jnp.logical_and(zb == z, z < last), lambda: one(Z))

    def z_send(i, zb, src):
        when(zb > z, lambda: bz_up(i, zb, src).start())
        when(zb < z, lambda: bz_dn(i, zb, src).start())

    def to_back(piece, t, value):
        p, r0, _, c0, w, _ = piece
        mine = pl.ds(pl.multiple_of(t.start + (p * part + r0), t.size), t.size)
        bbuf[mine, pl.ds(c0, w)] = value.astype(bf16)

    def line_y_first(i, piece, zb):
        c = pl.ds(0, piece[4])
        by_send(i, zb).wait_recv()

        def one(t):
            acc[t, c] = back_term(zb * 2 + y, piece, t) + y_bufs[i][zb, t, :].astype(f32)
        piece_tiles(piece, one)

        def add(slot):
            def more(t):
                acc[t, c] += z_bufs[i][slot, t, :].astype(f32)
            piece_tiles(piece, more)
        z_arrivals(i, zb, add)

        def pack(t):
            y_bufs[i][zb, t, :] = acc[t, c].astype(bf16)
        when(zb != z, lambda: piece_tiles(piece, pack))
        z_send(i, zb, y_bufs[i])
        when(zb == z, lambda: piece_tiles(piece, lambda t: to_back(piece, t, acc[t, c])))

    def line_z_first(i, piece, zb):
        n = piece[2]

        def rows_of(t, yy):
            return pl.ds(pl.multiple_of(t.start + yy * n, t.size), t.size)
        for yy in range(2):
            def one(t, yy=yy):
                acc[rows_of(t, yy), pl.ds(0, piece[4])] = back_term(zb * 2 + yy, piece, t)
            piece_tiles(piece, one)

        def add(slot):
            for yy in range(2):
                def more(t, yy=yy):
                    acc[rows_of(t, yy), pl.ds(0, piece[4])] += z_bufs[i][slot, yy, t, :].astype(f32)
                piece_tiles(piece, more)
        z_arrivals(i, zb, add)
        for yy in range(2):
            def pack(t, yy=yy):
                out_bufs[i][zb, yy, t, :] = acc[rows_of(t, yy), pl.ds(0, piece[4])].astype(bf16)
            piece_tiles(piece, pack)
        z_send(i, zb, out_bufs[i])
        when(zb == z, lambda: by_last(i).start())

    def finish_z_first(i, piece):
        by_last(i).wait_recv()

        def one(t):
            mine = out_bufs[i][z, y, t, :].astype(f32) + y_bufs[i][t, :].astype(f32)
            to_back(piece, t, mine)
        piece_tiles(piece, one)

    def numbered(p):
        return list(enumerate(pieces[p], first_piece[p]))

    def scatter_first(p):
        groups = []
        for i, piece in numbered(p):
            if piece[5] == Z_FIRST:
                if p == parts - 1:
                    scatter_step(i, piece, last)
            elif len(groups) > 1 and len(groups[-1]) == 1:
                groups[-1].append((i, piece))
            else:
                groups.append([(i, piece)])
        for group in groups:
            p0, r0, nr, c0, w, kind = group[0][1]
            both = (p0, r0, nr, c0, w * len(group), kind)

            def one_block(zb, group=group, both=both, w=w):
                def one(t):
                    value = back_term(zb * 2 + 1 - y, both, t).astype(bf16)
                    for j, (i, _) in enumerate(group):
                        out_bufs[i][zb, t, :] = value[:, j * w:(j + 1) * w]
                piece_tiles(both, one)
                by_send(group[0][0], zb).start()
            by_distance(one_block, far_first=True)
            for i, _ in group[1:]:
                by_distance(lambda zb, i=i: by_send(i, zb).start(), far_first=True)

    def scatter_step(i, piece, s):
        fn = line_z_first if piece[5] == Z_FIRST else line_y_first
        at_distance(s, lambda zb: fn(i, piece, zb))

    mom_tile = min(128, part)

    def held(p, t):
        return pl.ds(pl.multiple_of(t.start + min(p, 1) * part, t.size), t.size)

    def m_term(p, db):
        rhs = sub_rows(rrbuf, db)
        def one(t):
            acc[held(p, t), :] += lax.dot_general(
                lbuf[p, db, :, t], rhs[...], (((0,), (0,)), ((), ())), preferred_element_type=f32
            )
        tiles(part, tile, one)

    def zero_part():
        def one(t):
            acc[held(1, t), :] = jnp.zeros((tile, cols), f32)
        tiles(part, tile, one)

    def moments(p):
        def one(t):
            w = pl.ds(pl.multiple_of(t.start + p * part, mom_tile), mom_tile)
            rot = acc[held(p, t), :]
            new1 = decay_moment * mom1[t, :] + (1.0 - decay_moment) * rot
            new2 = decay_moment * mom2[t, :] + (1.0 - decay_moment) * rot * rot
            mom1[t, :] = new1
            mom2[t, :] = new2
            dbuf[w, :] = (new1 / (jnp.sqrt(new2) + epsilon)).astype(bf16)
        tiles(part, mom_tile, one)

    def direction(p):
        def y_part(zb):
            wait_y(2 + p, zb)
            m_term(p, zb * 2 + 1 - y)
        by_distance(y_part)
        for c in mom_loads(p):
            c.wait()
        moments(p)
        for c in mom_stores(p):
            c.start()

    def r_y_terms(near):
        def one(zb):
            db = zb * 2 + 1 - y
            mine = lax.rem(lax.div(db, q), 2) == core
            when(jnp.logical_xor(mine, near), lambda: r_term(db))
        by_distance(one)

    def l_step(i):
        s = i + 1
        when(s == last, lambda: mp_relay(1, rrbuf))
        ag_step(2, s, then=3 if parts > 1 else None)
        when(jnp.logical_and(s == min(2, last), jnp.logical_and(chip == own_chip, m != owner)), near_pair)
        when(s == 1, lambda: r_y_terms(True))
        when(s == min(2, last), lambda: r_y_terms(False))
    loop(Z - 1, l_step)
    if parts > 1:
        y_sends(3, z, start)
    mp_wait(1, rrbuf)
    by_distance(lambda zb: m_term(0, zb * 2 + y))
    direction(0)
    scatter_first(0)

    def r_final():
        for sub in range(q):
            for k in range(1, X):
                got = r2buf.at[:, k - 1, sub]
                send(got, got, rs1.at[0, 0], rr2.at[k - 1, sub], (d, partner)).wait_recv()
            for h in range(last_chunks):
                def one(t, sub=sub, h=h):
                    total = ssend[h, m * q + sub, t, :].astype(f32)
                    for k in range(1, X):
                        total += r2buf[h, k - 1, sub, t, :].astype(f32)
                    where = pl.ds(pl.multiple_of(sub * cols + t.start, 128), 128)
                    c = pl.ds(h * cw, cw)
                    fac_r[where, c] = decay_factor * fac_r[where, c] + (1.0 - decay_factor) * total
                tiles(cols, 128, one)

    def l_scale(t):
        fac_l[t, :] = decay_factor * fac_l[t, :]
    load[2].wait()
    load[3].wait()
    tiles(rows, tile, l_scale)

    def l_term(db):
        def one(t):
            fac_l[t, :] += (1.0 - decay_factor) * lax.dot_general(
                gbuf[db, t, :], pbuf[db], (((1,), (1,)), ((), ())), preferred_element_type=f32
            )
        tiles(rows, tile, one)

    for p in range(1, parts):
        def both(i, p=p):
            s = i + 1
            for j, piece in numbered(p - 1):
                scatter_step(j, piece, Z - s)
            ag_step(2 + p, s, then=3 + p if p + 1 < parts else None)
            if p == 1:
                when(jnp.logical_and(s == last, chip != own_chip), far_relay)
        loop(Z - 1, both)
        if p + 1 < parts:
            y_sends(3 + p, z, start)
        if p == 1:
            r_final()
            store_right.start()
            when(chip != own_chip, far_pair)
            loop(EARLY, l_term)
        zero_part()
        by_distance(lambda zb, p=p: m_term(p, zb * 2 + y))
        for j, piece in numbered(p - 1):
            scatter_step(j, piece, 0)
        for c in mom_stores(p - 1):
            c.wait()
        for c in mom_loads(p):
            c.start()
        direction(p)
        scatter_first(p)
        for j, piece in numbered(p - 1):
            if piece[5] == Z_FIRST:
                finish_z_first(j, piece)

    def r_sent(db):
        mine = lax.rem(lax.div(db, q), 2) == core
        when(jnp.logical_not(mine), lambda: r_near(db).wait_send())
        when(jnp.logical_and(mine, lax.div(db, 2 * q) != chip), lambda: r_far(db).wait_send())
    loop(dp, r_sent)

    def u_near(h, xb, sub):
        db = (xb * 2 + 1 - core) * q + sub
        return send(
            ssend.at[h, db], u1buf.at[h, xb, sub], us1.at[h, xb, sub], ur1.at[h, xb, sub], (d, partner)
        )

    def u_far(h, xb, sub):
        db = (xb * 2 + core) * q + sub
        slot = far_slot(chip - xb)
        return send(
            ssend.at[h, db], u2buf.at[h, slot, sub], us2.at[h, xb, sub], ur2.at[h, slot, sub], (d, xb * 2 + core)
        )

    def u_got(dst, sem):
        send(dst, dst, us1.at[0, 0, 0], sem, (d, partner)).wait_recv()

    def u_dot(h, db):
        c = pl.ds(h * cw, cw)
        p = parts - 1
        term = jnp.dot(lbuf[p, db], bbuf[pl.ds(p * part, part), c], preferred_element_type=f32)
        return ssend[h, db].astype(f32) + term

    def u_before():
        def one(db):
            for h0 in range(0, last_chunks, 2):
                c = pl.ds(h0 * cw, 2 * cw)
                total = None
                for p in range(parts - 1):
                    term = jnp.dot(lbuf[p, db], bbuf[pl.ds(p * part, part), c], preferred_element_type=f32)
                    total = term if total is None else total + term
                for h in range(2):
                    ssend[h0 + h, db] = total[:, h * cw:(h + 1) * cw].astype(bf16)
        loop(dp, one)

    def u_terms(h):
        def near(i):
            xb, sub = lax.rem(chip + 1 + lax.div(i, q), X), lax.rem(i, q)
            db = (xb * 2 + 1 - core) * q + sub
            ssend[h, db] = u_dot(h, db).astype(bf16)
            u_near(h, xb, sub).start()
        loop(X * q, near)

        def far(i):
            xb, sub = lax.rem(chip + 1 + lax.div(i, q), X), lax.rem(i, q)
            db = (xb * 2 + core) * q + sub
            mine = u_dot(h, db)
            u_got(u1buf.at[h, xb, sub], ur1.at[h, xb, sub])
            ssend[h, db] = (mine + u1buf[h, xb, sub].astype(f32)).astype(bf16)
            when(xb != chip, lambda: u_far(h, xb, sub).start())
        loop(X * q, far)

    def u_final(h):
        c = pl.ds(h * cw, cw)
        for sub in range(q):
            for k in range(1, X):
                u_got(u2buf.at[h, k - 1, sub], ur2.at[h, k - 1, sub])

            def one(t, sub=sub):
                total = ssend[h, m * q + sub, t, :].astype(f32)
                for k in range(1, X):
                    total += u2buf[h, k - 1, sub, t, :].astype(f32)
                where = pl.ds(pl.multiple_of(sub * cols + t.start, 128), 128)
                dbuf[where, c] = total.astype(bf16)
            tiles(cols, 128, one)

    steps, k = [], 0
    for h, (i, piece) in enumerate(numbered(parts - 1)):
        for t in range(last, -1, -1):
            if piece[5] == Y_FIRST:
                due = PIECE_US * k + HOP_US * (last - t) + 5 + (CHAIN_US if t == 0 else 0)
            else:
                due = Z_HOP_US * (last - t)
            if piece[5] == Y_FIRST or t < last:
                steps.append((due, len(steps), h, i, piece, t))
        if piece[5] == Z_FIRST:
            steps.append((Z_HOP_US * last + 10, len(steps), h, i, piece, -1))
        else:
            k += 1
    steps.sort(key=lambda e: e[:2])
    done = EARLY
    for n, (_, _, h, i, piece, t) in enumerate(steps):
        if n == U_AT:
            u_before()
        if t >= 0:
            scatter_step(i, piece, t)
        else:
            finish_z_first(i, piece)
        if t == (-1 if piece[5] == Z_FIRST else 0):
            u_terms(h)
        if n >= L_FROM and done < dp:
            l_term(done)
            done += 1
            if done == dp:
                store_left.start()
    if done < dp:
        loop(dp - done, lambda k, done=done: l_term(done + k))
        store_left.start()
    for h in range(last_chunks):
        u_final(h)
    store_update.start()

    for a in range(2 + parts):
        def sent(i, a=a):
            for hb in range(2):
                when(jnp.logical_and(z < last, i <= z), lambda: up(a, i, hb).wait_send())
                when(jnp.logical_and(z > 0, i >= z), lambda: dn(a, i, hb).wait_send())
            y_sends(a, i, lambda c: c.wait_send())
        loop(Z, sent)
        for hb in by_line(a):
            when(z > 0, lambda: extra(a, 1, hb).wait_send())
            when(z < last, lambda: extra(a, 0, hb).wait_send())
    mp_sent(0, rbuf)
    mp_sent(1, rrbuf)

    def near_sent():
        to_chips(lambda c: c.wait_send())
    when(chip == own_chip, near_sent)

    def own_sent():
        for hb in range(2):
            p_send(hb, hb, partner).wait_send()
    when(m == owner, own_sent)
    when(chip != own_chip, lambda: p_send(core, 0, partner).wait_send())
    def line_sent(i, piece):
        src = out_bufs[i] if piece[5] == Z_FIRST else y_bufs[i]

        def one(zb):
            if piece[5] == Y_FIRST:
                by_send(i, zb).wait_send()
            when(zb != z, lambda: bz_up(i, zb, src).wait_send())
        loop(Z, one)
        if piece[5] == Z_FIRST:
            by_last(i).wait_send()
    for p in range(parts):
        for i, piece in numbered(p):
            line_sent(i, piece)
    for h in range(last_chunks):
        for sub in range(q):
            for xb in range(X):
                u_near(h, xb, sub).wait_send()
                when(xb != chip, lambda h=h, xb=xb, sub=sub: u_far(h, xb, sub).wait_send())
    for c in mom_stores(parts - 1) + [store_left, store_right, store_update]:
        c.wait()


def write_out(*refs):
    n = (len(refs) - 2) // 3
    ins, outs, bufs, sem_in, sem_out = refs[:n], refs[n:2 * n], refs[2 * n:-2], refs[-2], refs[-1]
    reads = [pltpu.make_async_copy(a, b, sem_in.at[i]) for i, (a, b) in enumerate(zip(ins, bufs))]
    writes = [pltpu.make_async_copy(b, a, sem_out.at[i]) for i, (a, b) in enumerate(zip(outs, bufs))]
    for c in reads:
        c.start()
    for r, w in zip(reads, writes):
        r.wait()
        w.start()
    for w in writes:
        w.wait()


def solution(mesh):
    dp, mp = mesh.shape["dp"], mesh.shape["mp"]
    Z, X = dp // 2, mp // 2

    def per_device(*args):
        _, rows, cols = args[0].shape
        q = rows // cols
        parts = min(PARTS, rows // 128)
        last_chunks = min(LAST, cols // 128)
        part, cw = rows // parts, cols // last_chunks
        pieces = sum(scatter_pieces(rows, cols, parts, last_chunks), [])
        n = len(pieces)
        out_b, y_b, z_b = [], [], []
        for _, _, nr, _, w, kind in pieces:
            lead = (2,) if kind == Z_FIRST else ()
            out_b.append(pltpu.VMEM((Z,) + lead + (nr, w), bf16))
            y_b.append(pltpu.VMEM((nr, w) if lead else (Z, nr, w), bf16))
            z_b.append(pltpu.VMEM((Z + 1,) + lead + (nr, w), bf16))
        flat = [a.reshape(a.shape[1:]) for a in args]
        dma = pltpu.SemaphoreType.DMA
        outs = pl.pallas_call(
            functools.partial(kernel, dp, mp, rows, cols, parts, last_chunks),
            out_shape=[jax.ShapeDtypeStruct((rows, cols), t) for t in (f32, f32, f32, f32, bf16)],
            in_specs=[pl.BlockSpec(memory_space=pl.ANY)] * 7,
            out_specs=[pl.BlockSpec(memory_space=pl.ANY)] * 5,
            scratch_shapes=[
                pltpu.VMEM((dp, rows, cols), bf16),
                pltpu.VMEM((parts, dp, cols, part), bf16),
                pltpu.VMEM((mp, rows, cols), bf16),
                pltpu.VMEM((mp, rows, cols), bf16),
                pltpu.VMEM((dp, cols, cols), bf16),
                pltpu.VMEM((last_chunks, dp, cols, cw), bf16),
                pltpu.VMEM((last_chunks, X, q, cols, cw), bf16),
                pltpu.VMEM((last_chunks, X - 1, q, cols, cw), bf16),
                pltpu.VMEM((last_chunks, X - 1, q, cols, cw), bf16),
                pltpu.VMEM((rows, cols), f32),
                pltpu.VMEM((rows, cols), f32),
                pltpu.VMEM((part, cols), f32),
                pltpu.VMEM((part, cols), f32),
                pltpu.VMEM((rows, cols), f32),
                pltpu.VMEM((rows, cols), bf16),
                pltpu.VMEM((rows, cols), bf16),
                dma((4 + 3 * parts,)),
                dma((3 + 2 * parts,)),
                dma((2 + parts, Z, 2)),
                dma((2 + parts, Z, 2)),
                dma((2 + parts, Z, 2)),
                dma((2 + parts, Z, 2)),
                dma((2 + parts, Z, 2)),
                dma((2 + parts, 2, 2)),
                dma((2 + parts, 2, 2)),
                dma((2, 2 * X)),
                dma((2, mp)),
                dma((X, q)),
                dma((X, q)),
                dma((X, q)),
                dma((X - 1, q)),
                dma((last_chunks, X, q)),
                dma((last_chunks, X, q)),
                dma((last_chunks, X, q)),
                dma((last_chunks, X - 1, q)),
                dma((2 + X,)),
                dma((2,)),
                dma((n, Z)),
                dma((n, Z)),
                dma((n, Z)),
                dma((n, Z + 1)),
            ] + out_b + y_b + z_b,
            compiler_params=pltpu.CompilerParams(
                collective_id=0, has_side_effects=True, vmem_limit_bytes=67043328
            ),
        )(*flat)
        kinds = [jax.ShapeDtypeStruct(o.shape, o.dtype) for o in outs]
        outs = pl.pallas_call(
            write_out,
            out_shape=kinds,
            in_specs=[pl.BlockSpec(memory_space=pl.ANY)] * len(outs),
            out_specs=[pl.BlockSpec(memory_space=pl.ANY)] * len(outs),
            scratch_shapes=[pltpu.VMEM(o.shape, o.dtype) for o in outs] + [dma((len(outs),)), dma((len(outs),))],
            compiler_params=pltpu.CompilerParams(vmem_limit_bytes=67043328),
        )(*outs)
        return tuple(o.reshape((1,) + o.shape) for o in outs)

    return jax.shard_map(
        per_device,
        mesh=mesh,
        in_specs=(P(None, "mp", "dp"),) * 5 + (P(None, "dp", "mp"), P(None, "mp", "dp")),
        out_specs=(P(None, "mp", "dp"),) * 5,
        check_vma=False,
    )
```
